32 devices in a mesh: lon: 8 (over z, x), lat: 4 (over y, core).
Axes of the slice: x: 2, y: 2, z: 4, core: 2. Of those that a mesh axis runs over, the one named last changes fastest.
Arguments:
- thermal_anomaly: float32 [32, 64, 512], P(None, 'lon', 'lat'), may hold values from -5 to 5
- saltiness_anomaly: float32 [32, 64, 512], P(None, 'lon', 'lat'), may hold values from -5 to 5
- zonal_flow: float32 [32, 64, 512], P(None, 'lon', 'lat'), may hold values from -1.2 to 1.2
- meridional_flow: float32 [32, 64, 512], P(None, 'lon', 'lat'), may hold values from -1.2 to 1.2
- submerged_strata_number: int32 [64, 512], P('lon', 'lat'), may hold values from 1 to 32
- sea_indicator: int32 [64, 512], P('lon', 'lat'), may hold values 0 or 1
- strata_thickness: float32 [32], replicated, may hold values from 0.5 to 2
- earlier_sea_elevation: float32 [64, 512], P('lon', 'lat'), may hold values from -3 to 3
- sea_drive_term: float32 [64, 512], P('lon', 'lat'), may hold values from -10 to 10
Outputs:
- new_temperature: float32 [32, 64, 512], P(None, 'lon', 'lat')
- new_salinity: float32 [32, 64, 512], P(None, 'lon', 'lat')
- new_u_velocity: float32 [32, 64, 512], P(None, 'lon', 'lat')
- new_v_velocity: float32 [32, 64, 512], P(None, 'lon', 'lat')
- new_surface: float32 [64, 512], P('lon', 'lat')
- residual_rms: float32 [], replicated
The draws below stay inside these ranges and needn't reach their ends.
All inputs are finite; a program needn't handle non-finite values. No bound on the sum of `sea_indicator` on one device may be relied on, other than what follows from the above.
Results may differ from the reference program's by a relative error of at most 0.0003.
Values sent between devices are 32-bit elements; how exact they have to be, the bound alone decides.
A program may use at most 128 MiB of HBM per device.

```python
import math
import jax
import jax.numpy as jnp
from jax import lax

STRATA_TOTAL = 32
CLON = 8
ITERS = 4
ZONAL_POINTS = 64
MERIDIAN_ROWS = 512
N_LON = 8


def draw_sea_drive_term(key, part):
    key_rough = jax.random.fold_in(jax.random.fold_in(key, 11), 0)
    growth = 1.0 + 2.0 * jnp.arange(ZONAL_POINTS, dtype=jnp.float32)[:, None] / (ZONAL_POINTS - 1)
    random_part = jnp.clip(jax.random.normal(key_rough, (ZONAL_POINTS, MERIDIAN_ROWS), jnp.float32), -4.0, 4.0)
    return 0.5 * growth * random_part


def touch_ends(result, key, smallest, top_value):
    shape = result.shape
    spot = [jax.random.randint(jax.random.fold_in(key, axis), (), 0, shape[axis]) for axis in range(len(shape))]
    result = result.at[tuple(spot)].set(smallest)
    longest = shape.index(max(shape))
    spot[longest] = (spot[longest] + 1) % shape[longest]
    return result.at[tuple(spot)].set(top_value)


def block_scale(key, shape, pieces, low, high):
    gain, own = 1.0, jax.random.fold_in(key, 6)
    for axis_at, shards_of in pieces:
        steps = jnp.exp(jax.random.uniform(jax.random.fold_in(own, axis_at), (shards_of,), jnp.float32, low / len(pieces), high / len(pieces)))
        gain = gain * jnp.repeat(steps, shape[axis_at] // shards_of).reshape([-1 if axis == axis_at else 1 for axis in range(len(shape))])
    return gain


def normal_values(rng, dims, scale, limit, shards=(), kind=jnp.bfloat16):
    entries = scale * jax.random.normal(rng, dims, jnp.float32)
    if shards:
        entries = entries * block_scale(rng, dims, shards, -0.22, 0.18)
    return jnp.clip(entries, -limit, limit).astype(kind)


def setup_inputs(seed: int = 0) -> dict:
    streams_of = jax.random.split(jax.random.key(seed), 10)
    return {
        "thermal_anomaly": normal_values(streams_of[0], (STRATA_TOTAL, ZONAL_POINTS, MERIDIAN_ROWS), 1.0, 5.0, ((1, 8), (2, 4)), jnp.float32),
        "saltiness_anomaly": normal_values(streams_of[1], (STRATA_TOTAL, ZONAL_POINTS, MERIDIAN_ROWS), 1.0, 5.0, ((1, 8), (2, 4)), jnp.float32),
        "zonal_flow": normal_values(streams_of[2], (STRATA_TOTAL, ZONAL_POINTS, MERIDIAN_ROWS), 0.3, 1.2, ((1, 8), (2, 4)), jnp.float32),
        "meridional_flow": normal_values(streams_of[3], (STRATA_TOTAL, ZONAL_POINTS, MERIDIAN_ROWS), 0.3, 1.2, ((1, 8), (2, 4)), jnp.float32),
        "submerged_strata_number": touch_ends(jax.random.randint(streams_of[4], (ZONAL_POINTS, MERIDIAN_ROWS), 1, STRATA_TOTAL + 1), jax.random.fold_in(streams_of[4], 1), 1, STRATA_TOTAL).astype(jnp.int32),
        "sea_indicator": touch_ends((jax.random.randint(streams_of[5], (ZONAL_POINTS, MERIDIAN_ROWS), 0, 5) < 4).astype(jnp.int32), jax.random.fold_in(streams_of[5], 1), 0, 1),
        "strata_thickness": jnp.clip(jnp.exp(jax.random.uniform(streams_of[6], (STRATA_TOTAL,), jnp.float32, math.log(0.5), math.log(2.0))), 0.5, 2.0),
        "earlier_sea_elevation": normal_values(streams_of[7], (ZONAL_POINTS, MERIDIAN_ROWS), 0.5, 3.0, ((0, 8), (1, 4)), jnp.float32),
        "sea_drive_term": draw_sea_drive_term(jax.random.fold_in(streams_of[9], 71), 0),
    }


DIFFUSION = 0.15
MIXING = 0.1
EXPANSION = 0.2
CONTRACTION = 0.15
PRESSURE_SCALE = 0.02
CORIOLIS = 0.5
FRICTION = 0.01
DIVERGENCE = 0.3
STORAGE = 0.1
SPECTRUM_LOW = 0.1
SPECTRUM_HIGH = 1.9
GRAVITY = 0.3
EPSILON = 1e-06

def extend(field, sign_rows, width):
    folded = jnp.flip(field[:, :, MERIDIAN_ROWS - width:], (1, 2)) * sign_rows[:, None, None]
    southern = jnp.zeros((field.shape[0], ZONAL_POINTS, width), field.dtype)
    padded = jnp.concatenate([southern, field, folded], axis=2)
    return jnp.concatenate([padded[:, ZONAL_POINTS - width:], padded, padded[:, :width]], axis=1)

def center(field):
    return field[:, 1:-1, 1:-1]

def to_east(field):
    return field[:, 2:, 1:-1]

def to_west(field):
    return field[:, :-2, 1:-1]

def to_north(field):
    return field[:, 1:-1, 2:]

def to_south(field):
    return field[:, 1:-1, :-2]

def shrink(field):
    return field[:, 1:-1, 1:-1]

def level_mask(strata_bottoms, strata_indices):
    level_index = jnp.arange(strata_indices).astype(strata_bottoms.dtype)[:, None, None]
    return jnp.where(level_index + 0.5 < strata_bottoms, 1.0, 0.0).astype(strata_bottoms.dtype)

def laplace(field, mask):
    middle = center(field)
    total = to_east(mask) * (to_east(field) - middle) + to_west(mask) * (to_west(field) - middle)
    total = total + to_north(mask) * (to_north(field) - middle) + to_south(mask) * (to_south(field) - middle)
    return center(mask) * total

def tracer_step(tracer, u_field, v_field, mask, thickness):
    middle = center(tracer)
    wet_mid = center(mask)
    u_mid = center(u_field)
    v_mid = center(v_field)
    flux_east = wet_mid * to_east(mask) * (0.5 * (u_mid + to_east(u_field)) * 0.5 * (middle + to_east(tracer)) - DIFFUSION * (to_east(tracer) - middle))
    flux_west = wet_mid * to_west(mask) * (0.5 * (to_west(u_field) + u_mid) * 0.5 * (to_west(tracer) + middle) - DIFFUSION * (middle - to_west(tracer)))
    flux_north = wet_mid * to_north(mask) * (0.5 * (v_mid + to_north(v_field)) * 0.5 * (middle + to_north(tracer)) - DIFFUSION * (to_north(tracer) - middle))
    flux_south = wet_mid * to_south(mask) * (0.5 * (to_south(v_field) + v_mid) * 0.5 * (to_south(tracer) + middle) - DIFFUSION * (middle - to_south(tracer)))
    horizontal = flux_west - flux_east + flux_south - flux_north
    spacing = 0.5 * (thickness[1:] + thickness[:-1])
    vflux = wet_mid[1:] * wet_mid[:-1] * (middle[1:] - middle[:-1]) / spacing[:, None, None]
    zero_plane = jnp.zeros_like(middle[:1])
    upper_flux = jnp.concatenate([vflux, zero_plane], axis=0)
    lower_flux = jnp.concatenate([zero_plane, vflux], axis=0)
    vertical = MIXING * (upper_flux - lower_flux) / thickness[:, None, None]
    return wet_mid * (middle + horizontal + vertical)

def pressure_gradients(temp_rim, salt_rim, mask, thickness):
    density = (CONTRACTION * salt_rim - EXPANSION * temp_rim) * thickness[:, None, None] * mask
    pressure = jnp.cumsum(density, axis=0)
    middle = center(pressure)
    wet_mid = center(mask)
    grad_x = 0.5 * wet_mid * (to_east(mask) * (to_east(pressure) - middle) + to_west(mask) * (middle - to_west(pressure)))
    grad_y = 0.5 * wet_mid * (to_north(mask) * (to_north(pressure) - middle) + to_south(mask) * (middle - to_south(pressure)))
    return (grad_x, grad_y)

def baroclinic(narrow, mask_narrow, lap_u, lap_v, thickness, coriolis, strata_indices):
    temp_rim = narrow[:strata_indices]
    salt_rim = narrow[strata_indices:2 * strata_indices]
    u_rim = narrow[2 * strata_indices:3 * strata_indices]
    v_rim = narrow[3 * strata_indices:4 * strata_indices]
    new_temp = tracer_step(temp_rim, u_rim, v_rim, mask_narrow, thickness)
    new_salt = tracer_step(salt_rim, u_rim, v_rim, mask_narrow, thickness)
    grad_x, grad_y = pressure_gradients(temp_rim, salt_rim, mask_narrow, thickness)
    friction_u = laplace(lap_u, mask_narrow)
    friction_v = laplace(lap_v, mask_narrow)
    wet_mid = center(mask_narrow)
    u_mid = center(u_rim)
    v_mid = center(v_rim)
    u_star = wet_mid * (u_mid + coriolis * v_mid - PRESSURE_SCALE * grad_x - FRICTION * friction_u)
    v_star = wet_mid * (v_mid - coriolis * u_mid - PRESSURE_SCALE * grad_y - FRICTION * friction_v)
    height = lax.optimization_barrier(jnp.sum(thickness[:, None, None] * mask_narrow, axis=0, keepdims=True))
    return (new_temp, new_salt, u_star, v_star, height, wet_mid)

def solver_weights(height, strata_indices):
    middle = center(height)
    w_east = jnp.minimum(middle, to_east(height)) / strata_indices
    w_west = jnp.minimum(middle, to_west(height)) / strata_indices
    w_north = jnp.minimum(middle, to_north(height)) / strata_indices
    w_south = jnp.minimum(middle, to_south(height)) / strata_indices
    diagonal = STORAGE + w_east + w_west + w_north + w_south
    return (w_east, w_west, w_north, w_south, diagonal)

def apply_operator(weights, field_rim):
    w_east, w_west, w_north, w_south, diagonal = weights
    coupled = w_east * to_east(field_rim) + w_west * to_west(field_rim) + w_north * to_north(field_rim) + w_south * to_south(field_rim)
    return diagonal * center(field_rim) - coupled

def line_factor(w_west, w_east, diagonal):
    count = diagonal.shape[0]
    position = jnp.arange(count).reshape((count,) + (1,) * (diagonal.ndim - 1))
    lower_band = jnp.where(position > 0, -w_west, 0.0)
    upper_band = jnp.where(position < count - 1, -w_east, 0.0)

    def forward(previous, inputs):
        lower_row, diag_row, upper_row = inputs
        inverse = 1.0 / (diag_row - lower_row * previous)
        factor = upper_row * inverse
        return (factor, (factor, inverse))
    _, (factors, pivots) = lax.scan(forward, jnp.zeros_like(diagonal[0]), (lower_band, diagonal, upper_band))
    return (lower_band, factors, pivots)

def line_solve(lower_band, factors, pivots, values):

    def forward(previous, inputs):
        lower_row, inverse, value_row = inputs
        current = (value_row - lower_row * previous) * inverse
        return (current, current)
    _, partial_rows = lax.scan(forward, jnp.zeros_like(values[0]), (lower_band, pivots, values))

    def backward(following, inputs):
        factor, partial_row = inputs
        current = partial_row - factor * following
        return (current, current)
    _, solved = lax.scan(backward, jnp.zeros_like(values[0]), (factors, partial_rows), reverse=True)
    return solved

def to_lines(field):
    return jnp.transpose(field.reshape(N_LON, CLON, MERIDIAN_ROWS), (1, 0, 2))

def from_lines(field):
    return jnp.transpose(field, (1, 0, 2)).reshape(ZONAL_POINTS, MERIDIAN_ROWS)

def reference(thermal_anomaly, saltiness_anomaly, zonal_flow, meridional_flow, submerged_strata_number, sea_indicator, strata_thickness, earlier_sea_elevation, sea_drive_term):
    strata_indices = thermal_anomaly.shape[0]
    real_number_kind = thermal_anomaly.dtype
    wet_surface = sea_indicator.astype(real_number_kind)
    strata_bottoms = (submerged_strata_number * sea_indicator).astype(real_number_kind)[None]
    joined_tracers = jnp.concatenate([thermal_anomaly, saltiness_anomaly, zonal_flow, meridional_flow, strata_bottoms], axis=0)
    sign_rows = jnp.concatenate([jnp.ones(2 * strata_indices, real_number_kind), -jnp.ones(2 * strata_indices, real_number_kind), jnp.ones(1, real_number_kind)])
    wide_rim = extend(joined_tracers, sign_rows, 2)
    mask_wide = level_mask(wide_rim[4 * strata_indices:], strata_indices)
    narrow = shrink(wide_rim)
    mask_narrow = shrink(mask_wide)
    lap_u = laplace(wide_rim[2 * strata_indices:3 * strata_indices], mask_wide)
    lap_v = laplace(wide_rim[3 * strata_indices:4 * strata_indices], mask_wide)
    lat_index = jnp.arange(MERIDIAN_ROWS).astype(real_number_kind)
    coriolis = CORIOLIS * (2.0 * (lat_index + 0.5) / MERIDIAN_ROWS - 1.0)
    new_temp, new_salt, u_star, v_star, height, wet_mid = baroclinic(narrow, mask_narrow, lap_u, lap_v, strata_thickness, coriolis, strata_indices)
    weights = solver_weights(height, strata_indices)
    lower_band, factors, pivots = line_factor(to_lines(weights[1][0]), to_lines(weights[0][0]), to_lines(weights[4][0]))

    def precondition(values):
        return from_lines(line_solve(lower_band, factors, pivots, to_lines(values[0])))[None]
    transport_u = lax.optimization_barrier(jnp.sum(strata_thickness[:, None, None] * u_star, axis=0, keepdims=True))
    transport_v = lax.optimization_barrier(jnp.sum(strata_thickness[:, None, None] * v_star, axis=0, keepdims=True))
    start_field = (wet_surface * earlier_sea_elevation)[None]
    surface_signs = jnp.array([-1.0, -1.0, 1.0], real_number_kind)
    plus_one = jnp.ones(1, real_number_kind)
    moved = extend(jnp.concatenate([transport_u, transport_v, start_field], axis=0), surface_signs, 1)
    divergence = 0.5 * (to_east(moved[0:1]) - to_west(moved[0:1])) + 0.5 * (to_north(moved[1:2]) - to_south(moved[1:2]))
    right_side = wet_surface[None] * (sea_drive_term[None] - DIVERGENCE * divergence)
    solution = center(moved[2:3])
    residual = right_side - apply_operator(weights, moved[2:3])
    spectrum_mid = 0.5 * (SPECTRUM_HIGH + SPECTRUM_LOW)
    spectrum_half = 0.5 * (SPECTRUM_HIGH - SPECTRUM_LOW)
    spectrum_ratio = spectrum_mid / spectrum_half
    direction = precondition(residual) / spectrum_mid
    cheby_rho = 1.0 / spectrum_ratio
    for step_index in range(ITERS):
        solution = solution + direction
        if step_index + 1 < ITERS:
            residual = residual - apply_operator(weights, extend(direction, plus_one, 1))
            rho_next = 1.0 / (2.0 * spectrum_ratio - cheby_rho)
            direction = rho_next * cheby_rho * direction + 2.0 * rho_next / spectrum_half * precondition(residual)
            cheby_rho = rho_next
    final_rim = extend(solution, plus_one, 1)
    final_residual = right_side - apply_operator(weights, final_rim)
    residual_rms = jnp.sqrt(jnp.sum(final_residual * final_residual) / (ZONAL_POINTS * MERIDIAN_ROWS) + EPSILON)
    slope_x = 0.5 * (to_east(final_rim) - to_west(final_rim))
    slope_y = 0.5 * (to_north(final_rim) - to_south(final_rim))
    new_u = wet_mid * (u_star - GRAVITY * slope_x)
    new_v = wet_mid * (v_star - GRAVITY * slope_y)
    return (new_temp, new_salt, new_u, new_v, solution[0], residual_rms)
```

```python
import functools

import jax
import jax.numpy as jnp
from jax import lax
from jax.experimental import pallas as pl
from jax.experimental.pallas import tpu as pltpu
from jax.sharding import PartitionSpec as P

ITERS = 4
DIFFUSION = 0.15
MIXING = 0.1
EXPANSION = 0.2
CONTRACTION = 0.15
PRESSURE_SCALE = 0.02
CORIOLIS = 0.5
FRICTION = 0.01
DIVERGENCE = 0.3
STORAGE = 0.1
SPECTRUM_LOW = 0.1
SPECTRUM_HIGH = 1.9
GRAVITY = 0.3
EPSILON = 1e-06

MESH = pl.DeviceIdType.MESH
F32 = jnp.float32
SLOT_N, SLOT_NE, SLOT_NW, SLOT_S, SLOT_SE, SLOT_SW = range(6)
SEM_E, SEM_W = 6, 7
EARLY = 3
LATE = 2


def iota(shape, axis):
    return lax.broadcasted_iota(jnp.int32, shape, axis)


def flip_rows(x):
    n = x.shape[0]
    row = iota(x.shape, 0)
    bit = n // 2
    while bit:
        up = pltpu.roll(x, bit, 0)
        down = pltpu.roll(x, n - bit, 0)
        x = up if 2 * bit == n else jnp.where((row & bit) != 0, up, down)
        bit //= 2
    return x


def step_kernel(n_lon, n_lat, KC, *refs):
    sources, refs = refs[:9], refs[9:]
    (ot_ref, os_ref, ou_ref, ov_ref, ox_ref), refs = refs[:5], refs[5:]
    inputs, refs = refs[:9], refs[9:]
    t_ref, s_ref, u_ref, v_ref, num_ref, sea_ref, thick_ref, eta_ref, drive_ref = inputs
    (epk, wpk, ebase, wbase, npk, spk, slot_e, slot_w, base_e, base_w, slots, rim, early, late, held,
     load_sem, send_sem, recv_sem, side_send, side_recv, cast_send, cast_recv) = refs
    K, NI, NJ = t_ref.shape
    NC = K // KC
    loads = [pltpu.make_async_copy(src, dst, load_sem.at[i]) for i, (src, dst) in enumerate(zip(sources, inputs))]
    for load in loads[4:] + loads[:4]:
        load.start()
    p = lax.axis_index("lon")
    q = lax.axis_index("lat")
    east_dev = lax.rem(p + 1, n_lon)
    west_dev = lax.rem(p + n_lon - 1, n_lon)
    at_pole = q == n_lat - 1
    not_pole = q < n_lat - 1
    not_south = q > 0
    mirror = n_lon - 1 - p
    mirror_ne = lax.rem(2 * n_lon - 2 - p, n_lon)
    mirror_nw = lax.rem(2 * n_lon - p, n_lon)
    ne_remote = jnp.logical_or(not_pole, mirror_ne != p)
    nw_remote = jnp.logical_or(not_pole, mirror_nw != p)
    ne_self = jnp.logical_and(at_pole, mirror_ne == p)
    nw_self = jnp.logical_and(at_pole, mirror_nw == p)

    barrier = pltpu.get_barrier_semaphore()

    def greet(lon, lat):
        pl.semaphore_signal(barrier, inc=1, device_id={"lon": lon, "lat": lat}, device_id_type=MESH)

    greet(east_dev, q)
    greet(west_dev, q)

    @pl.when(not_south)
    def _():
        for lon in (p, east_dev, west_dev):
            greet(lon, q - 1)

    @pl.when(not_pole)
    def _():
        for lon in (p, east_dev, west_dev):
            greet(lon, q + 1)

    @pl.when(at_pole)
    def _():
        greet(mirror, q)

    @pl.when(jnp.logical_and(at_pole, mirror_ne != p))
    def _():
        greet(mirror_ne, q)

    @pl.when(jnp.logical_and(at_pole, mirror_nw != p))
    def _():
        greet(mirror_nw, q)

    parity = lax.rem(q, 2)
    partner = q + 1 - 2 * parity
    n_half = n_lon * n_lat // 2
    me_half = (q // 2) * n_lon + p

    def half_peer(r):
        other = lax.rem(me_half + r, n_half)
        return lax.rem(other, n_lon), 2 * (other // n_lon) + parity

    def greet_half(r, carry):
        greet(*half_peer(r))
        return carry

    lax.fori_loop(1, n_half, greet_half, 0)
    greet(p, partner)

    for load in loads:
        load.wait()
    sub = iota((NI, NJ), 0)
    lane = iota((NI, NJ), 1)
    depth = (num_ref[...] * sea_ref[...]).astype(F32)
    height = jnp.zeros((NI, NJ), F32)
    for k in range(K):
        height = height + jnp.where(depth > k + 0.5, thick_ref[k], 0.0)
    early[parity, me_half, 0] = height
    early[parity, me_half, 1] = sea_ref[...].astype(F32) * eta_ref[...]
    early[parity, me_half, 2] = drive_ref[...]

    fields = (t_ref, s_ref, u_ref, v_ref)
    for pk, base, d1, d2 in ((epk, ebase, NI - 1, NI - 2), (wpk, wbase, 0, 1)):
        for c in range(NC):
            levels = slice(c * KC, (c + 1) * KC)
            for f, (ref, d) in enumerate(((t_ref, d1), (s_ref, d1), (u_ref, d1), (v_ref, d1), (u_ref, d2), (v_ref, d2))):
                pk[c, f * KC:(f + 1) * KC, :] = ref[levels, d, :]
        base[...] = jnp.where(sub == 0, depth[d1:d1 + 1, :], depth[d2:d2 + 1, :])

    n0 = jnp.zeros((NI, NJ), F32)
    s0 = jnp.zeros((NI, NJ), F32)
    n1 = jnp.zeros((NI, NJ), F32)
    s1 = jnp.zeros((NI, NJ), F32)

    def put(acc, x, source, target):
        moved = pltpu.roll(x, (target - source) % NJ, 1) if source != target else x
        return jnp.where(lane == target, moved, acc)

    for f, ref in enumerate(fields):
        for k in range(K):
            x = ref[k]
            target = f * K + k
            n0 = put(n0, x, NJ - 1, target)
            s0 = put(s0, x, 0, target)
            if f >= 2:
                n1 = put(n1, x, NJ - 2, target)
                s1 = put(s1, x, 1, target)
    n1 = put(put(n1, depth, NJ - 1, 0), depth, NJ - 2, 1)
    s1 = put(put(s1, depth, 0, 0), depth, 1, 1)
    npk[0] = n0
    npk[1] = n1
    spk[0] = s0
    spk[1] = s1

    peers = (3 + n_half + 2 * not_pole.astype(jnp.int32) + 3 * not_south.astype(jnp.int32)
             + at_pole.astype(jnp.int32) * ((mirror_ne != p).astype(jnp.int32) + (mirror_nw != p).astype(jnp.int32)))
    pl.semaphore_wait(barrier, peers)

    def copy(src, dst, lon, lat, out, into):
        return pltpu.make_async_remote_copy(
            src_ref=src, dst_ref=dst, send_sem=out, recv_sem=into,
            device_id={"lon": lon, "lat": lat}, device_id_type=MESH)

    def edge(src, slot, lon, lat, out):
        return copy(src, slots.at[slot], lon, lat, send_sem.at[out], recv_sem.at[slot])

    def side_east(c):
        return copy(epk.at[c], slot_w.at[c], east_dev, q, side_send.at[0, c], side_recv.at[0, c])

    def side_west(c):
        return copy(wpk.at[c], slot_e.at[c], west_dev, q, side_send.at[1, c], side_recv.at[1, c])

    base_east = copy(ebase, base_w, east_dev, q, send_sem.at[SEM_E], recv_sem.at[SEM_W])
    base_west = copy(wbase, base_e, west_dev, q, send_sem.at[SEM_W], recv_sem.at[SEM_E])
    base_east.start()
    base_west.start()
    side_east(0).start()
    side_west(0).start()

    @pl.when(not_south)
    def _():
        edge(spk, SLOT_N, p, q - 1, SLOT_S).start()
        edge(spk, SLOT_NW, east_dev, q - 1, SLOT_SE).start()
        edge(spk, SLOT_NE, west_dev, q - 1, SLOT_SW).start()

    @pl.when(not_pole)
    def _():
        edge(npk, SLOT_S, p, q + 1, SLOT_N).start()
        edge(npk, SLOT_SW, east_dev, q + 1, SLOT_NE).start()
        edge(npk, SLOT_SE, west_dev, q + 1, SLOT_NW).start()

    @pl.when(at_pole)
    def _():
        edge(npk, SLOT_N, mirror, q, SLOT_N).start()

    @pl.when(jnp.logical_and(at_pole, mirror_ne != p))
    def _():
        edge(npk, SLOT_NE, mirror_ne, q, SLOT_NE).start()

    @pl.when(jnp.logical_and(at_pole, mirror_nw != p))
    def _():
        edge(npk, SLOT_NW, mirror_nw, q, SLOT_NW).start()

    def cast(buf, which):
        def send(r, carry):
            lon, lat = half_peer(r)
            mine = buf.at[parity, me_half]
            pltpu.make_async_remote_copy(
                src_ref=mine, dst_ref=mine, send_sem=cast_send.at[which], recv_sem=cast_recv.at[which],
                device_id={"lon": lon, "lat": lat}, device_id_type=MESH).start()
            return carry

        lax.fori_loop(1, n_half, send, 0)

    def cast_wait(buf, sem):
        rest = buf.at[parity, pl.ds(0, n_half - 1)]
        pltpu.make_async_copy(rest, rest, sem).wait()

    def hand_over(buf, which):
        return pltpu.make_async_remote_copy(
            src_ref=buf.at[parity], dst_ref=buf.at[parity], send_sem=cast_send.at[which],
            recv_sem=cast_recv.at[which], device_id={"lon": p, "lat": partner}, device_id_type=MESH)

    for c in range(1, NC):
        side_east(c).start()
        side_west(c).start()

    edge(npk, SLOT_N, p, q, SLOT_N).wait_recv()

    @pl.when(ne_remote)
    def _():
        edge(npk, SLOT_NE, p, q, SLOT_NE).wait_recv()

    @pl.when(nw_remote)
    def _():
        edge(npk, SLOT_NW, p, q, SLOT_NW).wait_recv()

    @pl.when(not_south)
    def _():
        for slot in (SLOT_S, SLOT_SE, SLOT_SW):
            edge(spk, slot, p, q, slot).wait_recv()

    sign = jnp.where(lane >= 2 * K, -1.0, 1.0).astype(F32)

    def northern(slot, own):
        out = []
        for i in range(2):
            x = slots[slot, i]
            if own is not None:
                x = jnp.where(own, npk[i], x)
            out.append(jnp.where(at_pole, flip_rows(x) * sign, x))
        return out

    def southern(slot):
        return [jnp.where(not_south, slots[slot, i], 0.0) for i in range(2)]

    pn0, pn1 = northern(SLOT_N, None)
    pne0, pne1 = northern(SLOT_NE, ne_self)
    pnw0, pnw1 = northern(SLOT_NW, nw_self)
    ps0, ps1 = southern(SLOT_S)
    pse0, pse1 = southern(SLOT_SE)
    psw0, psw1 = southern(SLOT_SW)

    def shift_e(x, row):
        return jnp.where(sub == NI - 1, row, pltpu.roll(x, NI - 1, 0))

    def shift_w(x, row):
        return jnp.where(sub == 0, row, pltpu.roll(x, 1, 0))

    level_l = (lane - K * (lane // K)).astype(F32) + 0.5

    def wet_l(d):
        return jnp.where(level_l < d, 1.0, 0.0)

    def spread(x, i):
        return jnp.broadcast_to(x[:, i:i + 1], (NI, NJ))

    def packed_lap(c0, c1, e0, e1, w0, w1, own, own_depth):
        d = spread(c1, 0)
        de = shift_e(d, jnp.broadcast_to(e1[0:1, 0:1], (NI, NJ)))
        dw = shift_w(d, jnp.broadcast_to(w1[NI - 1:NI, 0:1], (NI, NJ)))
        xe = shift_e(c0, jnp.broadcast_to(e0[0:1, :], (NI, NJ)))
        xw = shift_w(c0, jnp.broadcast_to(w0[NI - 1:NI, :], (NI, NJ)))
        total = wet_l(de) * (xe - c0) + wet_l(dw) * (xw - c0)
        total = total + wet_l(spread(c1, 1)) * (c1 - c0) + wet_l(own_depth) * (own - c0)
        return wet_l(d) * total

    lap_n = packed_lap(pn0, pn1, pne0, pne1, pnw0, pnw1, n0, spread(depth, NJ - 1))
    lap_s = packed_lap(ps0, ps1, pse0, pse1, psw0, psw1, s0, spread(depth, 0))
    rim[4, 0:NI, :] = lap_n
    rim[5, 0:NI, :] = lap_s
    rim[4, NI:2 * NI, :] = pn0
    rim[5, NI:2 * NI, :] = ps0

    base_east.wait_recv()
    base_west.wait_recv()

    row_c = iota((KC, NJ), 0)
    lane_c = iota((KC, NJ), 1)

    def wide(row):
        return jnp.broadcast_to(row, (KC, NJ))

    rim[6, 0:NI, :] = pne0
    rim[6, NI:2 * NI, :] = pse0
    rim[7, 0:NI, :] = pnw0
    rim[7, NI:2 * NI, :] = psw0
    side_depths = []
    for base, d1, cn1, cs1 in ((base_e, NI - 1, pne1[0:1], pse1[0:1]), (base_w, 0, pnw1[NI - 1:], psw1[NI - 1:])):
        d = wide(base[0:1, :])
        dn = jnp.where(lane_c == NJ - 1, jnp.broadcast_to(cn1[:, 0:1], (KC, NJ)), pltpu.roll(d, NJ - 1, 1))
        ds = jnp.where(lane_c == 0, jnp.broadcast_to(cs1[:, 0:1], (KC, NJ)), pltpu.roll(d, 1, 1))
        side_depths.append((d, wide(base[1:2, :]), wide(depth[d1:d1 + 1, :]), dn, ds))

    def side_laps(c):
        level_c = (row_c + c * KC).astype(F32) + 0.5
        for side, (slot, pk, corner) in enumerate(((slot_e, epk, 0), (slot_w, wpk, NI - 1))):
            mid, far, own, mn, ms = [jnp.where(level_c < d, 1.0, 0.0) for d in side_depths[side]]
            cn0 = rim[6 + side, corner:corner + 1, :]
            cs0 = rim[6 + side, NI + corner:NI + corner + 1, :]
            for i in range(2):
                f = 2 + i
                x = slot[c, f * KC:(f + 1) * KC, :]
                pick = lane_c == row_c + (c * KC + f * K)
                cn = jnp.sum(jnp.where(pick, wide(cn0), 0.0), axis=1, keepdims=True)
                cs = jnp.sum(jnp.where(pick, wide(cs0), 0.0), axis=1, keepdims=True)
                xn = jnp.where(lane_c == NJ - 1, jnp.broadcast_to(cn, (KC, NJ)), pltpu.roll(x, NJ - 1, 1))
                xs = jnp.where(lane_c == 0, jnp.broadcast_to(cs, (KC, NJ)), pltpu.roll(x, 1, 1))
                total = far * (slot[c, (4 + i) * KC:(5 + i) * KC, :] - x)
                total = total + own * (pk[c, f * KC:(f + 1) * KC, :] - x) + mn * (xn - x) + ms * (xs - x)
                rim[2 * side + i, 0:KC, :] = mid * total

    def shift_n(x, packed, source):
        return jnp.where(lane == NJ - 1, pltpu.roll(packed, NJ - 1 - source, 1), pltpu.roll(x, NJ - 1, 1))

    def shift_s(x, packed, source):
        return jnp.where(lane == 0, pltpu.roll(packed, lax.rem(NJ - source, NJ), 1), pltpu.roll(x, 1, 1))

    depth_e = shift_e(depth, base_e[0:1, :])
    depth_w = shift_w(depth, base_w[0:1, :])
    depth_n = shift_n(depth, pn1, 0)
    depth_s = jnp.where(lane == 0, ps1, pltpu.roll(depth, 1, 1))
    both_e = jnp.minimum(depth, depth_e)
    both_w = jnp.minimum(depth, depth_w)
    both_n = jnp.minimum(depth, depth_n)
    both_s = jnp.minimum(depth, depth_s)
    lat_index = (q * NJ + lane).astype(F32)
    coriolis = CORIOLIS * (2.0 * (lat_index + 0.5) / (n_lat * NJ) - 1.0)

    zero = jnp.zeros((NI, NJ), F32)
    cast(early, 0)

    def around(c, inner, ref, f):
        k = c * KC + inner
        x = ref[k]
        row = f * KC + inner
        return (x, shift_e(x, slot_e[c, row:row + 1, :]), shift_w(x, slot_w[c, row:row + 1, :]),
                shift_n(x, rim[4, NI:2 * NI, :], f * K + k), shift_s(x, rim[5, NI:2 * NI, :], f * K + k))

    def tracers(c, i, carry):
        k = c * KC + i
        flux_t, flux_s = carry
        kf = lax.convert_element_type(k, F32) + 0.5
        h = thick_ref[k]
        nxt = jnp.minimum(k + 1, K - 1)
        h_next = thick_ref[nxt]
        hv = jnp.full((NI, NJ), h, F32)
        inv_space = 1.0 / (0.5 * (hv + h_next))
        inv_h = MIXING / hv

        def wet(d):
            return jnp.where(d > kf, 1.0, 0.0)

        mc = wet(depth)
        me, mw, mn, ms = wet(both_e), wet(both_w), wet(both_n), wet(both_s)
        below = jnp.where(jnp.logical_and(depth > kf + 1.0, k < K - 1), inv_space, 0.0)
        t = around(c, i, t_ref, 0)
        s = around(c, i, s_ref, 1)
        u0, ue, uw = around(c, i, u_ref, 2)[:3]
        v0, _, _, vn, vs = around(c, i, v_ref, 3)
        ae = 0.25 * me * (u0 + ue)
        aw = 0.25 * mw * (u0 + uw)
        an = 0.25 * mn * (v0 + vn)
        as_ = 0.25 * ms * (v0 + vs)
        ge, gw, gn, gs = DIFFUSION * me, DIFFUSION * mw, DIFFUSION * mn, DIFFUSION * ms

        def tracer(x, ref, flux_above):
            c, e, w, n, so = x
            total = aw * (w + c) - gw * (c - w) - ae * (c + e) + ge * (e - c)
            total = total + as_ * (so + c) - gs * (c - so) - an * (c + n) + gn * (n - c)
            flux = below * (ref[nxt] - c)
            return mc * (c + total + inv_h * (flux - flux_above)), flux

        new_t, flux_t = tracer(t, t_ref, flux_t)
        new_s, flux_s = tracer(s, s_ref, flux_s)
        ot_ref[k] = new_t
        os_ref[k] = new_s
        return flux_t, flux_s

    def level(c, i, carry):
        k = c * KC + i
        inner = i
        pc, pe, pw, pn_, ps_, tu, tv = carry
        kf = lax.convert_element_type(k, F32) + 0.5
        h = thick_ref[k]

        def wet(d):
            return jnp.where(d > kf, 1.0, 0.0)

        mc = wet(depth)
        me, mw, mn, ms = wet(both_e), wet(both_w), wet(both_n), wet(both_s)
        lapn = rim[4, 0:NI, :]
        laps = rim[5, 0:NI, :]
        t = around(c, i, t_ref, 0)
        s = around(c, i, s_ref, 1)
        u = around(c, i, u_ref, 2)
        v = around(c, i, v_ref, 3)
        pressures = []
        for i, (acc, d) in enumerate(((pc, depth), (pe, depth_e), (pw, depth_w), (pn_, depth_n), (ps_, depth_s))):
            density = CONTRACTION * s[i] - EXPANSION * t[i]
            pressures.append(acc + jnp.where(d > kf, density * h, 0.0))
        pc, pe, pw, pn_, ps_ = pressures
        grad_x = 0.5 * (me * (pe - pc) + mw * (pc - pw))
        grad_y = 0.5 * (mn * (pn_ - pc) + ms * (pc - ps_))

        def biharmonic(x, i):
            c, e, w, n, so = x
            lap = me * (e - c) + mw * (w - c) + mn * (n - c) + ms * (so - c)
            le = shift_e(lap, rim[i, inner:inner + 1, :])
            lw = shift_w(lap, rim[2 + i, inner:inner + 1, :])
            source = (2 + i) * K + k
            ln = shift_n(lap, lapn, source)
            ls = shift_s(lap, laps, source)
            return me * (le - lap) + mw * (lw - lap) + mn * (ln - lap) + ms * (ls - lap)

        u_star = mc * (u[0] + coriolis * v[0] - PRESSURE_SCALE * grad_x - FRICTION * biharmonic(u, 0))
        v_star = mc * (v[0] - coriolis * u[0] - PRESSURE_SCALE * grad_y - FRICTION * biharmonic(v, 1))
        ou_ref[k] = u_star
        ov_ref[k] = v_star
        return (pc, pe, pw, pn_, ps_, tu + h * u_star, tv + h * v_star)

    def chunk(c, carry):
        side_east(c).wait_recv()
        side_west(c).wait_recv()
        side_laps(c)
        for i in range(KC):
            carry = level(c, i, carry)
        return carry

    carry = lax.fori_loop(0, NC, chunk, (zero,) * 7)
    late[parity, me_half, 0] = carry[5]
    late[parity, me_half, 1] = carry[6]
    cast(late, 1)

    def tracer_chunk(c, carry):
        for i in range(KC):
            carry = tracers(c, i, carry)
        return carry

    lax.fori_loop(0, NC, tracer_chunk, (zero,) * 2)

    cast_wait(early, cast_recv.at[0])
    early_over = hand_over(early, 2)
    early_over.start()
    early_over.wait_recv()

    def loader(buf, count):
        flat = buf.reshape(2 * n_half * count * NI, NJ)

        def load(f):
            return [[flat[pl.ds((((b % 2) * n_half + (b // 2) * n_lon) * count + f) * NI + s, n_lon,
                                stride=count * NI), :] for s in range(NI)] for b in range(n_lat)]

        return load

    def late_loader():
        cast_wait(late, cast_recv.at[1])
        late_over = hand_over(late, 3)
        late_over.start()
        late_over.wait_recv()
        return loader(late, LATE)

    x, slope_x, slope_y, rms = surface_solve(loader(early, EARLY), late_loader, n_lon, n_lat, K, NI, NJ,
                                             n_lon * NI * n_lat * NJ)
    for i, field in enumerate((x, slope_x, slope_y)):
        for b in range(n_lat):
            for s in range(NI):
                held[i, b, pl.ds(s, n_lon, stride=NI), :] = field[b][s]
    block = pl.ds(pl.multiple_of(p * NI, NI), NI)
    ox_ref[0] = held[0, q, block, :]
    ox_ref[1] = GRAVITY * held[1, q, block, :]
    ox_ref[2] = GRAVITY * held[2, q, block, :]
    ox_ref[3] = jnp.broadcast_to(rms, (NI, NJ))
    ox_ref[4] = depth

    cast_wait(early, cast_send.at[0])
    cast_wait(late, cast_send.at[1])
    early_over.wait_send()
    hand_over(late, 3).wait_send()

    base_east.wait_send()
    base_west.wait_send()
    for c in range(NC):
        side_east(c).wait_send()
        side_west(c).wait_send()

    @pl.when(not_south)
    def _():
        for out in (SLOT_S, SLOT_SE, SLOT_SW):
            edge(spk, SLOT_N, p, q, out).wait_send()

    edge(npk, SLOT_N, p, q, SLOT_N).wait_send()

    @pl.when(ne_remote)
    def _():
        edge(npk, SLOT_NE, p, q, SLOT_NE).wait_send()

    @pl.when(nw_remote)
    def _():
        edge(npk, SLOT_NW, p, q, SLOT_NW).wait_send()


def surface_solve(load, load_late, n_lon, n_lat, K, NI, NJ, cells):
    tiles = range(n_lat)
    lines = range(NI)
    lane = iota((n_lon, NJ), 1)

    def every(fn, *arrays):
        return [[fn(*(a[b][s] for a in arrays)) for s in lines] for b in tiles]

    def east(x):
        return [x[b][1:] + [pltpu.roll(x[b][0], n_lon - 1, 0)] for b in tiles]

    def west(x):
        return [[pltpu.roll(x[b][NI - 1], 1, 0)] + x[b][:-1] for b in tiles]

    def north(x, sign):
        out = []
        for b in tiles:
            row = []
            for s in lines:
                if b + 1 < n_lat:
                    beyond = pltpu.roll(x[b + 1][s], NJ - 1, 1)
                else:
                    beyond = flip_rows(x[b][NI - 1 - s])
                    beyond = -beyond if sign < 0 else beyond
                row.append(jnp.where(lane == NJ - 1, beyond, pltpu.roll(x[b][s], NJ - 1, 1)))
            out.append(row)
        return out

    def south(x):
        out = []
        for b in tiles:
            row = []
            for s in lines:
                beyond = pltpu.roll(x[b - 1][s], 1, 1) if b > 0 else 0.0
                row.append(jnp.where(lane == 0, beyond, pltpu.roll(x[b][s], 1, 1)))
            out.append(row)
        return out

    height = load(0)
    scale = lambda a, c: jnp.minimum(a, c) * (1.0 / K)
    w_e = every(scale, height, east(height))
    w_w = every(scale, height, west(height))
    w_n = every(scale, height, north(height, 1))
    w_s = every(scale, height, south(height))
    diag = every(lambda a, b, c, d: STORAGE + a + b + c + d, w_e, w_w, w_n, w_s)

    def apply(x):
        return every(
            lambda dg, c, we, e, ww, w, wn, n, ws, s: dg * c - (we * e + ww * w + wn * n + ws * s),
            diag, x, w_e, east(x), w_w, west(x), w_n, north(x, 1), w_s, south(x))

    factors = [[None] * NI for _ in tiles]
    pivots = [[None] * NI for _ in tiles]
    for b in tiles:
        for s in lines:
            pivot = diag[b][s]
            if s > 0:
                pivot = pivot + w_w[b][s] * factors[b][s - 1]
            pivots[b][s] = 1.0 / pivot
            factors[b][s] = -w_e[b][s] * pivots[b][s]

    def precondition(r):
        out = []
        for b in tiles:
            part = []
            for s in lines:
                value = r[b][s]
                if s > 0:
                    value = value + w_w[b][s] * part[s - 1]
                part.append(value * pivots[b][s])
            for s in range(NI - 2, -1, -1):
                part[s] = part[s] - factors[b][s] * part[s + 1]
            out.append(part)
        return out

    x = load(1)
    drive = load(2)
    start = every(lambda h, d, a: jnp.where(h > 0.0, d, 0.0) - a, height, drive, apply(x))
    load = load_late()
    t_u = load(0)
    t_v = load(1)
    residual = every(
        lambda h, d, e, w, n, s: d - jnp.where(h > 0.0, 0.5 * DIVERGENCE * ((e - w) + (n - s)), 0.0),
        height, start, east(t_u), west(t_u), north(t_v, -1), south(t_v))
    mid = 0.5 * (SPECTRUM_HIGH + SPECTRUM_LOW)
    half = 0.5 * (SPECTRUM_HIGH - SPECTRUM_LOW)
    ratio = mid / half
    direction = every(lambda a: a / mid, precondition(residual))
    rho = 1.0 / ratio
    for step in range(ITERS):
        x = every(lambda a, b: a + b, x, direction)
        residual = every(lambda a, b: a - b, residual, apply(direction))
        if step + 1 < ITERS:
            rho_next = 1.0 / (2.0 * ratio - rho)
            keep, gain = rho_next * rho, 2.0 * rho_next / half
            direction = every(lambda d, z: keep * d + gain * z, direction, precondition(residual))
            rho = rho_next
    squares = every(lambda a: a * a, residual)
    total = functools.reduce(lambda a, b: a + b, [squares[b][s] for b in tiles for s in lines])
    total = jnp.sum(jnp.sum(total, axis=1, keepdims=True), axis=0, keepdims=True)
    rms = jnp.sqrt(total / cells + EPSILON)
    slope_x = every(lambda e, w: 0.5 * (e - w), east(x), west(x))
    slope_y = every(lambda n, s: 0.5 * (n - s), north(x, 1), south(x))
    return x, slope_x, slope_y, rms


def finish_kernel(KC, t_ref, s_ref, u_ref, v_ref, x_ref, ot_ref, os_ref, ou_ref, ov_ref, ox_ref, orms_ref,
                  bufs, plain_sem, chunk_sem):
    plain = [pltpu.make_async_copy(src, dst, plain_sem.at[i])
             for i, (src, dst) in enumerate(((t_ref, ot_ref), (s_ref, os_ref), (x_ref.at[0], ox_ref)))]
    for copy in plain:
        copy.start()
    depth = x_ref[4]
    K = t_ref.shape[0]
    chunks = []
    for c in range(K // KC):
        levels = pl.ds(c * KC, KC)
        for f, (src, dst) in enumerate(((u_ref, ou_ref), (v_ref, ov_ref))):
            slope = x_ref[1 + f]
            for k in range(c * KC, (c + 1) * KC):
                bufs[f, k] = jnp.where(depth > k + 0.5, src[k] - slope, 0.0)
            copy = pltpu.make_async_copy(bufs.at[f, levels], dst.at[levels], chunk_sem.at[f, c])
            copy.start()
            chunks.append(copy)
    orms_ref[0] = jnp.max(x_ref[3])
    for copy in plain + chunks:
        copy.wait()


def per_device(n_lon, n_lat, temp, salt, u, v, num, sea, thick, eta, drive):
    K, NI, NJ = temp.shape
    KC = 8 if K % 8 == 0 else K
    NC = K // KC
    n_half = n_lon * n_lat // 2
    vmem = pl.BlockSpec(memory_space=pltpu.VMEM)
    smem = pl.BlockSpec(memory_space=pltpu.SMEM)
    anywhere = pl.BlockSpec(memory_space=pltpu.HBM)
    big = jax.ShapeDtypeStruct((K, NI, NJ), F32)
    kept = pltpu.VMEM((K, NI, NJ), F32)
    flat = jax.ShapeDtypeStruct((NI, NJ), F32)
    one = jax.ShapeDtypeStruct((1,), F32)
    args = (temp, salt, u, v, num, sea, thick, eta, drive)
    sides = pltpu.VMEM((NC, 6 * KC, NJ), F32)
    tile = pltpu.VMEM((NI, NJ), F32)
    parts = pl.pallas_call(
        functools.partial(step_kernel, n_lon, n_lat, KC),
        out_shape=(kept, kept, kept, kept, pltpu.VMEM((5, NI, NJ), F32)),
        in_specs=[anywhere] * 9,
        out_specs=(vmem,) * 5,
        scratch_shapes=[(pltpu.SMEM if a.ndim == 1 else pltpu.VMEM)(a.shape, a.dtype) for a in args] + [
            sides, sides, tile, tile,
            pltpu.VMEM((2, NI, NJ), F32), pltpu.VMEM((2, NI, NJ), F32),
            sides, sides, tile, tile,
            pltpu.VMEM((6, 2, NI, NJ), F32), pltpu.VMEM((8, max(KC, 2 * NI), NJ), F32),
            pltpu.VMEM((2, n_half, EARLY, NI, NJ), F32), pltpu.VMEM((2, n_half, LATE, NI, NJ), F32),
            pltpu.VMEM((3, n_lat, n_lon * NI, NJ), F32),
            pltpu.SemaphoreType.DMA((9,)),
            pltpu.SemaphoreType.DMA((8,)), pltpu.SemaphoreType.DMA((8,)),
            pltpu.SemaphoreType.DMA((2, NC)), pltpu.SemaphoreType.DMA((2, NC)),
            pltpu.SemaphoreType.DMA((4,)), pltpu.SemaphoreType.DMA((4,)),
        ],
        compiler_params=pltpu.CompilerParams(
            collective_id=0, has_side_effects=True),
        name="step",
    )(*args)
    outs = pl.pallas_call(
        functools.partial(finish_kernel, KC),
        out_shape=(big, big, big, big, flat, one),
        in_specs=[vmem] * 5,
        out_specs=(anywhere,) * 5 + (smem,),
        scratch_shapes=[pltpu.VMEM((2, K, NI, NJ), F32), pltpu.SemaphoreType.DMA((3,)),
                        pltpu.SemaphoreType.DMA((2, NC))],
        name="finish",
    )(*[pltpu.with_memory_space_constraint(part, pltpu.VMEM) for part in parts])
    return outs[:5] + (outs[5].reshape(()),)


def solution(mesh):
    n_lon, n_lat = mesh.shape["lon"], mesh.shape["lat"]
    spec3 = P(None, "lon", "lat")
    spec2 = P("lon", "lat")
    return jax.shard_map(
        functools.partial(per_device, n_lon, n_lat),
        mesh=mesh,
        in_specs=(spec3, spec3, spec3, spec3, spec2, spec2, P(), spec2, spec2),
        out_specs=(spec3, spec3, spec3, spec3, spec2, P()),
        check_vma=False,
    )
```

```python
import functools

import jax
import jax.numpy as jnp
from jax import lax
from jax.experimental import pallas as pl
from jax.experimental.pallas import tpu as pltpu
from jax.sharding import PartitionSpec as P

ITERS = 4
DIFFUSION = 0.15
MIXING = 0.1
EXPANSION = 0.2
CONTRACTION = 0.15
PRESSURE_SCALE = 0.02
CORIOLIS = 0.5
FRICTION = 0.01
DIVERGENCE = 0.3
STORAGE = 0.1
SPECTRUM_LOW = 0.1
SPECTRUM_HIGH = 1.9
GRAVITY = 0.3
EPSILON = 1e-06

MESH = pl.DeviceIdType.MESH
F32 = jnp.float32
SLOT_N, SLOT_NE, SLOT_NW, SLOT_S, SLOT_SE, SLOT_SW = range(6)
EARLY = 3
LATE = 2
TILES = EARLY + LATE + 1


def iota(shape, axis):
    return lax.broadcasted_iota(jnp.int32, shape, axis)


def flip_rows(x):
    n = x.shape[0]
    row = iota(x.shape, 0)
    bit = n // 2
    while bit:
        up = pltpu.roll(x, bit, 0)
        down = pltpu.roll(x, n - bit, 0)
        x = up if 2 * bit == n else jnp.where((row & bit) != 0, up, down)
        bit //= 2
    return x


def flip_lanes(x):
    n = x.shape[1]
    lane = iota(x.shape, 1)
    bit = n // 2
    while bit:
        up = pltpu.roll(x, bit, 1)
        x = up if 2 * bit == n else jnp.where((lane & bit) != 0, up, pltpu.roll(x, n - bit, 1))
        bit //= 2
    return x


def step_kernel(n_lon, n_lat, KC, *refs):
    sources, refs = refs[:9], refs[9:]
    (kept, ox_ref), refs = refs[:2], refs[2:]
    (fields, ints, floats, thick_ref, pack_out, pack_in, edges, slots, rim, side_lap, laps, pressure, tiles, strips,
     rims, sums, held, load_sem, send_sem, chunk_sem, edge_sem, cast_send, cast_recv) = refs
    _, K, NI, NJ = fields.shape
    NC = K // KC
    SIDE = 3 * KC
    BASE = NC * SIDE
    REST = BASE + NI
    t_ref, s_ref, u_ref, v_ref = (fields.at[f] for f in range(4))
    ot_ref, os_ref, ou_ref, ov_ref = (kept.at[f] for f in range(4))
    num_ref, sea_ref, eta_ref, drive_ref = ints.at[0], ints.at[1], floats.at[0], floats.at[1]
    p = lax.axis_index("lon")
    q = lax.axis_index("lat")
    east_dev = lax.rem(p + 1, n_lon)
    west_dev = lax.rem(p + n_lon - 1, n_lon)
    at_pole = q == n_lat - 1
    not_pole = q < n_lat - 1
    not_south = q > 0
    mirror = n_lon - 1 - p
    mirror_ne = lax.rem(2 * n_lon - 2 - p, n_lon)
    mirror_nw = lax.rem(2 * n_lon - p, n_lon)
    ne_remote = jnp.logical_or(not_pole, mirror_ne != p)
    nw_remote = jnp.logical_or(not_pole, mirror_nw != p)
    both_remote = jnp.logical_and(ne_remote, nw_remote)
    one_remote = jnp.logical_not(both_remote)
    ne_self = jnp.logical_and(at_pole, mirror_ne == p)
    nw_self = jnp.logical_and(at_pole, mirror_nw == p)

    barrier = pltpu.get_barrier_semaphore()

    def greet(lon, lat):
        pl.semaphore_signal(barrier, inc=1, device_id={"lon": lon, "lat": lat}, device_id_type=MESH)

    greet(east_dev, q)
    if n_lon > 2:
        greet(west_dev, q)

    def around_lon(first, last, fn):
        def visit(r, carry):
            fn(lax.rem(p + r, n_lon))
            return carry

        if last - first <= 8:
            for r in range(first, last):
                visit(r, 0)
        else:
            lax.fori_loop(first, last, visit, 0)

    @pl.when(at_pole)
    def _():
        around_lon(2, n_lon - 1, lambda lon: greet(lon, q))

    @pl.when(not_south)
    def _():
        around_lon(0, n_lon, lambda lon: greet(lon, q - 1))

    @pl.when(not_pole)
    def _():
        around_lon(0, n_lon, lambda lon: greet(lon, q + 1))

    def load(i, dst, sem):
        pltpu.make_async_copy(sources[i], dst, load_sem.at[sem]).start()

    load(4, num_ref, 1)
    load(5, sea_ref, 1)
    load(7, eta_ref, 1)
    load(8, drive_ref, 1)
    for f in (2, 3, 0, 1):
        load(f, fields.at[f], 0)
    thick_load = pltpu.make_async_copy(sources[6], thick_ref, load_sem.at[2])
    thick_load.start()

    @pl.when(not_pole)
    def _():
        around_lon(2, n_lon - 1, lambda lon: greet(lon, q))

    for lat in range(n_lat):
        @pl.when(jnp.logical_or(q - lat > 1, lat - q > 1))
        def _():
            greet(p, lat)

    def drain(ref, sem):
        pltpu.make_async_copy(ref, ref, sem).wait()

    thick_load.wait()
    drain(fields.at[0, 0:4], load_sem.at[1])
    drain(fields, load_sem.at[0])
    sub = iota((NI, NJ), 0)
    lane = iota((NI, NJ), 1)
    depth = (num_ref[...] * sea_ref[...]).astype(F32)

    row_c = iota((KC, NJ), 0)
    lane_c = iota((KC, NJ), 1)
    thick_c = []
    for c in range(NC):
        h = jnp.zeros((KC, NJ), F32)
        for i in range(KC):
            h = jnp.where(row_c == i, thick_ref[c * KC + i], h)
        thick_c.append(h)

    def wide(row):
        return jnp.broadcast_to(row, (KC, NJ))

    for side, (d1, d2) in enumerate(((NI - 1, NI - 2), (0, 1))):
        own_depth = wide(depth[d1:d1 + 1, :])
        carried = jnp.zeros((KC, NJ), F32)
        for c in range(NC):
            levels = slice(c * KC, (c + 1) * KC)
            row = c * SIDE
            pack_out[side, row:row + KC, :] = u_ref[levels, d1, :]
            pack_out[side, row + KC:row + 2 * KC, :] = v_ref[levels, d1, :]
            t_col, s_col = t_ref[levels, d1, :], s_ref[levels, d1, :]
            wet = own_depth > row_c.astype(F32) + (c * KC + 0.5)
            x = jnp.where(wet, (CONTRACTION * s_col - EXPANSION * t_col) * thick_c[c], 0.0)
            step = 1
            while step < KC:
                x = x + jnp.where(row_c >= step, pltpu.roll(x, step, 0), 0.0)
                step *= 2
            x = x + carried
            pack_out[side, row + 2 * KC:row + 3 * KC, :] = x
            carried = wide(x[KC - 1:KC, :])
            for f, (ref, d) in enumerate(((u_ref, d2), (v_ref, d2))):
                row = REST + (2 + f) * K + c * KC
                pack_out[side, row:row + KC, :] = ref[levels, d, :]
            for f, x in enumerate((t_col, s_col)):
                row = REST + f * K + c * KC
                pack_out[side, row:row + KC, :] = x
        pack_out[side, BASE:REST, :] = jnp.where(sub == 0, depth[d1:d1 + 1, :], depth[d2:d2 + 1, :])

    zero = jnp.zeros((NI, NJ), F32)

    def put(acc, x, source, target):
        moved = pltpu.roll(x, (target - source) % NJ, 1) if source != target else x
        return jnp.where(lane == target, moved, acc)

    n0 = s0 = n1 = s1 = zero
    for f, ref in enumerate((t_ref, s_ref, u_ref, v_ref)):
        for k in range(K):
            x = ref[k]
            target = f * K + k
            n0 = put(n0, x, NJ - 1, target)
            s0 = put(s0, x, 0, target)
            if f >= 2:
                n1 = put(n1, x, NJ - 2, target)
                s1 = put(s1, x, 1, target)
    n1 = put(put(n1, depth, NJ - 1, 0), depth, NJ - 2, 1)
    s1 = put(put(s1, depth, 0, 0), depth, 1, 1)
    npk, spk = edges.at[0], edges.at[1]
    npk[0] = n0
    npk[1] = n1
    spk[0] = s0
    spk[1] = s1

    peers = n_lon + n_lat - 2 + (n_lon - 1) * (not_south.astype(jnp.int32) + not_pole.astype(jnp.int32))
    pl.semaphore_wait(barrier, peers)

    def copy(src, dst, lon, lat, out, into):
        return pltpu.make_async_remote_copy(
            src_ref=src, dst_ref=dst, send_sem=out, recv_sem=into,
            device_id={"lon": lon, "lat": lat}, device_id_type=MESH)

    def edge(src, slot, lon, lat, out, row=None):
        dst = slots.at[slot]
        if slot in (SLOT_NE, SLOT_SE, SLOT_NW, SLOT_SW):
            if row is None:
                row = 0 if slot in (SLOT_NE, SLOT_SE) else NI - 1
            src, dst = src.at[:, row:row + 1, :], dst.at[:, row:row + 1, :]
        into = 0 if slot in (SLOT_N, SLOT_NE, SLOT_NW) else 1
        copy(src, dst, lon, lat, send_sem.at[out], edge_sem.at[into]).start()

    @pl.when(at_pole)
    def _():
        edge(npk, SLOT_N, mirror, q, 2)

    @pl.when(jnp.logical_and(at_pole, mirror_ne != p))
    def _():
        edge(npk, SLOT_NE, mirror_ne, q, 2, NI - 1)

    @pl.when(jnp.logical_and(at_pole, mirror_nw != p))
    def _():
        edge(npk, SLOT_NW, mirror_nw, q, 2, 0)

    @pl.when(not_south)
    def _():
        edge(spk, SLOT_NW, east_dev, q - 1, 1)
        edge(spk, SLOT_NE, west_dev, q - 1, 1)
        edge(spk, SLOT_N, p, q - 1, 1)

    @pl.when(not_pole)
    def _():
        edge(npk, SLOT_SW, east_dev, q + 1, 2)
        edge(npk, SLOT_SE, west_dev, q + 1, 2)
        edge(npk, SLOT_S, p, q + 1, 2)

    def sides(first, rows, sem):
        rows = pl.ds(first, rows)
        copy(pack_out.at[0, rows], pack_in.at[1, rows], east_dev, q, send_sem.at[0], chunk_sem.at[sem]).start()
        copy(pack_out.at[1, rows], pack_in.at[0, rows], west_dev, q, send_sem.at[0], chunk_sem.at[sem]).start()

    sides(BASE, NI, NC)
    for c in range(NC):
        sides(c * SIDE, SIDE, c)

    height = zero
    for k in range(K):
        height = height + jnp.where(depth > k + 0.5, thick_ref[k], 0.0)
    width = NJ // NI
    in_block = lane // width == sub
    parts = ((0, EARLY, EARLY * NI), (EARLY, LATE + 1, LATE * NI + 4))

    def pack_strips(which, sign, *arrays):
        first, count, _ = parts[which]
        south = zero
        north = zero
        for i, x in enumerate(arrays):
            for start in (0, width):
                moved = pltpu.roll(x, start, 1, stride=width, stride_axis=0)
                row = jnp.sum(jnp.where(in_block, moved, 0.0), axis=0, keepdims=True)
                row = jnp.broadcast_to(row, (NI, NJ))
                if start:
                    north = jnp.where(sub == i, row, north)
                else:
                    south = jnp.where(sub == i, row, south)
        north = jnp.where(at_pole, sign * flip_lanes(north), north)
        rows = slice(first, first + count)
        strips[0, rows] = south[:count]
        strips[1, rows] = north[:count]

        @pl.when(at_pole)
        def _():
            rims[0, mirror, rows] = north[:count]

    def cast(which):
        first, _, size = parts[which]
        mine = tiles.at[p, pl.ds(first * NI, size)]
        around_lon(1, n_lon, lambda lon: copy(mine, mine, lon, q, cast_send.at[0], cast_recv.at[which, 0]).start())

    def cast_strips(which):
        first, count, _ = parts[which]
        rows = pl.ds(first, count)

        def send(way, side, slot, lon, lat, out):
            copy(strips.at[way, rows], rims.at[side, slot, rows], lon, lat, cast_send.at[out],
                 cast_recv.at[which, 1 + side]).start()

        @pl.when(not_south)
        def _():
            around_lon(0, n_lon, lambda lon: send(0, 0, p, lon, q - 1, 1))

        @pl.when(not_pole)
        def _():
            around_lon(0, n_lon, lambda lon: send(1, 1, p, lon, q + 1, 2))

        @pl.when(at_pole)
        def _():
            around_lon(1, n_lon, lambda lon: send(1, 0, mirror, lon, q, 2))

    def cast_wait(which):
        first, count, size = parts[which]
        rows = pl.ds(first, count)
        drain(tiles.at[pl.ds(0, n_lon - 1), pl.ds(first * NI, size)], cast_recv.at[which, 0])

        @pl.when(at_pole)
        def _():
            drain(rims.at[0, pl.ds(0, n_lon - 1), rows], cast_recv.at[which, 1])

        @pl.when(not_pole)
        def _():
            drain(rims.at[0, pl.ds(0, n_lon), rows], cast_recv.at[which, 1])

        @pl.when(not_south)
        def _():
            drain(rims.at[1, pl.ds(0, n_lon), rows], cast_recv.at[which, 2])

    first_guess = sea_ref[...].astype(F32) * eta_ref[...]
    for i, x in enumerate((height, first_guess, drive_ref[...])):
        tiles[p, i * NI:(i + 1) * NI] = x
    pack_strips(0, 1.0, height, first_guess, drive_ref[...])
    cast(0)
    cast_strips(0)
    level_i = lane - K * (lane // K)
    level_l = level_i.astype(F32) + 0.5
    thick_l = zero
    for k in range(K):
        thick_l = jnp.where(level_i == k, thick_ref[k], thick_l)

    near_e = jnp.where(sub == NI - 1, 0.0, jnp.minimum(depth, pltpu.roll(depth, NI - 1, 0)))
    near_w = jnp.where(sub == 0, 0.0, jnp.minimum(depth, pltpu.roll(depth, 1, 0)))
    near_n = jnp.where(lane == NJ - 1, 0.0, jnp.minimum(depth, pltpu.roll(depth, NJ - 1, 1)))
    near_s = jnp.where(lane == 0, 0.0, jnp.minimum(depth, pltpu.roll(depth, 1, 1)))
    lat_index = (q * NJ + lane).astype(F32)
    coriolis = CORIOLIS * (2.0 * (lat_index + 0.5) / (n_lat * NJ) - 1.0)

    def gate(d, kf, x):
        return jnp.where(d > kf, x, 0.0)

    def inner_lap(x, kf):
        total = gate(near_e, kf, pltpu.roll(x, NI - 1, 0) - x) + gate(near_w, kf, pltpu.roll(x, 1, 0) - x)
        return total + (gate(near_n, kf, pltpu.roll(x, NJ - 1, 1) - x) + gate(near_s, kf, pltpu.roll(x, 1, 1) - x))

    def before_level(k, pc):
        kf = lax.convert_element_type(k, F32) + 0.5
        u, v = u_ref[k], v_ref[k]
        laps[0, k] = inner_lap(u, kf)
        laps[1, k] = inner_lap(v, kf)
        pc = pc + gate(depth, kf, (CONTRACTION * s_ref[k] - EXPANSION * t_ref[k]) * thick_ref[k])
        pressure[k] = pc
        grad_x = gate(near_e, kf, pltpu.roll(pc, NI - 1, 0) - pc) + gate(near_w, kf, pc - pltpu.roll(pc, 1, 0))
        grad_y = gate(near_n, kf, pltpu.roll(pc, NJ - 1, 1) - pc) + gate(near_s, kf, pc - pltpu.roll(pc, 1, 1))
        ou_ref[k] = u + coriolis * v - (0.5 * PRESSURE_SCALE) * grad_x
        ov_ref[k] = v - coriolis * u - (0.5 * PRESSURE_SCALE) * grad_y
        return pc

    def before_chunk(c, pc):
        for i in range(KC):
            pc = before_level(c * KC + i, pc)
        return pc

    lax.fori_loop(0, NC, before_chunk, zero)

    full = pl.ds(0, 2 * NI + 4)

    @pl.when(both_remote)
    def _():
        drain(pack_in.at[0, full], edge_sem.at[0])

    @pl.when(one_remote)
    def _():
        drain(pack_in.at[0, pl.ds(0, 2 * NI + 2)], edge_sem.at[0])

    @pl.when(not_south)
    def _():
        drain(pack_in.at[0, full], edge_sem.at[1])

    sign = jnp.where(lane >= 2 * K, -1.0, 1.0).astype(F32)

    def northern(slot, own):
        out = []
        for i in range(2):
            x = slots[slot, i]
            if own is not None:
                x = jnp.where(own, npk[i], x)
            out.append(jnp.where(at_pole, flip_rows(x) * sign, x))
        return out

    def southern(slot):
        return [jnp.where(not_south, slots[slot, i], 0.0) for i in range(2)]

    pn0, pn1 = northern(SLOT_N, None)
    pne0, pne1 = northern(SLOT_NE, ne_self)
    pnw0, pnw1 = northern(SLOT_NW, nw_self)
    ps0, ps1 = southern(SLOT_S)
    pse0, pse1 = southern(SLOT_SE)
    psw0, psw1 = southern(SLOT_SW)

    def shift_e(x, row):
        return jnp.where(sub == NI - 1, row, pltpu.roll(x, NI - 1, 0))

    def shift_w(x, row):
        return jnp.where(sub == 0, row, pltpu.roll(x, 1, 0))

    def wet_l(d):
        return jnp.where(level_l < d, 1.0, 0.0)

    def spread(x, i):
        return jnp.broadcast_to(x[:, i:i + 1], (NI, NJ))

    def packed_lap(c0, c1, e0, e1, w0, w1, own, own_depth):
        d = spread(c1, 0)
        de = shift_e(d, jnp.broadcast_to(e1[0:1, 0:1], (NI, NJ)))
        dw = shift_w(d, jnp.broadcast_to(w1[NI - 1:NI, 0:1], (NI, NJ)))
        xe = shift_e(c0, jnp.broadcast_to(e0[0:1, :], (NI, NJ)))
        xw = shift_w(c0, jnp.broadcast_to(w0[NI - 1:NI, :], (NI, NJ)))
        total = wet_l(de) * (xe - c0) + wet_l(dw) * (xw - c0)
        total = total + wet_l(spread(c1, 1)) * (c1 - c0) + wet_l(own_depth) * (own - c0)
        return wet_l(d) * total

    def packed_pressure(c0, c1):
        x = (CONTRACTION * pltpu.roll(c0, NJ - K, 1) - EXPANSION * c0) * thick_l * wet_l(spread(c1, 0))
        step = 1
        while step < K:
            x = x + jnp.where(level_i >= step, pltpu.roll(x, step, 1), 0.0)
            step *= 2
        return x

    lap_n = packed_lap(pn0, pn1, pne0, pne1, pnw0, pnw1, n0, spread(depth, NJ - 1))
    lap_s = packed_lap(ps0, ps1, pse0, pse1, psw0, psw1, s0, spread(depth, 0))
    rim[0] = pn0
    rim[1] = ps0
    rim[2] = lap_n
    rim[3] = lap_s
    rim[4] = packed_pressure(pn0, pn1)
    rim[5] = packed_pressure(ps0, ps1)

    drain(pack_in.at[:, BASE:REST], chunk_sem.at[NC])
    base_e = pack_in[0, BASE:BASE + 1, :]
    base_w = pack_in[1, BASE:BASE + 1, :]
    is_w = sub == 0
    is_s = lane == 0
    depth_ew = jnp.where(is_w, base_w, base_e)
    depth_ns = jnp.where(is_s, ps1, pltpu.roll(pn1, NJ - 1, 1))
    on_ew = jnp.logical_or(is_w, sub == NI - 1)
    on_ns = jnp.logical_or(is_s, lane == NJ - 1)
    near_ew = jnp.where(on_ew, jnp.minimum(depth, depth_ew), 0.0)
    near_ns = jnp.where(on_ns, jnp.minimum(depth, depth_ns), 0.0)
    scale_ew = jnp.where(is_w, 0.5 * PRESSURE_SCALE, -0.5 * PRESSURE_SCALE)
    scale_ns = jnp.where(is_s, 0.5 * PRESSURE_SCALE, -0.5 * PRESSURE_SCALE)

    def rim_ns(north, south, k):
        x = pltpu.roll(north, (NJ - 1 - k) % NJ, 1)
        return jnp.where(is_s, pltpu.roll(south, (NJ - k) % NJ, 1), x)

    def side_ew(c, row):
        row = c * SIDE + row
        return jnp.where(is_w, pack_in[1, row:row + 1, :], pack_in[0, row:row + 1, :])

    totals = [zero] * 2
    exports = [zero] * 2
    for c in range(NC):
        drain(pack_in.at[:, c * SIDE:(c + 1) * SIDE], chunk_sem.at[c])
        for i in range(KC):
            k = c * KC + i
            kf = k + 0.5
            h = thick_ref[k]
            pc = pressure[k]
            u_part = ou_ref[k] + scale_ew * gate(near_ew, kf, side_ew(c, 2 * KC + i) - pc)
            v_part = ov_ref[k] + scale_ns * gate(near_ns, kf, rim_ns(rim[4], rim[5], k) - pc)
            for m, (x, part, out) in enumerate(((u_ref[k], u_part, ou_ref), (v_ref[k], v_part, ov_ref))):
                at = (2 + m) * K + k
                lap = laps[m, k] + gate(near_ew, kf, side_ew(c, m * KC + i) - x)
                lap = lap + gate(near_ns, kf, rim_ns(rim[0], rim[1], at) - x)
                edge_lap = gate(near_ew, kf, lap)
                friction = inner_lap(lap, kf) - edge_lap
                friction = friction + gate(near_ns, kf, rim_ns(rim[2], rim[3], at) - lap)
                star = gate(depth, kf, part - FRICTION * friction)
                out[k] = star
                totals[m] = totals[m] + h * star
                exports[m] = exports[m] + h * edge_lap

    tiles[p, EARLY * NI:(EARLY + 1) * NI] = totals[0]
    tiles[p, (EARLY + 1) * NI:(EARLY + 2) * NI] = totals[1]
    exports = [-FRICTION * x for x in exports]
    for m in range(2):
        row = (EARLY + LATE) * NI + 2 * m
        tiles[p, row:row + 1] = exports[m][0:1]
        tiles[p, row + 1:row + 2] = exports[m][NI - 1:]
    cast(1)
    out_rows = zero
    for row, x in ((0, exports[0][0:1]), (1, exports[1][0:1]), (NI - 2, exports[1][NI - 1:]), (NI - 1, exports[0][NI - 1:])):
        out_rows = jnp.where(sub == row, jnp.broadcast_to(x, (NI, NJ)), out_rows)
    pack_strips(1, -1.0, totals[0], totals[1], out_rows)
    cast_strips(1)
    rest = pl.ds(REST, 4 * K)
    copy(pack_out.at[0, rest], pack_in.at[1, rest], east_dev, q, send_sem.at[0], chunk_sem.at[NC + 1]).start()
    copy(pack_out.at[1, rest], pack_in.at[0, rest], west_dev, q, send_sem.at[0], chunk_sem.at[NC + 1]).start()

    cast_wait(0)
    flat = tiles.reshape(n_lon * TILES * NI, NJ)
    flat_rim = rims.reshape(2 * n_lon * NI, NJ)
    lanes = iota((n_lon, NJ), 1)

    def loader(f):
        main = [flat[pl.ds(f * NI + s, n_lon, stride=TILES * NI), :] for s in range(NI)]
        north = flat_rim[pl.ds(f, n_lon, stride=NI), :]
        south = jnp.where(not_south, flat_rim[pl.ds(n_lon * NI + f, n_lon, stride=NI), :], 0.0)
        outer = []
        for s in range(NI):
            x = jnp.where(lanes >= NJ - width, pltpu.roll(south, (NJ - width - width * s) % NJ, 1), 0.0)
            outer.append(jnp.where(lanes < width, pltpu.roll(north, (NJ - width * s) % NJ, 1), x))
        return [main, outer]

    def late_wait():
        cast_wait(1)

    def share(total):
        sums[q] = jnp.broadcast_to(total, (NI, NJ))
        for r in range(1, n_lat):
            lat = lax.rem(q + r, n_lat)
            copy(sums.at[q], sums.at[q], p, lat, cast_send.at[3], cast_recv.at[2, 0]).start()

    x, slope_x, slope_y = surface_solve(loader, late_wait, share, n_lon, K, NI, NJ)
    for i, field in enumerate((x, slope_x, slope_y)):
        for s in range(NI):
            held[i, pl.ds(s, n_lon, stride=NI), :] = field[s]
    block = pl.ds(pl.multiple_of(p * NI, NI), NI)
    ox_ref[0] = held[0, block, :]
    slope_u = GRAVITY * held[1, block, :]
    slope_v = GRAVITY * held[2, block, :]
    drain(pack_in.at[:, rest], chunk_sem.at[NC + 1])
    turned = zero
    for i, row in enumerate((pne0[0:1], pse0[0:1], pnw0[NI - 1:], psw0[NI - 1:])):
        turned = jnp.where(sub == i, jnp.broadcast_to(row, (NI, NJ)), turned)
    turned = flip_lanes(turned)
    after = pltpu.roll(turned, 1, 1)
    corners = ((wide(turned[0:1]), wide(after[1:2])), (wide(turned[2:3]), wide(after[3:4])))
    corner_depths = ((pne1[0:1], pse1[0:1]), (pnw1[NI - 1:], psw1[NI - 1:]))
    side_depths = []
    for side, d1 in enumerate((NI - 1, 0)):
        base = pack_in[side, BASE:REST, :]
        cn1, cs1 = corner_depths[side]
        d = wide(base[0:1, :])
        dn = jnp.where(lane_c == NJ - 1, jnp.broadcast_to(cn1[:, 0:1], (KC, NJ)), pltpu.roll(d, NJ - 1, 1))
        ds = jnp.where(lane_c == 0, jnp.broadcast_to(cs1[:, 0:1], (KC, NJ)), pltpu.roll(d, 1, 1))
        own = wide(depth[d1:d1 + 1, :])
        side_depths.append([jnp.minimum(d, o) for o in (wide(base[1:2, :]), own, dn, ds)])

    for c in range(NC):
        level_c = row_c.astype(F32) + (c * KC + 0.5)

        def part(d, x):
            return jnp.where(level_c < d, x, 0.0)

        for side in range(2):
            far, own, dn, ds = side_depths[side]
            cn0, cs0 = corners[side]
            for m in range(2):
                row = c * SIDE + m * KC
                outer = REST + (2 + m) * K + c * KC
                x = pack_in[side, row:row + KC, :]
                at = (2 + m) * K + c * KC
                cn = pltpu.roll(cn0, at, 1, stride=1, stride_axis=0)
                cs = pltpu.roll(cs0, at, 1, stride=1, stride_axis=0)
                xn = jnp.where(lane_c == NJ - 1, cn, pltpu.roll(x, NJ - 1, 1))
                xs = jnp.where(lane_c == 0, cs, pltpu.roll(x, 1, 1))
                total = part(far, pack_in[side, outer:outer + KC, :] - x)
                total = total + part(own, pack_out[side, row:row + KC, :] - x)
                side_lap[c, 2 * side + m] = total + (part(dn, xn - x) + part(ds, xs - x))

    both_e = jnp.minimum(depth, shift_e(depth, base_e))
    both_w = jnp.minimum(depth, shift_w(depth, base_w))
    both_n = jnp.where(lane == NJ - 1, near_ns, near_n)
    both_s = jnp.where(is_s, near_ns, near_s)

    def shift_n(x, packed, source):
        return jnp.where(lane == NJ - 1, pltpu.roll(packed, NJ - 1 - source, 1), pltpu.roll(x, NJ - 1, 1))

    def shift_s(x, packed, source):
        return jnp.where(lane == 0, pltpu.roll(packed, lax.rem(NJ - source, NJ), 1), pltpu.roll(x, 1, 1))

    def around(c, inner, ref, f):
        k = c * KC + inner
        x = ref[k]
        row = pl.ds(c * SIDE + (f - 2) * KC + inner if f >= 2 else REST + f * K + k, 1)
        return (x, shift_e(x, pack_in[0, row, :]), shift_w(x, pack_in[1, row, :]),
                shift_n(x, rim[0], f * K + k), shift_s(x, rim[1], f * K + k))

    def tracers(c, i, carry):
        inner = pl.ds(i, 1)
        k = c * KC + i
        flux_t, flux_s = carry
        kf = lax.convert_element_type(k, F32) + 0.5
        h = thick_ref[k]
        nxt = jnp.minimum(k + 1, K - 1)
        h_next = thick_ref[nxt]
        hv = jnp.full((NI, NJ), h, F32)
        inv_space = 1.0 / (0.5 * (hv + h_next))
        inv_h = MIXING / hv

        def wet(d):
            return jnp.where(d > kf, 1.0, 0.0)

        mc = wet(depth)
        me, mw, mn, ms = wet(both_e), wet(both_w), wet(both_n), wet(both_s)
        below = jnp.where(jnp.logical_and(depth > kf + 1.0, k < K - 1), inv_space, 0.0)
        t = around(c, i, t_ref, 0)
        s = around(c, i, s_ref, 1)
        u0, ue, uw = around(c, i, u_ref, 2)[:3]
        v0, _, _, vn, vs = around(c, i, v_ref, 3)
        ae = 0.25 * me * (u0 + ue)
        aw = 0.25 * mw * (u0 + uw)
        an = 0.25 * mn * (v0 + vn)
        as_ = 0.25 * ms * (v0 + vs)
        ge, gw, gn, gs = DIFFUSION * me, DIFFUSION * mw, DIFFUSION * mn, DIFFUSION * ms

        def tracer(x, ref, flux_above):
            c, e, w, n, so = x
            total = aw * (w + c) - gw * (c - w) - ae * (c + e) + ge * (e - c)
            total = total + as_ * (so + c) - gs * (c - so) - an * (c + n) + gn * (n - c)
            flux = below * (ref[nxt] - c)
            return mc * (c + total + inv_h * (flux - flux_above)), flux

        new_t, flux_t = tracer(t, t_ref, flux_t)
        new_s, flux_s = tracer(s, s_ref, flux_s)
        ot_ref[k] = new_t
        os_ref[k] = new_s
        for m, (out, slope) in enumerate(((ou_ref, slope_u), (ov_ref, slope_v))):
            lap_ew = jnp.where(is_w, side_lap[c, 2 + m, inner, :], side_lap[c, m, inner, :])
            star = out[k] - FRICTION * gate(near_ew, kf, lap_ew)
            out[k] = gate(depth, kf, star - slope)
        return flux_t, flux_s

    def tracer_chunk(c, carry):
        for i in range(KC):
            carry = tracers(c, i, carry)
        return carry

    lax.fori_loop(0, NC, tracer_chunk, (zero,) * 2)

    drain(pack_out, send_sem.at[0])

    @pl.when(not_south)
    def _():
        drain(pack_in.at[0, full], send_sem.at[1])

    @pl.when(both_remote)
    def _():
        drain(pack_in.at[0, full], send_sem.at[2])

    @pl.when(one_remote)
    def _():
        drain(pack_in.at[0, pl.ds(0, 2 * NI + 2)], send_sem.at[2])

    used = pl.ds(0, TILES)
    drain(tiles.at[pl.ds(0, n_lon - 1), pl.ds(0, (EARLY + LATE) * NI + 4)], cast_send.at[0])

    @pl.when(not_south)
    def _():
        drain(rims.at[0, pl.ds(0, n_lon), used], cast_send.at[1])

    @pl.when(not_pole)
    def _():
        drain(rims.at[0, pl.ds(0, n_lon), used], cast_send.at[2])

    @pl.when(at_pole)
    def _():
        drain(rims.at[0, pl.ds(0, n_lon - 1), used], cast_send.at[2])

    drain(sums.at[pl.ds(0, n_lat - 1)], cast_recv.at[2, 0])
    total = functools.reduce(lambda a, b: a + b, [sums[lat] for lat in range(n_lat)])
    ox_ref[1] = jnp.sqrt(total / (n_lon * NI * n_lat * NJ) + EPSILON)
    drain(sums.at[pl.ds(0, n_lat - 1)], cast_send.at[3])


def surface_solve(load, late_wait, share, n_lon, K, NI, NJ):
    tiles = range(2)
    lines = range(NI)
    lane = iota((n_lon, NJ), 1)

    def every(fn, *arrays):
        return [[fn(*(a[b][s] for a in arrays)) for s in lines] for b in tiles]

    def east(x):
        return [x[b][1:] + [pltpu.roll(x[b][0], n_lon - 1, 0)] for b in tiles]

    def west(x):
        return [[pltpu.roll(x[b][NI - 1], 1, 0)] + x[b][:-1] for b in tiles]

    def joined(x, shift, edge):
        moved = [[pltpu.roll(x[b][s], shift, 1) for s in lines] for b in tiles]
        return [[jnp.where(lane == edge, moved[1 - b][s], moved[b][s]) for s in lines] for b in tiles]

    def north(x):
        return joined(x, NJ - 1, NJ - 1)

    def south(x):
        return joined(x, 1, 0)

    height = load(0)
    scale = lambda a, c: jnp.minimum(a, c) * (1.0 / K)
    w_e = every(scale, height, east(height))
    w_w = every(scale, height, west(height))
    w_n = every(scale, height, north(height))
    w_s = every(scale, height, south(height))
    diag = every(lambda a, b, c, d: STORAGE + a + b + c + d, w_e, w_w, w_n, w_s)

    def apply(x):
        return every(
            lambda dg, c, we, e, ww, w, wn, n, ws, s: dg * c - (we * e + ww * w + wn * n + ws * s),
            diag, x, w_e, east(x), w_w, west(x), w_n, north(x), w_s, south(x))

    middle = NI // 2
    spans = [(s, s - 1, s + 1) for s in range(middle)]
    spans += [(s, s + 1, s - 1) for s in range(NI - 1, middle - 1, -1)]
    pivots, carries, factors = ([[None] * NI for _ in tiles] for _ in range(3))
    joints = []
    for b in tiles:
        for s, before, after in spans:
            back, ahead = (w_w, w_e) if after > s else (w_e, w_w)
            pivot = diag[b][s]
            if s not in (0, NI - 1):
                pivot = pivot + back[b][s] * factors[b][before]
            pivots[b][s] = 1.0 / pivot
            carries[b][s] = back[b][s] * pivots[b][s]
            factors[b][s] = -ahead[b][s] * pivots[b][s]
        joints.append(1.0 / (1.0 - factors[b][middle - 1] * factors[b][middle]))

    def precondition(r):
        out = []
        for b in tiles:
            part = [None] * NI
            for s, before, after in spans:
                part[s] = r[b][s] * pivots[b][s]
                if s not in (0, NI - 1):
                    part[s] = part[s] + carries[b][s] * part[before]
            low, high = part[middle - 1], part[middle]
            part[middle - 1] = (low - factors[b][middle - 1] * high) * joints[b]
            part[middle] = (high - factors[b][middle] * low) * joints[b]
            for s in range(middle - 2, -1, -1):
                part[s] = part[s] - factors[b][s] * part[s + 1]
            for s in range(middle + 1, NI):
                part[s] = part[s] - factors[b][s] * part[s - 1]
            out.append(part)
        return out

    x = load(1)
    drive = load(2)
    start = every(lambda h, d, a: jnp.where(h > 0.0, d, 0.0) - a, height, drive, apply(x))
    late_wait()
    t_u = load(EARLY)
    t_v = load(EARLY + 1)
    inner, outer = load(EARLY + LATE)
    for m, t in enumerate((t_u, t_v)):
        for b, (from_w, from_e) in enumerate(((inner[2 * m], inner[2 * m + 1]), (outer[m], outer[NI - 1 - m]))):
            t[b][NI - 1] = t[b][NI - 1] + pltpu.roll(from_w, n_lon - 1, 0)
            t[b][0] = t[b][0] + pltpu.roll(from_e, 1, 0)
    residual = every(
        lambda h, d, e, w, n, s: d - jnp.where(h > 0.0, 0.5 * DIVERGENCE * ((e - w) + (n - s)), 0.0),
        height, start, east(t_u), west(t_u), north(t_v), south(t_v))
    mid = 0.5 * (SPECTRUM_HIGH + SPECTRUM_LOW)
    half = 0.5 * (SPECTRUM_HIGH - SPECTRUM_LOW)
    ratio = mid / half
    direction = every(lambda a: a / mid, precondition(residual))
    rho = 1.0 / ratio
    for step in range(ITERS):
        x = every(lambda a, b: a + b, x, direction)
        residual = every(lambda a, b: a - b, residual, apply(direction))
        if step + 1 < ITERS:
            rho_next = 1.0 / (2.0 * ratio - rho)
            keep, gain = rho_next * rho, 2.0 * rho_next / half
            direction = every(lambda d, z: keep * d + gain * z, direction, precondition(residual))
            rho = rho_next
    squares = functools.reduce(lambda a, b: a + b, [a * a for a in residual[0]])
    share(jnp.sum(jnp.sum(squares, axis=1, keepdims=True), axis=0, keepdims=True))
    slope_x = every(lambda e, w: 0.5 * (e - w), east(x), west(x))
    slope_y = every(lambda n, s: 0.5 * (n - s), north(x), south(x))
    return x[0], slope_x[0], slope_y[0]


def finish_kernel(kept, x_ref, ot_ref, os_ref, ou_ref, ov_ref, ox_ref, orms_ref, rms, sem):
    for f, target in enumerate((ot_ref, os_ref, ou_ref, ov_ref)):
        pltpu.make_async_copy(kept.at[f], target, sem.at[0]).start()
    surface = pltpu.make_async_copy(x_ref.at[0], ox_ref, sem.at[1])
    surface.start()
    rms[0] = jnp.max(x_ref[1])
    scalar = pltpu.make_async_copy(rms, orms_ref, sem.at[2])
    scalar.start()
    pltpu.make_async_copy(kept, kept, sem.at[0]).wait()
    surface.wait()
    scalar.wait()


def per_device(n_lon, n_lat, *args):
    K, NI, NJ = args[0].shape
    KC = 8 if K % 8 == 0 else K
    NC = K // KC
    vmem = pl.BlockSpec(memory_space=pltpu.VMEM)
    hbm = pl.BlockSpec(memory_space=pltpu.HBM)
    big = jax.ShapeDtypeStruct((K, NI, NJ), F32)
    tile = jax.ShapeDtypeStruct((NI, NJ), F32)
    one = jax.ShapeDtypeStruct((1,), F32)
    pack = pltpu.VMEM((2, 7 * K + NI, NJ), F32)

    def room(*lead):
        return pltpu.VMEM((*lead, NI, NJ), F32)

    parts = pl.pallas_call(
        functools.partial(step_kernel, n_lon, n_lat, KC),
        out_shape=(room(4, K), room(2)),
        in_specs=[hbm] * 9,
        out_specs=(vmem,) * 2,
        scratch_shapes=[
            room(4, K), pltpu.VMEM((2, NI, NJ), jnp.int32), room(2), pltpu.SMEM((K,), F32),
            pack, pack, room(2, 2), room(6, 2), room(6), pltpu.VMEM((NC, 4, KC, NJ), F32),
            room(2, K), room(K), pltpu.VMEM((n_lon, TILES * NI, NJ), F32), room(2), room(2, n_lon), room(n_lat),
            pltpu.VMEM((3, n_lon * NI, NJ), F32),
            pltpu.SemaphoreType.DMA((3,)), pltpu.SemaphoreType.DMA((3,)), pltpu.SemaphoreType.DMA((NC + 2,)),
            pltpu.SemaphoreType.DMA((2,)), pltpu.SemaphoreType.DMA((4,)), pltpu.SemaphoreType.DMA((3, 3)),
        ],
        compiler_params=pltpu.CompilerParams(
            collective_id=0, has_side_effects=True),
        name="step",
    )(*args)
    outs = pl.pallas_call(
        finish_kernel,
        out_shape=(big, big, big, big, tile, one),
        in_specs=[vmem] * 2,
        out_specs=(hbm,) * 6,
        scratch_shapes=[pltpu.SMEM((1,), F32), pltpu.SemaphoreType.DMA((3,))],
        name="finish",
    )(*[pltpu.with_memory_space_constraint(part, pltpu.VMEM) for part in parts])
    return outs[:5] + (outs[5].reshape(()),)


def solution(mesh):
    n_lon, n_lat = mesh.shape["lon"], mesh.shape["lat"]
    spec3 = P(None, "lon", "lat")
    spec2 = P("lon", "lat")
    return jax.shard_map(
        functools.partial(per_device, n_lon, n_lat),
        mesh=mesh,
        in_specs=(spec3, spec3, spec3, spec3, spec2, spec2, P(), spec2, spec2),
        out_specs=(spec3, spec3, spec3, spec3, spec2, P()),
        check_vma=False,
    )
```

```python
import functools

import jax
import jax.numpy as jnp
from jax import lax
from jax.experimental import pallas as pl
from jax.experimental.pallas import tpu as pltpu
from jax.sharding import PartitionSpec as P

ITERS = 4
DIFFUSION = 0.15
MIXING = 0.1
EXPANSION = 0.2
CONTRACTION = 0.15
PRESSURE_SCALE = 0.02
CORIOLIS = 0.5
FRICTION = 0.01
DIVERGENCE = 0.3
STORAGE = 0.1
SPECTRUM_LOW = 0.1
SPECTRUM_HIGH = 1.9
GRAVITY = 0.3
EPSILON = 1e-06

MESH = pl.DeviceIdType.MESH
F32 = jnp.float32
EARLY = 3
LATE = 2
TILES = EARLY + LATE + 1


def iota(shape, axis):
    return lax.broadcasted_iota(jnp.int32, shape, axis)


def flip_rows(x):
    n = x.shape[0]
    row = iota(x.shape, 0)
    bit = n // 2
    while bit:
        up = pltpu.roll(x, bit, 0)
        down = pltpu.roll(x, n - bit, 0)
        x = up if 2 * bit == n else jnp.where((row & bit) != 0, up, down)
        bit //= 2
    return x


def flip_lanes(x):
    n = x.shape[1]
    lane = iota(x.shape, 1)
    bit = n // 2
    while bit:
        up = pltpu.roll(x, bit, 1)
        x = up if 2 * bit == n else jnp.where((lane & bit) != 0, up, pltpu.roll(x, n - bit, 1))
        bit //= 2
    return x


def step_kernel(n_lon, n_lat, KC, *refs):
    sources, refs = refs[:9], refs[9:]
    (kept, ox_ref), refs = refs[:2], refs[2:]
    (fields, ints, floats, thick_ref, pack_out, pack_in, edges, slots, lap_edges, lap_slots, rim, laps, pressure, tiles, strips,
     rims, sums, held, load_sem, send_sem, chunk_sem, edge_sem, cast_send, cast_recv) = refs
    _, K, NI, NJ = fields.shape
    NC = K // KC
    SIDE = 3 * KC
    REST = NI + NC * SIDE
    t_ref, s_ref, u_ref, v_ref = (fields.at[f] for f in range(4))
    ot_ref, os_ref, ou_ref, ov_ref = (kept.at[f] for f in range(4))
    num_ref, sea_ref, eta_ref, drive_ref = ints.at[0], ints.at[1], floats.at[0], floats.at[1]
    p = lax.axis_index("lon")
    q = lax.axis_index("lat")
    east_dev = lax.rem(p + 1, n_lon)
    west_dev = lax.rem(p + n_lon - 1, n_lon)
    at_pole = q == n_lat - 1
    not_pole = q < n_lat - 1
    not_south = q > 0
    mirror = n_lon - 1 - p
    lons = [lax.rem(p + r, n_lon) for r in range(min(n_lon, 8))]

    barrier = pltpu.get_barrier_semaphore()

    def greet(lon, lat):
        pl.semaphore_signal(barrier, inc=1, device_id={"lon": lon, "lat": lat}, device_id_type=MESH)

    greet(east_dev, q)
    if n_lon > 2:
        greet(west_dev, q)

    def around_lon(first, last, fn):
        def visit(r, carry):
            fn(lax.rem(p + r, n_lon))
            return carry

        if n_lon <= 8:
            for lon in lons[first:last]:
                fn(lon)
        else:
            lax.fori_loop(first, last, visit, 0)

    @pl.when(at_pole)
    def _():
        around_lon(2, n_lon - 1, lambda lon: greet(lon, q))

    @pl.when(not_south)
    def _():
        around_lon(0, n_lon, lambda lon: greet(lon, q - 1))

    @pl.when(not_pole)
    def _():
        around_lon(0, n_lon, lambda lon: greet(lon, q + 1))

    def load(i, dst, sem):
        pltpu.make_async_copy(sources[i], dst, load_sem.at[sem]).start()

    load(4, num_ref, 1)
    load(5, sea_ref, 1)
    load(7, eta_ref, 1)
    load(8, drive_ref, 1)
    for f in (2, 3, 0, 1):
        load(f, fields.at[f], 0)
    thick_load = pltpu.make_async_copy(sources[6], thick_ref, load_sem.at[2])
    thick_load.start()

    @pl.when(not_pole)
    def _():
        around_lon(2, n_lon - 1, lambda lon: greet(lon, q))

    for lat in range(n_lat):
        @pl.when(jnp.logical_or(q - lat > 1, lat - q > 1))
        def _():
            greet(p, lat)

    def drain(ref, sem):
        pltpu.make_async_copy(ref, ref, sem).wait()

    thick_load.wait()
    drain(fields.at[0, 0:4], load_sem.at[1])
    drain(fields, load_sem.at[0])
    sub = iota((NI, NJ), 0)
    lane = iota((NI, NJ), 1)
    depth = (num_ref[...] * sea_ref[...]).astype(F32)

    row_c = iota((KC, NJ), 0)
    lane_c = iota((KC, NJ), 1)
    thick_c = []
    for c in range(NC):
        h = jnp.zeros((KC, NJ), F32)
        for i in range(KC):
            h = jnp.where(row_c == i, thick_ref[c * KC + i], h)
        thick_c.append(h)

    def wide(row):
        return jnp.broadcast_to(row, (KC, NJ))

    for side, d1 in enumerate((NI - 1, 0)):
        own_depth = wide(depth[d1:d1 + 1, :])
        carried = jnp.zeros((KC, NJ), F32)
        for c in range(NC):
            levels = slice(c * KC, (c + 1) * KC)
            row = NI + c * SIDE
            pack_out[side, row:row + KC, :] = u_ref[levels, d1, :]
            pack_out[side, row + KC:row + 2 * KC, :] = v_ref[levels, d1, :]
            t_col, s_col = t_ref[levels, d1, :], s_ref[levels, d1, :]
            wet = own_depth > row_c.astype(F32) + (c * KC + 0.5)
            x = jnp.where(wet, (CONTRACTION * s_col - EXPANSION * t_col) * thick_c[c], 0.0)
            step = 1
            while step < KC:
                x = x + jnp.where(row_c >= step, pltpu.roll(x, step, 0), 0.0)
                step *= 2
            x = x + carried
            pack_out[side, row + 2 * KC:row + 3 * KC, :] = x
            carried = wide(x[KC - 1:KC, :])
            for f, x in enumerate((t_col, s_col)):
                row = REST + f * K + c * KC
                pack_out[side, row:row + KC, :] = x
        pack_out[side, 0:NI, :] = jnp.broadcast_to(depth[d1:d1 + 1, :], (NI, NJ))

    zero = jnp.zeros((NI, NJ), F32)

    def put(acc, x, source, target):
        moved = pltpu.roll(x, (target - source) % NJ, 1) if source != target else x
        return jnp.where(lane == target, moved, acc)

    n0 = s0 = zero
    for f, ref in enumerate((t_ref, s_ref, u_ref, v_ref)):
        for k in range(K):
            n0 = put(n0, ref[k], NJ - 1, f * K + k)
            s0 = put(s0, ref[k], 0, f * K + k)
    npk, spk = edges.at[0], edges.at[1]
    npk[0] = n0
    npk[1] = put(zero, depth, NJ - 1, 0)
    spk[0] = s0
    spk[1] = put(zero, depth, 0, 0)

    peers = n_lon + n_lat - 2 + (n_lon - 1) * (not_south.astype(jnp.int32) + not_pole.astype(jnp.int32))
    pl.semaphore_wait(barrier, peers)

    def copy(src, dst, lon, lat, out, into):
        return pltpu.make_async_remote_copy(
            src_ref=src, dst_ref=dst, send_sem=out, recv_sem=into,
            device_id={"lon": lon, "lat": lat}, device_id_type=MESH)

    def meet(pack, slot, sem):
        @pl.when(at_pole)
        def _():
            copy(pack.at[0], slot.at[0], mirror, q, send_sem.at[2], edge_sem.at[sem]).start()

        @pl.when(not_south)
        def _():
            copy(pack.at[1], slot.at[0], p, q - 1, send_sem.at[1], edge_sem.at[sem]).start()

        @pl.when(not_pole)
        def _():
            copy(pack.at[0], slot.at[1], p, q + 1, send_sem.at[2], edge_sem.at[sem + 1]).start()

    def met(slot, sem):
        drain(slot.at[0], edge_sem.at[sem])

        @pl.when(not_south)
        def _():
            drain(slot.at[1], edge_sem.at[sem + 1])

    meet(edges, slots, 0)

    def sides(first, rows, sem):
        rows = pl.ds(first, rows)
        copy(pack_out.at[0, rows], pack_in.at[1, rows], east_dev, q, send_sem.at[0], chunk_sem.at[sem]).start()
        copy(pack_out.at[1, rows], pack_in.at[0, rows], west_dev, q, send_sem.at[0], chunk_sem.at[sem]).start()

    starts = [0] + [NI + c * SIDE for c in range(1, NC + 1)]
    for c in range(NC):
        sides(starts[c], starts[c + 1] - starts[c], c)

    height = zero
    for k in range(K):
        height = height + jnp.where(depth > k + 0.5, thick_ref[k], 0.0)
    width = NJ // NI
    in_block = lane // width == sub
    parts = ((0, EARLY, EARLY * NI), (EARLY, LATE + 3, LATE * NI + 6))

    def pack_strips(which, sign, arrays, rows=()):
        first, count, _ = parts[which]
        given = len(arrays)
        south = zero
        north = zero
        for i, x in enumerate(arrays):
            for start in (0, width):
                moved = pltpu.roll(x, start, 1, stride=width, stride_axis=0)
                row = jnp.sum(jnp.where(in_block, moved, 0.0), axis=0, keepdims=True)
                row = jnp.broadcast_to(row, (NI, NJ))
                if start:
                    north = jnp.where(sub == i, row, north)
                else:
                    south = jnp.where(sub == i, row, south)
        for i, row in enumerate(rows):
            north = jnp.where(sub == given + i, row, north)
            south = jnp.where(sub == given + i, row, south)
        turned = jnp.where(sub >= given, pltpu.roll(north, width, 1), north) if rows else north
        north = jnp.where(at_pole, sign * flip_lanes(turned), north)
        rows = slice(first, first + count)
        strips[0, rows] = south[:count]
        strips[1, rows] = north[:count]

        @pl.when(at_pole)
        def _():
            rims[0, mirror, rows] = north[:count]

    def cast(which):
        first, _, size = parts[which]
        mine = tiles.at[p, pl.ds(first * NI, size)]
        around_lon(1, n_lon, lambda lon: copy(mine, mine, lon, q, cast_send.at[0], cast_recv.at[which, 0]).start())

    def cast_strips(which):
        first, count, _ = parts[which]
        rows = pl.ds(first, count)

        def send(way, side, slot, lon, lat, out):
            copy(strips.at[way, rows], rims.at[side, slot, rows], lon, lat, cast_send.at[out],
                 cast_recv.at[which, 1 + side]).start()

        @pl.when(not_south)
        def _():
            around_lon(0, n_lon, lambda lon: send(0, 0, p, lon, q - 1, 1))

        @pl.when(not_pole)
        def _():
            around_lon(0, n_lon, lambda lon: send(1, 1, p, lon, q + 1, 2))

        @pl.when(at_pole)
        def _():
            around_lon(1, n_lon, lambda lon: send(1, 0, mirror, lon, q, 2))

    def cast_wait(which):
        first, count, size = parts[which]
        rows = pl.ds(first, count)
        drain(tiles.at[pl.ds(0, n_lon - 1), pl.ds(first * NI, size)], cast_recv.at[which, 0])

        @pl.when(at_pole)
        def _():
            drain(rims.at[0, pl.ds(0, n_lon - 1), rows], cast_recv.at[which, 1])

        @pl.when(not_pole)
        def _():
            drain(rims.at[0, pl.ds(0, n_lon), rows], cast_recv.at[which, 1])

        @pl.when(not_south)
        def _():
            drain(rims.at[1, pl.ds(0, n_lon), rows], cast_recv.at[which, 2])

    first_guess = sea_ref[...].astype(F32) * eta_ref[...]
    for i, x in enumerate((height, first_guess, drive_ref[...])):
        tiles[p, i * NI:(i + 1) * NI] = x
    pack_strips(0, 1.0, (height, first_guess, drive_ref[...]))
    cast(0)
    cast_strips(0)
    level_i = lane - K * (lane // K)
    level_l = level_i.astype(F32) + 0.5
    thick_l = zero
    for k in range(K):
        thick_l = jnp.where(level_i == k, thick_ref[k], thick_l)

    near_e = jnp.where(sub == NI - 1, 0.0, jnp.minimum(depth, pltpu.roll(depth, NI - 1, 0)))
    near_w = jnp.where(sub == 0, 0.0, jnp.minimum(depth, pltpu.roll(depth, 1, 0)))
    near_n = jnp.where(lane == NJ - 1, 0.0, jnp.minimum(depth, pltpu.roll(depth, NJ - 1, 1)))
    near_s = jnp.where(lane == 0, 0.0, jnp.minimum(depth, pltpu.roll(depth, 1, 1)))
    lat_index = (q * NJ + lane).astype(F32)
    coriolis = CORIOLIS * (2.0 * (lat_index + 0.5) / (n_lat * NJ) - 1.0)

    def gate(d, kf, x):
        return jnp.where(d > kf, x, 0.0)

    def inner_lap(x, kf):
        total = gate(near_e, kf, pltpu.roll(x, NI - 1, 0) - x) + gate(near_w, kf, pltpu.roll(x, 1, 0) - x)
        return total + (gate(near_n, kf, pltpu.roll(x, NJ - 1, 1) - x) + gate(near_s, kf, pltpu.roll(x, 1, 1) - x))

    def before_level(k, pc):
        kf = lax.convert_element_type(k, F32) + 0.5
        u, v = u_ref[k], v_ref[k]
        laps[0, k] = inner_lap(u, kf)
        laps[1, k] = inner_lap(v, kf)
        pc = pc + gate(depth, kf, (CONTRACTION * s_ref[k] - EXPANSION * t_ref[k]) * thick_ref[k])
        pressure[k] = pc
        grad_x = gate(near_e, kf, pltpu.roll(pc, NI - 1, 0) - pc) + gate(near_w, kf, pc - pltpu.roll(pc, 1, 0))
        grad_y = gate(near_n, kf, pltpu.roll(pc, NJ - 1, 1) - pc) + gate(near_s, kf, pc - pltpu.roll(pc, 1, 1))
        ou_ref[k] = u + coriolis * v - (0.5 * PRESSURE_SCALE) * grad_x
        ov_ref[k] = v - coriolis * u - (0.5 * PRESSURE_SCALE) * grad_y
        return pc

    def before_chunk(c, pc):
        for i in range(KC):
            pc = before_level(c * KC + i, pc)
        return pc

    lax.fori_loop(0, NC, before_chunk, zero)

    met(slots, 0)

    sign = jnp.where(lane >= 2 * K, -1.0, 1.0).astype(F32)

    def arrived(slot, i, fold):
        north = jnp.where(at_pole, flip_rows(slot[0, i]) * fold, slot[0, i])
        return north, jnp.where(not_south, slot[1, i], 0.0)

    pn0, ps0 = arrived(slots, 0, sign)
    pn1, ps1 = arrived(slots, 1, 1.0)

    def shift_e(x, row):
        return jnp.where(sub == NI - 1, row, pltpu.roll(x, NI - 1, 0))

    def shift_w(x, row):
        return jnp.where(sub == 0, row, pltpu.roll(x, 1, 0))

    def wet_l(d):
        return jnp.where(level_l < d, 1.0, 0.0)

    def spread(x, i):
        return jnp.broadcast_to(x[:, i:i + 1], (NI, NJ))

    def packed_pressure(c0, c1):
        x = (CONTRACTION * pltpu.roll(c0, NJ - K, 1) - EXPANSION * c0) * thick_l * wet_l(spread(c1, 0))
        step = 1
        while step < K:
            x = x + jnp.where(level_i >= step, pltpu.roll(x, step, 1), 0.0)
            step *= 2
        return x

    rim[0] = pn0
    rim[1] = ps0
    rim[2] = packed_pressure(pn0, pn1)
    rim[3] = packed_pressure(ps0, ps1)

    drain(pack_in.at[:, 0:starts[1]], chunk_sem.at[0])
    base_e = pack_in[0, 0:1, :]
    base_w = pack_in[1, 0:1, :]
    is_w = sub == 0
    is_s = lane == 0
    depth_ew = jnp.where(is_w, base_w, base_e)
    depth_ns = jnp.where(is_s, ps1, pltpu.roll(pn1, NJ - 1, 1))
    on_ew = jnp.logical_or(is_w, sub == NI - 1)
    on_ns = jnp.logical_or(is_s, lane == NJ - 1)
    near_ew = jnp.where(on_ew, jnp.minimum(depth, depth_ew), 0.0)
    near_ns = jnp.where(on_ns, jnp.minimum(depth, depth_ns), 0.0)
    scale_ew = jnp.where(is_w, 0.5 * PRESSURE_SCALE, -0.5 * PRESSURE_SCALE)
    scale_ns = jnp.where(is_s, 0.5 * PRESSURE_SCALE, -0.5 * PRESSURE_SCALE)

    def rim_ns(north, south, k):
        x = pltpu.roll(north, (NJ - 1 - k) % NJ, 1)
        return jnp.where(is_s, pltpu.roll(south, (NJ - k) % NJ, 1), x)

    def side_ew(c, row):
        row = NI + c * SIDE + row
        return jnp.where(is_w, pack_in[1, row:row + 1, :], pack_in[0, row:row + 1, :])

    totals = [zero] * 2
    exports = [zero] * 2
    exports_ns = [zero] * 2
    for c in range(NC):
        if c:
            drain(pack_in.at[:, starts[c]:starts[c + 1]], chunk_sem.at[c])
        for i in range(KC):
            k = c * KC + i
            kf = k + 0.5
            h = thick_ref[k]
            pc = pressure[k]
            u_part = ou_ref[k] + scale_ew * gate(near_ew, kf, side_ew(c, 2 * KC + i) - pc)
            v_part = ov_ref[k] + scale_ns * gate(near_ns, kf, rim_ns(rim[2], rim[3], k) - pc)
            for m, (x, part, out) in enumerate(((u_ref[k], u_part, ou_ref), (v_ref[k], v_part, ov_ref))):
                at = (2 + m) * K + k
                lap = laps[m, k] + gate(near_ew, kf, side_ew(c, m * KC + i) - x)
                lap = lap + gate(near_ns, kf, rim_ns(rim[0], rim[1], at) - x)
                edge_lap = gate(near_ew, kf, lap)
                laps[m, k] = lap
                edge_ns = gate(near_ns, kf, lap)
                friction = inner_lap(lap, kf) - edge_lap - edge_ns
                star = gate(depth, kf, part - FRICTION * friction)
                out[k] = star
                totals[m] = totals[m] + h * star
                exports[m] = exports[m] + h * edge_lap
                exports_ns[m] = exports_ns[m] + h * edge_ns

    tiles[p, EARLY * NI:(EARLY + 1) * NI] = totals[0]
    tiles[p, (EARLY + 1) * NI:(EARLY + 2) * NI] = totals[1]
    exports = [-FRICTION * x for x in exports]
    for m in range(2):
        row = (EARLY + LATE) * NI + 2 * m
        tiles[p, row:row + 1] = exports[m][0:1]
        tiles[p, row + 1:row + 2] = exports[m][NI - 1:]
    out_rows = zero
    for row, x in ((0, exports[0][0:1]), (1, exports[1][0:1]), (NI - 2, exports[1][NI - 1:]), (NI - 1, exports[0][NI - 1:])):
        out_rows = jnp.where(sub == row, jnp.broadcast_to(x, (NI, NJ)), out_rows)
    ns_rows = []
    for m, x in enumerate(exports_ns):
        x = -FRICTION * x
        x = jnp.where(lane == 0, pltpu.roll(x, 1, 1), jnp.where(lane == NJ - 1, pltpu.roll(x, NJ - 1, 1), 0.0))
        x = jnp.sum(pltpu.roll(x, 0, 1, stride=width, stride_axis=0), axis=0, keepdims=True)
        row = (EARLY + LATE) * NI + 4 + m
        tiles[p, row:row + 1] = x
        ns_rows.append(jnp.broadcast_to(x, (NI, NJ)))
    pack_strips(1, -1.0, (*totals, out_rows), ns_rows)
    cast_strips(1)
    cast(1)

    for side, d in enumerate((NI - 1, 0)):
        for m in range(2):
            row = REST + (2 + m) * K
            pack_out[side, row:row + K, :] = laps[m, :, d, :]
    n2 = s2 = zero
    for m in range(2):
        for k in range(K):
            n2 = put(n2, laps[m, k], NJ - 1, m * K + k)
            s2 = put(s2, laps[m, k], 0, m * K + k)
    lap_edges[0] = n2
    lap_edges[1] = s2

    cast_wait(0)
    flat = tiles.reshape(n_lon * TILES * NI, NJ)
    flat_rim = rims.reshape(2 * n_lon * NI, NJ)
    lanes = iota((n_lon, NJ), 1)

    def loader(f):
        main = [flat[pl.ds(f * NI + s, n_lon, stride=TILES * NI), :] for s in range(NI)]
        north = flat_rim[pl.ds(f, n_lon, stride=NI), :]
        south = jnp.where(not_south, flat_rim[pl.ds(n_lon * NI + f, n_lon, stride=NI), :], 0.0)
        outer = []
        for s in range(NI):
            x = jnp.where(lanes >= NJ - width, pltpu.roll(south, (NJ - width - width * s) % NJ, 1), 0.0)
            outer.append(jnp.where(lanes < width, pltpu.roll(north, (NJ - width * s) % NJ, 1), x))
        return [main, outer]

    def rim_rows(f):
        north = flat_rim[pl.ds(f, n_lon, stride=NI), :]
        south = jnp.where(not_south, flat_rim[pl.ds(n_lon * NI + f, n_lon, stride=NI), :], 0.0)
        return jnp.where(lanes % width == width - 1, north, south)

    def share(total):
        sums[q] = jnp.broadcast_to(total, (NI, NJ))
        for r in range(1, n_lat):
            lat = lax.rem(q + r, n_lat)
            copy(sums.at[q], sums.at[q], p, lat, cast_send.at[3], cast_recv.at[2, 0]).start()

    rest = pl.ds(REST, 4 * K)

    def late_wait():
        meet(lap_edges, lap_slots, 2)
        sides(REST, 4 * K, NC)
        cast_wait(1)

    x, slope_x, slope_y = surface_solve(loader, rim_rows, late_wait, share, n_lon, K, NI, NJ)
    for i, field in enumerate((x, slope_x, slope_y)):
        for s in range(NI):
            held[i, pl.ds(s, n_lon, stride=NI), :] = field[s]
    block = pl.ds(pl.multiple_of(p * NI, NI), NI)
    ox_ref[0] = held[0, block, :]
    slope_u = GRAVITY * held[1, block, :]
    slope_v = GRAVITY * held[2, block, :]
    drain(pack_in.at[:, rest], chunk_sem.at[NC])
    met(lap_slots, 2)
    rim[4] = jnp.where(at_pole, -flip_rows(lap_slots[0]), lap_slots[0])
    rim[5] = jnp.where(not_south, lap_slots[1], 0.0)
    both_e = jnp.minimum(depth, shift_e(depth, base_e))
    both_w = jnp.minimum(depth, shift_w(depth, base_w))
    both_n = jnp.where(lane == NJ - 1, near_ns, near_n)
    both_s = jnp.where(is_s, near_ns, near_s)

    def shift_n(x, packed, source):
        return jnp.where(lane == NJ - 1, pltpu.roll(packed, NJ - 1 - source, 1), pltpu.roll(x, NJ - 1, 1))

    def shift_s(x, packed, source):
        return jnp.where(lane == 0, pltpu.roll(packed, lax.rem(NJ - source, NJ), 1), pltpu.roll(x, 1, 1))

    def around(c, inner, ref, f):
        k = c * KC + inner
        x = ref[k]
        row = pl.ds(NI + c * SIDE + (f - 2) * KC + inner if f >= 2 else REST + f * K + k, 1)
        return (x, shift_e(x, pack_in[0, row, :]), shift_w(x, pack_in[1, row, :]),
                shift_n(x, rim[0], f * K + k), shift_s(x, rim[1], f * K + k))

    def tracers(c, i, carry):
        k = c * KC + i
        flux_t, flux_s = carry
        kf = lax.convert_element_type(k, F32) + 0.5
        h = thick_ref[k]
        nxt = jnp.minimum(k + 1, K - 1)
        h_next = thick_ref[nxt]
        hv = jnp.full((NI, NJ), h, F32)
        inv_space = 1.0 / (0.5 * (hv + h_next))
        inv_h = MIXING / hv

        def wet(d):
            return jnp.where(d > kf, 1.0, 0.0)

        mc = wet(depth)
        me, mw, mn, ms = wet(both_e), wet(both_w), wet(both_n), wet(both_s)
        below = jnp.where(jnp.logical_and(depth > kf + 1.0, k < K - 1), inv_space, 0.0)
        t = around(c, i, t_ref, 0)
        s = around(c, i, s_ref, 1)
        u0, ue, uw = around(c, i, u_ref, 2)[:3]
        v0, _, _, vn, vs = around(c, i, v_ref, 3)
        ae = 0.25 * me * (u0 + ue)
        aw = 0.25 * mw * (u0 + uw)
        an = 0.25 * mn * (v0 + vn)
        as_ = 0.25 * ms * (v0 + vs)
        ge, gw, gn, gs = DIFFUSION * me, DIFFUSION * mw, DIFFUSION * mn, DIFFUSION * ms

        def tracer(x, ref, flux_above):
            c, e, w, n, so = x
            total = aw * (w + c) - gw * (c - w) - ae * (c + e) + ge * (e - c)
            total = total + as_ * (so + c) - gs * (c - so) - an * (c + n) + gn * (n - c)
            flux = below * (ref[nxt] - c)
            return mc * (c + total + inv_h * (flux - flux_above)), flux

        new_t, flux_t = tracer(t, t_ref, flux_t)
        new_s, flux_s = tracer(s, s_ref, flux_s)
        ot_ref[k] = new_t
        os_ref[k] = new_s
        for m, (out, slope) in enumerate(((ou_ref, slope_u), (ov_ref, slope_v))):
            row = pl.ds(REST + (2 + m) * K + k, 1)
            lap_ew = jnp.where(is_w, pack_in[1, row, :], pack_in[0, row, :])
            at = m * K + k
            lap_n = pltpu.roll(rim[4], NJ - 1 - at, 1)
            lap_ns = jnp.where(is_s, pltpu.roll(rim[5], lax.rem(NJ - at, NJ), 1), lap_n)
            star = out[k] - FRICTION * (gate(near_ew, kf, lap_ew) + gate(near_ns, kf, lap_ns))
            out[k] = gate(depth, kf, star - slope)
        return flux_t, flux_s

    def tracer_chunk(c, carry):
        for i in range(KC):
            carry = tracers(c, i, carry)
        return carry

    lax.fori_loop(0, NC, tracer_chunk, (zero,) * 2)

    drain(pack_out, send_sem.at[0])

    sent = pack_in.at[0, 0:3 * NI]

    @pl.when(not_south)
    def _():
        drain(sent, send_sem.at[1])

    drain(sent, send_sem.at[2])

    used = pl.ds(0, NI)
    drain(tiles.at[pl.ds(0, n_lon - 1), pl.ds(0, (EARLY + LATE) * NI + 6)], cast_send.at[0])

    @pl.when(not_south)
    def _():
        drain(rims.at[0, pl.ds(0, n_lon), used], cast_send.at[1])

    @pl.when(not_pole)
    def _():
        drain(rims.at[0, pl.ds(0, n_lon), used], cast_send.at[2])

    @pl.when(at_pole)
    def _():
        drain(rims.at[0, pl.ds(0, n_lon - 1), used], cast_send.at[2])

    drain(sums.at[pl.ds(0, n_lat - 1)], cast_recv.at[2, 0])
    total = functools.reduce(lambda a, b: a + b, [sums[lat] for lat in range(n_lat)])
    ox_ref[1] = jnp.sqrt(total / (n_lon * NI * n_lat * NJ) + EPSILON)
    drain(sums.at[pl.ds(0, n_lat - 1)], cast_send.at[3])


def surface_solve(load, rim_rows, late_wait, share, n_lon, K, NI, NJ):
    width = NJ // NI
    tiles = range(2)
    lines = range(NI)
    lane = iota((n_lon, NJ), 1)
    edge = jnp.logical_or(lane == 0, lane == NJ - 1)

    def every(fn, *arrays):
        return [[fn(*(a[b][s] for a in arrays)) for s in lines] for b in tiles]

    def east(x):
        return [x[b][1:] + [pltpu.roll(x[b][0], n_lon - 1, 0)] for b in tiles]

    def west(x):
        return [[pltpu.roll(x[b][NI - 1], 1, 0)] + x[b][:-1] for b in tiles]

    def joined(x, shift, edge):
        moved = [[pltpu.roll(x[b][s], shift, 1) for s in lines] for b in tiles]
        return [[jnp.where(lane == edge, moved[1 - b][s], moved[b][s]) for s in lines] for b in tiles]

    def north(x):
        return joined(x, NJ - 1, NJ - 1)

    def south(x):
        return joined(x, 1, 0)

    height = load(0)
    scale = lambda a, c: jnp.minimum(a, c) * (1.0 / K)
    w_e = every(scale, height, east(height))
    w_w = every(scale, height, west(height))
    w_n = every(scale, height, north(height))
    w_s = every(scale, height, south(height))
    diag = every(lambda a, b, c, d: STORAGE + a + b + c + d, w_e, w_w, w_n, w_s)

    def apply(x):
        return every(
            lambda dg, c, we, e, ww, w, wn, n, ws, s: dg * c - (we * e + ww * w + wn * n + ws * s),
            diag, x, w_e, east(x), w_w, west(x), w_n, north(x), w_s, south(x))

    middle = NI // 2
    spans = [(s, s - 1, s + 1) for s in range(middle)]
    spans += [(s, s + 1, s - 1) for s in range(NI - 1, middle - 1, -1)]
    pivots, carries, factors = ([[None] * NI for _ in tiles] for _ in range(3))
    joints = []
    for b in tiles:
        for s, before, after in spans:
            back, ahead = (w_w, w_e) if after > s else (w_e, w_w)
            pivot = diag[b][s]
            if s not in (0, NI - 1):
                pivot = pivot + back[b][s] * factors[b][before]
            pivots[b][s] = 1.0 / pivot
            carries[b][s] = back[b][s] * pivots[b][s]
            factors[b][s] = -ahead[b][s] * pivots[b][s]
        joints.append(1.0 / (1.0 - factors[b][middle - 1] * factors[b][middle]))

    def precondition(r):
        out = []
        for b in tiles:
            part = [None] * NI
            for s, before, after in spans:
                part[s] = r[b][s] * pivots[b][s]
                if s not in (0, NI - 1):
                    part[s] = part[s] + carries[b][s] * part[before]
            low, high = part[middle - 1], part[middle]
            part[middle - 1] = (low - factors[b][middle - 1] * high) * joints[b]
            part[middle] = (high - factors[b][middle] * low) * joints[b]
            for s in range(middle - 2, -1, -1):
                part[s] = part[s] - factors[b][s] * part[s + 1]
            for s in range(middle + 1, NI):
                part[s] = part[s] - factors[b][s] * part[s - 1]
            out.append(part)
        return out

    x = load(1)
    drive = load(2)
    start = every(lambda h, d, a: jnp.where(h > 0.0, d, 0.0) - a, height, drive, apply(x))
    late_wait()
    t_u = load(EARLY)
    t_v = load(EARLY + 1)
    inner, outer = load(EARLY + LATE)
    for m, t in enumerate((t_u, t_v)):
        for b, (from_w, from_e) in enumerate(((inner[2 * m], inner[2 * m + 1]), (outer[m], outer[NI - 1 - m]))):
            t[b][NI - 1] = t[b][NI - 1] + pltpu.roll(from_w, n_lon - 1, 0)
            t[b][0] = t[b][0] + pltpu.roll(from_e, 1, 0)
        own, beyond = inner[4 + m], rim_rows(EARLY + LATE + 1 + m)
        for s in lines:
            for b, row in ((0, beyond), (1, own)):
                moved = pltpu.roll(row, (NJ - width * s) % NJ, 1) if s else row
                t[b][s] = t[b][s] + jnp.where(edge, moved, 0.0)
    residual = every(
        lambda h, d, e, w, n, s: d - jnp.where(h > 0.0, 0.5 * DIVERGENCE * ((e - w) + (n - s)), 0.0),
        height, start, east(t_u), west(t_u), north(t_v), south(t_v))
    mid = 0.5 * (SPECTRUM_HIGH + SPECTRUM_LOW)
    half = 0.5 * (SPECTRUM_HIGH - SPECTRUM_LOW)
    ratio = mid / half
    direction = every(lambda a: a / mid, precondition(residual))
    rho = 1.0 / ratio
    for step in range(ITERS):
        x = every(lambda a, b: a + b, x, direction)
        residual = every(lambda a, b: a - b, residual, apply(direction))
        if step + 1 < ITERS:
            rho_next = 1.0 / (2.0 * ratio - rho)
            keep, gain = rho_next * rho, 2.0 * rho_next / half
            direction = every(lambda d, z: keep * d + gain * z, direction, precondition(residual))
            rho = rho_next
    squares = functools.reduce(lambda a, b: a + b, [a * a for a in residual[0]])
    share(jnp.sum(jnp.sum(squares, axis=1, keepdims=True), axis=0, keepdims=True))
    slope_x = every(lambda e, w: 0.5 * (e - w), east(x), west(x))
    slope_y = every(lambda n, s: 0.5 * (n - s), north(x), south(x))
    return x[0], slope_x[0], slope_y[0]


def finish_kernel(kept, x_ref, ot_ref, os_ref, ou_ref, ov_ref, ox_ref, orms_ref, rms, sem):
    for f, target in enumerate((ot_ref, os_ref, ou_ref, ov_ref)):
        pltpu.make_async_copy(kept.at[f], target, sem.at[0]).start()
    surface = pltpu.make_async_copy(x_ref.at[0], ox_ref, sem.at[1])
    surface.start()
    rms[0] = jnp.max(x_ref[1])
    scalar = pltpu.make_async_copy(rms, orms_ref, sem.at[2])
    scalar.start()
    pltpu.make_async_copy(kept, kept, sem.at[0]).wait()
    surface.wait()
    scalar.wait()


def per_device(n_lon, n_lat, *args):
    K, NI, NJ = args[0].shape
    KC = 8 if K % 8 == 0 else K
    NC = K // KC
    vmem = pl.BlockSpec(memory_space=pltpu.VMEM)
    hbm = pl.BlockSpec(memory_space=pltpu.HBM)
    big = jax.ShapeDtypeStruct((K, NI, NJ), F32)
    tile = jax.ShapeDtypeStruct((NI, NJ), F32)
    one = jax.ShapeDtypeStruct((1,), F32)
    pack = pltpu.VMEM((2, NI + NC * 3 * KC + 4 * K, NJ), F32)

    def room(*lead):
        return pltpu.VMEM((*lead, NI, NJ), F32)

    parts = pl.pallas_call(
        functools.partial(step_kernel, n_lon, n_lat, KC),
        out_shape=(room(4, K), room(2)),
        in_specs=[hbm] * 9,
        out_specs=(vmem,) * 2,
        scratch_shapes=[
            room(4, K), pltpu.VMEM((2, NI, NJ), jnp.int32), room(2), pltpu.SMEM((K,), F32),
            pack, pack, room(2, 2), room(2, 2), room(2), room(2), room(6),
            room(2, K), room(K), pltpu.VMEM((n_lon, TILES * NI, NJ), F32), room(2), room(2, n_lon), room(n_lat),
            pltpu.VMEM((3, n_lon * NI, NJ), F32),
            pltpu.SemaphoreType.DMA((3,)), pltpu.SemaphoreType.DMA((3,)), pltpu.SemaphoreType.DMA((NC + 1,)),
            pltpu.SemaphoreType.DMA((4,)), pltpu.SemaphoreType.DMA((4,)), pltpu.SemaphoreType.DMA((3, 3)),
        ],
        compiler_params=pltpu.CompilerParams(
            collective_id=0, has_side_effects=True),
        name="step",
    )(*args)
    outs = pl.pallas_call(
        finish_kernel,
        out_shape=(big, big, big, big, tile, one),
        in_specs=[vmem] * 2,
        out_specs=(hbm,) * 6,
        scratch_shapes=[pltpu.SMEM((1,), F32), pltpu.SemaphoreType.DMA((3,))],
        name="finish",
    )(*[pltpu.with_memory_space_constraint(part, pltpu.VMEM) for part in parts])
    return outs[:5] + (outs[5].reshape(()),)


def solution(mesh):
    n_lon, n_lat = mesh.shape["lon"], mesh.shape["lat"]
    spec3 = P(None, "lon", "lat")
    spec2 = P("lon", "lat")
    return jax.shard_map(
        functools.partial(per_device, n_lon, n_lat),
        mesh=mesh,
        in_specs=(spec3, spec3, spec3, spec3, spec2, spec2, P(), spec2, spec2),
        out_specs=(spec3, spec3, spec3, spec3, spec2, P()),
        check_vma=False,
    )
```

```python
import functools

import jax
import jax.numpy as jnp
from jax import lax
from jax.experimental import pallas as pl
from jax.experimental.pallas import tpu as pltpu
from jax.sharding import PartitionSpec as P

ITERS = 4
DIFFUSION = 0.15
MIXING = 0.1
EXPANSION = 0.2
CONTRACTION = 0.15
PRESSURE_SCALE = 0.02
CORIOLIS = 0.5
FRICTION = 0.01
DIVERGENCE = 0.3
STORAGE = 0.1
SPECTRUM_LOW = 0.1
SPECTRUM_HIGH = 1.9
GRAVITY = 0.3
EPSILON = 1e-06

MESH = pl.DeviceIdType.MESH
F32 = jnp.float32
EARLY = 3
LATE = 2
TILES = EARLY + LATE + 1


def iota(shape, axis):
    return lax.broadcasted_iota(jnp.int32, shape, axis)


def flip(x, axis):
    return jnp.take_along_axis(x, x.shape[axis] - 1 - iota(x.shape, axis), axis=axis)


def flip_rows(x):
    return flip(x, 0)


def flip_lanes(x):
    return flip(x, 1)


def step_kernel(n_lon, n_lat, KC, *refs):
    sources, refs = refs[:9], refs[9:]
    (kept, ox_ref), refs = refs[:2], refs[2:]
    (fields, ints, floats, thick_ref, pack_out, pack_in, edges, slots, lap_edges, lap_slots, rim, laps, pressure, tiles, strips,
     rims, sums, held, load_sem, send_sem, chunk_sem, edge_sem, cast_send, cast_recv) = refs
    _, K, NI, NJ = fields.shape
    NC = K // KC
    SIDE = 2 * KC
    REST = NI + NC * SIDE
    t_ref, s_ref, u_ref, v_ref = (fields.at[f] for f in range(4))
    ot_ref, os_ref, ou_ref, ov_ref = (kept.at[f] for f in range(4))
    num_ref, sea_ref, eta_ref, drive_ref = ints.at[0], ints.at[1], floats.at[0], floats.at[1]
    p = lax.axis_index("lon")
    q = lax.axis_index("lat")
    east_dev = lax.rem(p + 1, n_lon)
    west_dev = lax.rem(p + n_lon - 1, n_lon)
    at_pole = q == n_lat - 1
    not_pole = q < n_lat - 1
    not_south = q > 0
    mirror = n_lon - 1 - p
    lons = [lax.rem(p + r, n_lon) for r in range(min(n_lon, 8))]

    barrier = pltpu.get_barrier_semaphore()

    def greet(lon, lat):
        pl.semaphore_signal(barrier, inc=1, device_id={"lon": lon, "lat": lat}, device_id_type=MESH)

    greet(east_dev, q)
    if n_lon > 2:
        greet(west_dev, q)

    def around_lon(first, last, fn):
        def visit(r, carry):
            fn(lax.rem(p + r, n_lon))
            return carry

        if n_lon <= 8:
            for lon in lons[first:last]:
                fn(lon)
        else:
            lax.fori_loop(first, last, visit, 0)

    @pl.when(at_pole)
    def _():
        around_lon(2, n_lon - 1, lambda lon: greet(lon, q))

    @pl.when(not_south)
    def _():
        around_lon(0, n_lon, lambda lon: greet(lon, q - 1))

    @pl.when(not_pole)
    def _():
        around_lon(0, n_lon, lambda lon: greet(lon, q + 1))

    def load(i, dst, sem):
        pltpu.make_async_copy(sources[i], dst, load_sem.at[sem]).start()

    load(4, num_ref, 1)
    load(5, sea_ref, 1)
    load(7, eta_ref, 1)
    load(8, drive_ref, 1)
    for f in (2, 3, 0, 1):
        load(f, fields.at[f], 0)
    thick_load = pltpu.make_async_copy(sources[6], thick_ref, load_sem.at[2])
    thick_load.start()

    @pl.when(not_pole)
    def _():
        around_lon(2, n_lon - 1, lambda lon: greet(lon, q))

    for lat in range(n_lat):
        @pl.when(jnp.logical_or(q - lat > 1, lat - q > 1))
        def _():
            greet(p, lat)

    def drain(ref, sem):
        pltpu.make_async_copy(ref, ref, sem).wait()

    thick_load.wait()
    drain(fields.at[0, 0:4], load_sem.at[1])
    drain(fields, load_sem.at[0])
    sub = iota((NI, NJ), 0)
    lane = iota((NI, NJ), 1)
    depth = (num_ref[...] * sea_ref[...]).astype(F32)

    for side, d1 in enumerate((NI - 1, 0)):
        for c in range(NC):
            levels = slice(c * KC, (c + 1) * KC)
            for m, ref in enumerate((u_ref, v_ref)):
                row = NI + c * SIDE + m * KC
                pack_out[side, row:row + KC, :] = ref[levels, d1, :]
        for m, ref in enumerate((t_ref, s_ref)):
            row = REST + m * K
            pack_out[side, row:row + K, :] = ref[:, d1, :]
        pack_out[side, 0:NI, :] = jnp.broadcast_to(depth[d1:d1 + 1, :], (NI, NJ))

    zero = jnp.zeros((NI, NJ), F32)

    def put(acc, x, source, target):
        moved = pltpu.roll(x, (target - source) % NJ, 1) if source != target else x
        return jnp.where(lane == target, moved, acc)

    n0 = s0 = zero
    for f, ref in enumerate((t_ref, s_ref, u_ref, v_ref)):
        for k in range(K):
            n0 = put(n0, ref[k], NJ - 1, f * K + k)
            s0 = put(s0, ref[k], 0, f * K + k)
    npk, spk = edges.at[0], edges.at[1]
    npk[0] = n0
    npk[1] = put(zero, depth, NJ - 1, 0)
    spk[0] = s0
    spk[1] = put(zero, depth, 0, 0)

    peers = n_lon + n_lat - 2 + (n_lon - 1) * (not_south.astype(jnp.int32) + not_pole.astype(jnp.int32))
    pl.semaphore_wait(barrier, peers)

    def copy(src, dst, lon, lat, out, into):
        return pltpu.make_async_remote_copy(
            src_ref=src, dst_ref=dst, send_sem=out, recv_sem=into,
            device_id={"lon": lon, "lat": lat}, device_id_type=MESH)

    def meet(pack, slot, sem):
        @pl.when(at_pole)
        def _():
            copy(pack.at[0], slot.at[0], mirror, q, send_sem.at[2], edge_sem.at[sem]).start()

        @pl.when(not_south)
        def _():
            copy(pack.at[1], slot.at[0], p, q - 1, send_sem.at[1], edge_sem.at[sem]).start()

        @pl.when(not_pole)
        def _():
            copy(pack.at[0], slot.at[1], p, q + 1, send_sem.at[2], edge_sem.at[sem + 1]).start()

    def met(slot, sem):
        drain(slot.at[0], edge_sem.at[sem])

        @pl.when(not_south)
        def _():
            drain(slot.at[1], edge_sem.at[sem + 1])

    meet(edges, slots, 0)

    def sides(first, rows, sem):
        rows = pl.ds(first, rows)
        copy(pack_out.at[0, rows], pack_in.at[1, rows], east_dev, q, send_sem.at[0], chunk_sem.at[sem]).start()
        copy(pack_out.at[1, rows], pack_in.at[0, rows], west_dev, q, send_sem.at[0], chunk_sem.at[sem]).start()

    starts = [0] + [NI + c * SIDE for c in range(1, NC + 1)]
    for c in range(NC):
        sides(starts[c], starts[c + 1] - starts[c], c)

    height = zero
    for k in range(K):
        height = height + jnp.where(depth > k + 0.5, thick_ref[k], 0.0)
    width = NJ // NI
    in_block = lane // width == sub
    parts = ((0, EARLY, EARLY * NI), (EARLY, LATE + 3, LATE * NI + 6))

    def pack_strips(which, sign, arrays, rows=()):
        first, count, _ = parts[which]
        given = len(arrays)
        south = zero
        north = zero
        for i, x in enumerate(arrays):
            for start in (0, width):
                moved = pltpu.roll(x, start, 1, stride=width, stride_axis=0)
                row = jnp.sum(jnp.where(in_block, moved, 0.0), axis=0, keepdims=True)
                row = jnp.broadcast_to(row, (NI, NJ))
                if start:
                    north = jnp.where(sub == i, row, north)
                else:
                    south = jnp.where(sub == i, row, south)
        for i, row in enumerate(rows):
            north = jnp.where(sub == given + i, row, north)
            south = jnp.where(sub == given + i, row, south)
        turned = jnp.where(sub >= given, pltpu.roll(north, width, 1), north) if rows else north
        north = jnp.where(at_pole, sign * flip_lanes(turned), north)
        rows = slice(first, first + count)
        strips[0, rows] = south[:count]
        strips[1, rows] = north[:count]

        @pl.when(at_pole)
        def _():
            rims[0, mirror, rows] = north[:count]

    def cast(which):
        first, _, size = parts[which]
        mine = tiles.at[p, pl.ds(first * NI, size)]
        around_lon(1, n_lon, lambda lon: copy(mine, mine, lon, q, cast_send.at[0], cast_recv.at[which, 0]).start())

    def cast_strips(which):
        first, count, _ = parts[which]
        rows = pl.ds(first, count)

        def send(way, side, slot, lon, lat, out):
            copy(strips.at[way, rows], rims.at[side, slot, rows], lon, lat, cast_send.at[out],
                 cast_recv.at[which, 1 + side]).start()

        @pl.when(not_south)
        def _():
            around_lon(0, n_lon, lambda lon: send(0, 0, p, lon, q - 1, 1))

        pole = at_pole.astype(jnp.int32)
        side, lat = 1 - pole, q + 1 - pole
        slot = jnp.where(at_pole, mirror, p)

        @pl.when(not_pole)
        def _():
            around_lon(0, 1, lambda lon: send(1, 1, p, lon, q + 1, 2))

        around_lon(1, n_lon, lambda lon: send(1, side, slot, lon, lat, 2))

    def cast_wait(which):
        first, count, size = parts[which]
        rows = pl.ds(first, count)
        drain(tiles.at[pl.ds(0, n_lon - 1), pl.ds(first * NI, size)], cast_recv.at[which, 0])

        @pl.when(at_pole)
        def _():
            drain(rims.at[0, pl.ds(0, n_lon - 1), rows], cast_recv.at[which, 1])

        @pl.when(not_pole)
        def _():
            drain(rims.at[0, pl.ds(0, n_lon), rows], cast_recv.at[which, 1])

        @pl.when(not_south)
        def _():
            drain(rims.at[1, pl.ds(0, n_lon), rows], cast_recv.at[which, 2])

    first_guess = sea_ref[...].astype(F32) * eta_ref[...]
    for i, x in enumerate((height, first_guess, drive_ref[...])):
        tiles[p, i * NI:(i + 1) * NI] = x
    pack_strips(0, 1.0, (height, first_guess, drive_ref[...]))

    near_e = jnp.where(sub == NI - 1, 0.0, jnp.minimum(depth, pltpu.roll(depth, NI - 1, 0)))
    near_w = jnp.where(sub == 0, 0.0, jnp.minimum(depth, pltpu.roll(depth, 1, 0)))
    near_n = jnp.where(lane == NJ - 1, 0.0, jnp.minimum(depth, pltpu.roll(depth, NJ - 1, 1)))
    near_s = jnp.where(lane == 0, 0.0, jnp.minimum(depth, pltpu.roll(depth, 1, 1)))
    lat_index = (q * NJ + lane).astype(F32)
    coriolis = CORIOLIS * (2.0 * (lat_index + 0.5) / (n_lat * NJ) - 1.0)

    def gate(d, kf, x):
        return jnp.where(d > kf, x, 0.0)

    def inner_lap(x, kf):
        total = gate(near_e, kf, pltpu.roll(x, NI - 1, 0) - x) + gate(near_w, kf, pltpu.roll(x, 1, 0) - x)
        return total + (gate(near_n, kf, pltpu.roll(x, NJ - 1, 1) - x) + gate(near_s, kf, pltpu.roll(x, 1, 1) - x))

    def before_level(k, pc):
        kf = lax.convert_element_type(k, F32) + 0.5
        u, v = u_ref[k], v_ref[k]
        laps[0, k] = inner_lap(u, kf)
        laps[1, k] = inner_lap(v, kf)
        pc = pc + gate(depth, kf, (CONTRACTION * s_ref[k] - EXPANSION * t_ref[k]) * thick_ref[k])
        pressure[k] = pc
        grad_x = gate(near_e, kf, pltpu.roll(pc, NI - 1, 0) - pc) + gate(near_w, kf, pc - pltpu.roll(pc, 1, 0))
        grad_y = gate(near_n, kf, pltpu.roll(pc, NJ - 1, 1) - pc) + gate(near_s, kf, pc - pltpu.roll(pc, 1, 1))
        ou_ref[k] = u + coriolis * v - (0.5 * PRESSURE_SCALE) * grad_x
        ov_ref[k] = v - coriolis * u - (0.5 * PRESSURE_SCALE) * grad_y
        return pc

    def before_chunk(c, pc):
        for i in range(KC):
            pc = before_level(c * KC + i, pc)
        return pc

    lax.fori_loop(0, NC, before_chunk, zero)

    cast(0)
    cast_strips(0)
    sides(REST, 2 * K, NC)
    met(slots, 0)

    sign = jnp.where(lane >= 2 * K, -1.0, 1.0).astype(F32)

    def arrived(slot, i, fold):
        north = jnp.where(at_pole, flip_rows(slot[0, i]) * fold, slot[0, i])
        return north, jnp.where(not_south, slot[1, i], 0.0)

    pn0, ps0 = arrived(slots, 0, sign)
    pn1, ps1 = arrived(slots, 1, 1.0)

    def shift_e(x, row):
        return jnp.where(sub == NI - 1, row, pltpu.roll(x, NI - 1, 0))

    def shift_w(x, row):
        return jnp.where(sub == 0, row, pltpu.roll(x, 1, 0))

    rim[0] = pn0
    rim[1] = ps0

    drain(pack_in.at[:, 0:starts[1]], chunk_sem.at[0])
    base_e = pack_in[0, 0:1, :]
    base_w = pack_in[1, 0:1, :]
    is_w = sub == 0
    is_s = lane == 0
    depth_ew = jnp.where(is_w, base_w, base_e)
    depth_ns = jnp.where(is_s, ps1, pltpu.roll(pn1, NJ - 1, 1))
    on_ew = jnp.logical_or(is_w, sub == NI - 1)
    on_ns = jnp.logical_or(is_s, lane == NJ - 1)
    near_ew = jnp.where(on_ew, jnp.minimum(depth, depth_ew), 0.0)
    near_ns = jnp.where(on_ns, jnp.minimum(depth, depth_ns), 0.0)
    scale_ew = jnp.where(is_w, 0.5 * PRESSURE_SCALE, -0.5 * PRESSURE_SCALE)
    scale_ns = jnp.where(is_s, 0.5 * PRESSURE_SCALE, -0.5 * PRESSURE_SCALE)

    def rim_ns(north, south, k):
        x = pltpu.roll(north, (NJ - 1 - k) % NJ, 1)
        return jnp.where(is_s, pltpu.roll(south, (NJ - k) % NJ, 1), x)

    def side_ew(c, row):
        row = NI + c * SIDE + row
        return jnp.where(is_w, pack_in[1, row:row + 1, :], pack_in[0, row:row + 1, :])

    totals = [zero] * 2
    exports = [zero] * 2
    exports_ns = [zero] * 2
    for c in range(NC):
        if c:
            drain(pack_in.at[:, starts[c]:starts[c + 1]], chunk_sem.at[c])
        for i in range(KC):
            k = c * KC + i
            kf = k + 0.5
            h = thick_ref[k]
            pc = pressure[k]
            push_ew = scale_ew * gate(near_ew, kf, pc)
            push_ns = scale_ns * gate(near_ns, kf, pc)
            exports[0] = exports[0] - h * push_ew
            exports_ns[1] = exports_ns[1] - h * push_ns
            u_part = ou_ref[k] - push_ew
            v_part = ov_ref[k] - push_ns
            for m, (x, part, out) in enumerate(((u_ref[k], u_part, ou_ref), (v_ref[k], v_part, ov_ref))):
                at = (2 + m) * K + k
                lap = laps[m, k] + gate(near_ew, kf, side_ew(c, m * KC + i) - x)
                lap = lap + gate(near_ns, kf, rim_ns(rim[0], rim[1], at) - x)
                edge_lap = FRICTION * gate(near_ew, kf, lap)
                laps[m, k] = lap
                edge_ns = FRICTION * gate(near_ns, kf, lap)
                star = gate(depth, kf, part - FRICTION * inner_lap(lap, kf) + (edge_lap + edge_ns))
                out[k] = star
                totals[m] = totals[m] + h * star
                exports[m] = exports[m] - h * edge_lap
                exports_ns[m] = exports_ns[m] - h * edge_ns

    tiles[p, EARLY * NI:(EARLY + 1) * NI] = totals[0]
    tiles[p, (EARLY + 1) * NI:(EARLY + 2) * NI] = totals[1]
    for m in range(2):
        row = (EARLY + LATE) * NI + 2 * m
        tiles[p, row:row + 1] = exports[m][0:1]
        tiles[p, row + 1:row + 2] = exports[m][NI - 1:]
    out_rows = zero
    for row, x in ((0, exports[0][0:1]), (1, exports[1][0:1]), (NI - 2, exports[1][NI - 1:]), (NI - 1, exports[0][NI - 1:])):
        out_rows = jnp.where(sub == row, jnp.broadcast_to(x, (NI, NJ)), out_rows)
    ns_rows = []
    for m, x in enumerate(exports_ns):
        x = jnp.where(lane == 0, pltpu.roll(x, 1, 1), jnp.where(lane == NJ - 1, pltpu.roll(x, NJ - 1, 1), 0.0))
        x = jnp.sum(pltpu.roll(x, 0, 1, stride=width, stride_axis=0), axis=0, keepdims=True)
        row = (EARLY + LATE) * NI + 4 + m
        tiles[p, row:row + 1] = x
        ns_rows.append(jnp.broadcast_to(x, (NI, NJ)))
    pack_strips(1, -1.0, (*totals, out_rows), ns_rows)
    cast(1)
    cast_strips(1)

    levels_out = (pressure, laps.at[0], laps.at[1])
    for side, d in enumerate((NI - 1, 0)):
        for m, x in enumerate(levels_out):
            row = REST + (2 + m) * K
            pack_out[side, row:row + K, :] = x[:, d, :]
    n2 = s2 = zero
    for m, x in enumerate(levels_out):
        for k in range(K):
            n2 = put(n2, x[k], NJ - 1, m * K + k)
            s2 = put(s2, x[k], 0, m * K + k)
    lap_edges[0] = n2
    lap_edges[1] = s2
    meet(lap_edges, lap_slots, 2)
    sides(REST + 2 * K, 3 * K, NC + 1)

    cast_wait(0)
    flat = tiles.reshape(n_lon * TILES * NI, NJ)
    flat_rim = rims.reshape(2 * n_lon * NI, NJ)
    lanes = iota((n_lon, NJ), 1)

    def loader(f):
        main = [flat[pl.ds(f * NI + s, n_lon, stride=TILES * NI), :] for s in range(NI)]
        north = flat_rim[pl.ds(f, n_lon, stride=NI), :]
        south = jnp.where(not_south, flat_rim[pl.ds(n_lon * NI + f, n_lon, stride=NI), :], 0.0)
        outer = []
        for s in range(NI):
            x = jnp.where(lanes >= NJ - width, pltpu.roll(south, (NJ - width - width * s) % NJ, 1), 0.0)
            outer.append(jnp.where(lanes < width, pltpu.roll(north, (NJ - width * s) % NJ, 1), x))
        return [main, outer]

    def rim_rows(f):
        north = flat_rim[pl.ds(f, n_lon, stride=NI), :]
        south = jnp.where(not_south, flat_rim[pl.ds(n_lon * NI + f, n_lon, stride=NI), :], 0.0)
        return jnp.where(lanes % width == width - 1, north, south)

    def share(total):
        sums[q] = jnp.broadcast_to(total, (NI, NJ))
        for r in range(1, n_lat):
            lat = lax.rem(q + r, n_lat)
            copy(sums.at[q], sums.at[q], p, lat, cast_send.at[3], cast_recv.at[2, 0]).start()


    def late_wait():
        cast_wait(1)

    x, slope_x, slope_y = surface_solve(loader, rim_rows, late_wait, share, n_lon, K, NI, NJ)
    for i, field in enumerate((x, slope_x, slope_y)):
        for s in range(NI):
            held[i, pl.ds(s, n_lon, stride=NI), :] = field[s]
    block = pl.ds(pl.multiple_of(p * NI, NI), NI)
    ox_ref[0] = held[0, block, :]
    slope_u = GRAVITY * held[1, block, :]
    slope_v = GRAVITY * held[2, block, :]
    drain(pack_in.at[:, REST:REST + 2 * K], chunk_sem.at[NC])
    drain(pack_in.at[:, REST + 2 * K:], chunk_sem.at[NC + 1])
    met(lap_slots, 2)
    fold = jnp.where(lane < K, 1.0, -1.0)
    rim[2] = jnp.where(at_pole, flip_rows(lap_slots[0]) * fold, lap_slots[0])
    rim[3] = jnp.where(not_south, lap_slots[1], 0.0)
    both_e = jnp.minimum(depth, shift_e(depth, base_e))
    both_w = jnp.minimum(depth, shift_w(depth, base_w))
    both_n = jnp.where(lane == NJ - 1, near_ns, near_n)
    both_s = jnp.where(is_s, near_ns, near_s)

    def shift_n(x, packed, source):
        return jnp.where(lane == NJ - 1, pltpu.roll(packed, NJ - 1 - source, 1), pltpu.roll(x, NJ - 1, 1))

    def shift_s(x, packed, source):
        return jnp.where(lane == 0, pltpu.roll(packed, lax.rem(NJ - source, NJ), 1), pltpu.roll(x, 1, 1))

    def around(c, inner, ref, f):
        k = c * KC + inner
        x = ref[k]
        row = pl.ds(NI + c * SIDE + (f - 2) * KC + inner if f >= 2 else REST + f * K + k, 1)
        return (x, shift_e(x, pack_in[0, row, :]), shift_w(x, pack_in[1, row, :]),
                shift_n(x, rim[0], f * K + k), shift_s(x, rim[1], f * K + k))

    def beyond_ew(f, k):
        row = pl.ds(REST + f * K + k, 1)
        return jnp.where(is_w, pack_in[1, row, :], pack_in[0, row, :])

    def beyond_ns(f, k):
        at = f * K + k
        north = pltpu.roll(rim[2], NJ - 1 - at, 1)
        return jnp.where(is_s, pltpu.roll(rim[3], lax.rem(NJ - at, NJ), 1), north)

    def tracers(c, i, carry):
        k = c * KC + i
        flux_t, flux_s = carry
        kf = lax.convert_element_type(k, F32) + 0.5
        h = thick_ref[k]
        nxt = jnp.minimum(k + 1, K - 1)
        h_next = thick_ref[nxt]
        hv = jnp.full((NI, NJ), h, F32)
        inv_space = 1.0 / (0.5 * (hv + h_next))
        inv_h = MIXING / hv

        def wet(d):
            return jnp.where(d > kf, 1.0, 0.0)

        mc = wet(depth)
        me, mw, mn, ms = wet(both_e), wet(both_w), wet(both_n), wet(both_s)
        below = jnp.where(jnp.logical_and(depth > kf + 1.0, k < K - 1), inv_space, 0.0)
        t = around(c, i, t_ref, 0)
        s = around(c, i, s_ref, 1)
        u0, ue, uw = around(c, i, u_ref, 2)[:3]
        v0, _, _, vn, vs = around(c, i, v_ref, 3)
        ae = 0.25 * me * (u0 + ue)
        aw = 0.25 * mw * (u0 + uw)
        an = 0.25 * mn * (v0 + vn)
        as_ = 0.25 * ms * (v0 + vs)
        ge, gw, gn, gs = DIFFUSION * me, DIFFUSION * mw, DIFFUSION * mn, DIFFUSION * ms

        def tracer(x, ref, flux_above):
            c, e, w, n, so = x
            total = aw * (w + c) - gw * (c - w) - ae * (c + e) + ge * (e - c)
            total = total + as_ * (so + c) - gs * (c - so) - an * (c + n) + gn * (n - c)
            flux = below * (ref[nxt] - c)
            return mc * (c + total + inv_h * (flux - flux_above)), flux

        new_t, flux_t = tracer(t, t_ref, flux_t)
        new_s, flux_s = tracer(s, s_ref, flux_s)
        ot_ref[k] = new_t
        os_ref[k] = new_s
        for m, (out, slope) in enumerate(((ou_ref, slope_u), (ov_ref, slope_v))):
            lap_ew, lap_ns = beyond_ew(3 + m, k), beyond_ns(1 + m, k)
            push = -FRICTION * (gate(near_ew, kf, lap_ew) + gate(near_ns, kf, lap_ns))
            if m == 0:
                push = push + scale_ew * gate(near_ew, kf, beyond_ew(2, k))
            else:
                push = push + scale_ns * gate(near_ns, kf, beyond_ns(0, k))
            star = out[k] + push
            out[k] = gate(depth, kf, star - slope)
        return flux_t, flux_s

    def tracer_chunk(c, carry):
        for i in range(KC):
            carry = tracers(c, i, carry)
        return carry

    lax.fori_loop(0, NC, tracer_chunk, (zero,) * 2)

    drain(pack_out, send_sem.at[0])

    sent = pack_in.at[0, 0:3 * NI]

    @pl.when(not_south)
    def _():
        drain(sent, send_sem.at[1])

    drain(sent, send_sem.at[2])

    used = pl.ds(0, NI)
    drain(tiles.at[pl.ds(0, n_lon - 1), pl.ds(0, (EARLY + LATE) * NI + 6)], cast_send.at[0])

    @pl.when(not_south)
    def _():
        drain(rims.at[0, pl.ds(0, n_lon), used], cast_send.at[1])

    @pl.when(not_pole)
    def _():
        drain(rims.at[0, pl.ds(0, n_lon), used], cast_send.at[2])

    @pl.when(at_pole)
    def _():
        drain(rims.at[0, pl.ds(0, n_lon - 1), used], cast_send.at[2])

    drain(sums.at[pl.ds(0, n_lat - 1)], cast_recv.at[2, 0])
    total = functools.reduce(lambda a, b: a + b, [sums[lat] for lat in range(n_lat)])
    ox_ref[1] = jnp.sqrt(total / (n_lon * NI * n_lat * NJ) + EPSILON)
    drain(sums.at[pl.ds(0, n_lat - 1)], cast_send.at[3])


def surface_solve(load, rim_rows, late_wait, share, n_lon, K, NI, NJ):
    width = NJ // NI
    tiles = range(2)
    lines = range(NI)
    lane = iota((n_lon, NJ), 1)
    edge = jnp.logical_or(lane == 0, lane == NJ - 1)

    def every(fn, *arrays):
        return [[fn(*(a[b][s] for a in arrays)) for s in lines] for b in tiles]

    def east(x):
        return [x[b][1:] + [pltpu.roll(x[b][0], n_lon - 1, 0)] for b in tiles]

    def west(x):
        return [[pltpu.roll(x[b][NI - 1], 1, 0)] + x[b][:-1] for b in tiles]

    def joined(x, shift, edge):
        moved = [[pltpu.roll(x[b][s], shift, 1) for s in lines] for b in tiles]
        return [[jnp.where(lane == edge, moved[1 - b][s], moved[b][s]) for s in lines] for b in tiles]

    def north(x):
        return joined(x, NJ - 1, NJ - 1)

    def south(x):
        return joined(x, 1, 0)

    height = load(0)
    scale = lambda a, c: jnp.minimum(a, c) * (1.0 / K)
    w_e = every(scale, height, east(height))
    w_w = every(scale, height, west(height))
    w_n = every(scale, height, north(height))
    w_s = every(scale, height, south(height))
    diag = every(lambda a, b, c, d: STORAGE + a + b + c + d, w_e, w_w, w_n, w_s)

    def apply(x):
        return every(
            lambda dg, c, we, e, ww, w, wn, n, ws, s: dg * c - (we * e + ww * w + wn * n + ws * s),
            diag, x, w_e, east(x), w_w, west(x), w_n, north(x), w_s, south(x))

    middle = NI // 2
    spans = [(s, s - 1, s + 1) for s in range(middle)]
    spans += [(s, s + 1, s - 1) for s in range(NI - 1, middle - 1, -1)]
    pivots, carries, factors = ([[None] * NI for _ in tiles] for _ in range(3))
    joints = []
    for b in tiles:
        for s, before, after in spans:
            back, ahead = (w_w, w_e) if after > s else (w_e, w_w)
            pivot = diag[b][s]
            if s not in (0, NI - 1):
                pivot = pivot + back[b][s] * factors[b][before]
            pivots[b][s] = 1.0 / pivot
            carries[b][s] = back[b][s] * pivots[b][s]
            factors[b][s] = -ahead[b][s] * pivots[b][s]
        joints.append(1.0 / (1.0 - factors[b][middle - 1] * factors[b][middle]))

    def precondition(r):
        out = []
        for b in tiles:
            part = [None] * NI
            for s, before, after in spans:
                part[s] = r[b][s] * pivots[b][s]
                if s not in (0, NI - 1):
                    part[s] = part[s] + carries[b][s] * part[before]
            low, high = part[middle - 1], part[middle]
            part[middle - 1] = (low - factors[b][middle - 1] * high) * joints[b]
            part[middle] = (high - factors[b][middle] * low) * joints[b]
            for s in range(middle - 2, -1, -1):
                part[s] = part[s] - factors[b][s] * part[s + 1]
            for s in range(middle + 1, NI):
                part[s] = part[s] - factors[b][s] * part[s - 1]
            out.append(part)
        return out

    x = load(1)
    drive = load(2)
    start = every(lambda h, d, a: jnp.where(h > 0.0, d, 0.0) - a, height, drive, apply(x))
    late_wait()
    t_u = load(EARLY)
    t_v = load(EARLY + 1)
    inner, outer = load(EARLY + LATE)
    for m, t in enumerate((t_u, t_v)):
        for b, (from_w, from_e) in enumerate(((inner[2 * m], inner[2 * m + 1]), (outer[m], outer[NI - 1 - m]))):
            t[b][NI - 1] = t[b][NI - 1] + pltpu.roll(from_w, n_lon - 1, 0)
            t[b][0] = t[b][0] + pltpu.roll(from_e, 1, 0)
        own, beyond = inner[4 + m], rim_rows(EARLY + LATE + 1 + m)
        for s in lines:
            for b, row in ((0, beyond), (1, own)):
                moved = pltpu.roll(row, (NJ - width * s) % NJ, 1) if s else row
                t[b][s] = t[b][s] + jnp.where(edge, moved, 0.0)
    residual = every(
        lambda h, d, e, w, n, s: d - jnp.where(h > 0.0, 0.5 * DIVERGENCE * ((e - w) + (n - s)), 0.0),
        height, start, east(t_u), west(t_u), north(t_v), south(t_v))
    mid = 0.5 * (SPECTRUM_HIGH + SPECTRUM_LOW)
    half = 0.5 * (SPECTRUM_HIGH - SPECTRUM_LOW)
    ratio = mid / half
    direction = every(lambda a: a / mid, precondition(residual))
    rho = 1.0 / ratio
    for step in range(ITERS):
        x = every(lambda a, b: a + b, x, direction)
        residual = every(lambda a, b: a - b, residual, apply(direction))
        if step + 1 < ITERS:
            rho_next = 1.0 / (2.0 * ratio - rho)
            keep, gain = rho_next * rho, 2.0 * rho_next / half
            direction = every(lambda d, z: keep * d + gain * z, direction, precondition(residual))
            rho = rho_next
    squares = functools.reduce(lambda a, b: a + b, [a * a for a in residual[0]])
    share(jnp.sum(jnp.sum(squares, axis=1, keepdims=True), axis=0, keepdims=True))
    slope_x = every(lambda e, w: 0.5 * (e - w), east(x), west(x))
    slope_y = every(lambda n, s: 0.5 * (n - s), north(x), south(x))
    return x[0], slope_x[0], slope_y[0]


def finish_kernel(kept, x_ref, ot_ref, os_ref, ou_ref, ov_ref, ox_ref, orms_ref, rms, sem):
    for f, target in enumerate((ot_ref, os_ref, ou_ref, ov_ref)):
        pltpu.make_async_copy(kept.at[f], target, sem.at[0]).start()
    surface = pltpu.make_async_copy(x_ref.at[0], ox_ref, sem.at[1])
    surface.start()
    rms[0] = jnp.max(x_ref[1])
    scalar = pltpu.make_async_copy(rms, orms_ref, sem.at[2])
    scalar.start()
    pltpu.make_async_copy(kept, kept, sem.at[0]).wait()
    surface.wait()
    scalar.wait()


def per_device(n_lon, n_lat, *args):
    K, NI, NJ = args[0].shape
    KC = 8 if K % 8 == 0 else K
    NC = K // KC
    vmem = pl.BlockSpec(memory_space=pltpu.VMEM)
    hbm = pl.BlockSpec(memory_space=pltpu.HBM)
    big = jax.ShapeDtypeStruct((K, NI, NJ), F32)
    tile = jax.ShapeDtypeStruct((NI, NJ), F32)
    one = jax.ShapeDtypeStruct((1,), F32)
    pack = pltpu.VMEM((2, NI + NC * 2 * KC + 5 * K, NJ), F32)

    def room(*lead):
        return pltpu.VMEM((*lead, NI, NJ), F32)

    parts = pl.pallas_call(
        functools.partial(step_kernel, n_lon, n_lat, KC),
        out_shape=(room(4, K), room(2)),
        in_specs=[hbm] * 9,
        out_specs=(vmem,) * 2,
        scratch_shapes=[
            room(4, K), pltpu.VMEM((2, NI, NJ), jnp.int32), room(2), pltpu.SMEM((K,), F32),
            pack, pack, room(2, 2), room(2, 2), room(2), room(2), room(4),
            room(2, K), room(K), pltpu.VMEM((n_lon, TILES * NI, NJ), F32), room(2), room(2, n_lon), room(n_lat),
            pltpu.VMEM((3, n_lon * NI, NJ), F32),
            pltpu.SemaphoreType.DMA((3,)), pltpu.SemaphoreType.DMA((3,)), pltpu.SemaphoreType.DMA((NC + 2,)),
            pltpu.SemaphoreType.DMA((4,)), pltpu.SemaphoreType.DMA((4,)), pltpu.SemaphoreType.DMA((3, 3)),
        ],
        compiler_params=pltpu.CompilerParams(
            collective_id=0, has_side_effects=True),
        name="step",
    )(*args)
    outs = pl.pallas_call(
        finish_kernel,
        out_shape=(big, big, big, big, tile, one),
        in_specs=[vmem] * 2,
        out_specs=(hbm,) * 6,
        scratch_shapes=[pltpu.SMEM((1,), F32), pltpu.SemaphoreType.DMA((3,))],
        name="finish",
    )(*[pltpu.with_memory_space_constraint(part, pltpu.VMEM) for part in parts])
    return outs[:5] + (outs[5].reshape(()),)


def solution(mesh):
    n_lon, n_lat = mesh.shape["lon"], mesh.shape["lat"]
    spec3 = P(None, "lon", "lat")
    spec2 = P("lon", "lat")
    return jax.shard_map(
        functools.partial(per_device, n_lon, n_lat),
        mesh=mesh,
        in_specs=(spec3, spec3, spec3, spec3, spec2, spec2, P(), spec2, spec2),
        out_specs=(spec3, spec3, spec3, spec3, spec2, P()),
        check_vma=False,
    )
```

```python
import functools

import jax
import jax.numpy as jnp
from jax import lax
from jax.experimental import pallas as pl
from jax.experimental.pallas import tpu as pltpu
from jax.sharding import PartitionSpec as P

ITERS = 4
DIFFUSION = 0.15
MIXING = 0.1
EXPANSION = 0.2
CONTRACTION = 0.15
PRESSURE_SCALE = 0.02
CORIOLIS = 0.5
FRICTION = 0.01
DIVERGENCE = 0.3
STORAGE = 0.1
SPECTRUM_LOW = 0.1
SPECTRUM_HIGH = 1.9
GRAVITY = 0.3
EPSILON = 1e-06

MESH = pl.DeviceIdType.MESH
F32 = jnp.float32
EARLY = 3
LATE = 2
TILES = EARLY + LATE + 1


def iota(shape, axis):
    return lax.broadcasted_iota(jnp.int32, shape, axis)


def flip(x, axis):
    return jnp.take_along_axis(x, x.shape[axis] - 1 - iota(x.shape, axis), axis=axis)


def flip_rows(x):
    return flip(x, 0)


def flip_lanes(x):
    return flip(x, 1)


def step_kernel(n_lon, n_lat, KC, *refs):
    sources, refs = refs[:9], refs[9:]
    (kept, ox_ref), refs = refs[:2], refs[2:]
    (fields, ints, floats, thick_ref, pack_out, pack_in, edges, slots, lap_edges, lap_slots, rim, laps, pressure, tiles, strips,
     rims, sums, held, load_sem, send_sem, chunk_sem, edge_sem, cast_send, cast_recv) = refs
    _, K, NI, NJ = fields.shape
    NC = K // KC
    SIDE = 2 * KC
    REST = NI + NC * SIDE
    t_ref, s_ref, u_ref, v_ref = (fields.at[f] for f in range(4))
    ot_ref, os_ref, ou_ref, ov_ref = (kept.at[f] for f in range(4))
    num_ref, sea_ref, eta_ref, drive_ref = ints.at[0], ints.at[1], floats.at[0], floats.at[1]
    p = lax.axis_index("lon")
    q = lax.axis_index("lat")
    east_dev = lax.rem(p + 1, n_lon)
    west_dev = lax.rem(p + n_lon - 1, n_lon)
    at_pole = q == n_lat - 1
    not_pole = q < n_lat - 1
    not_south = q > 0
    mirror = n_lon - 1 - p
    lons = [lax.rem(p + r, n_lon) for r in range(min(n_lon, 8))]

    barrier = pltpu.get_barrier_semaphore()

    def greet(lon, lat):
        pl.semaphore_signal(barrier, inc=1, device_id={"lon": lon, "lat": lat}, device_id_type=MESH)

    greet(east_dev, q)
    if n_lon > 2:
        greet(west_dev, q)

    def around_lon(first, last, fn):
        def visit(r, carry):
            fn(lax.rem(p + r, n_lon))
            return carry

        if n_lon <= 8:
            for lon in lons[first:last]:
                fn(lon)
        else:
            lax.fori_loop(first, last, visit, 0)

    @pl.when(at_pole)
    def _():
        around_lon(2, n_lon - 1, lambda lon: greet(lon, q))

    @pl.when(not_south)
    def _():
        around_lon(0, n_lon, lambda lon: greet(lon, q - 1))

    @pl.when(not_pole)
    def _():
        around_lon(0, n_lon, lambda lon: greet(lon, q + 1))

    def load(i, dst, sem):
        pltpu.make_async_copy(sources[i], dst, load_sem.at[sem]).start()

    load(4, num_ref, 1)
    load(5, sea_ref, 1)
    load(7, eta_ref, 1)
    load(8, drive_ref, 1)
    for f in (2, 3, 0, 1):
        load(f, fields.at[f], 0)
    thick_load = pltpu.make_async_copy(sources[6], thick_ref, load_sem.at[2])
    thick_load.start()

    @pl.when(not_pole)
    def _():
        around_lon(2, n_lon - 1, lambda lon: greet(lon, q))

    for lat in range(n_lat):
        @pl.when(jnp.logical_or(q - lat > 1, lat - q > 1))
        def _():
            greet(p, lat)

    def drain(ref, sem):
        pltpu.make_async_copy(ref, ref, sem).wait()

    thick_load.wait()
    drain(fields.at[0, 0:4], load_sem.at[1])
    drain(fields, load_sem.at[0])
    sub = iota((NI, NJ), 0)
    lane = iota((NI, NJ), 1)
    depth = (num_ref[...] * sea_ref[...]).astype(F32)

    for side, d1 in enumerate((NI - 1, 0)):
        for c in range(NC):
            levels = slice(c * KC, (c + 1) * KC)
            for m, ref in enumerate((u_ref, v_ref)):
                row = NI + c * SIDE + m * KC
                pack_out[side, row:row + KC, :] = ref[levels, d1, :]
        for m, ref in enumerate((t_ref, s_ref)):
            row = REST + m * K
            pack_out[side, row:row + K, :] = ref[:, d1, :]
        pack_out[side, 0:NI, :] = jnp.broadcast_to(depth[d1:d1 + 1, :], (NI, NJ))

    zero = jnp.zeros((NI, NJ), F32)

    def put(acc, x, source, target):
        moved = pltpu.roll(x, (target - source) % NJ, 1) if source != target else x
        return jnp.where(lane == target, moved, acc)

    n0 = s0 = zero
    for f, ref in enumerate((t_ref, s_ref, u_ref, v_ref)):
        for k in range(K):
            n0 = put(n0, ref[k], NJ - 1, f * K + k)
            s0 = put(s0, ref[k], 0, f * K + k)
    npk, spk = edges.at[0], edges.at[1]
    npk[0] = n0
    npk[1] = put(zero, depth, NJ - 1, 0)
    spk[0] = s0
    spk[1] = put(zero, depth, 0, 0)

    peers = n_lon + n_lat - 2 + (n_lon - 1) * (not_south.astype(jnp.int32) + not_pole.astype(jnp.int32))
    pl.semaphore_wait(barrier, peers)

    def copy(src, dst, lon, lat, out, into):
        return pltpu.make_async_remote_copy(
            src_ref=src, dst_ref=dst, send_sem=out, recv_sem=into,
            device_id={"lon": lon, "lat": lat}, device_id_type=MESH)

    def meet(pack, slot, sem):
        @pl.when(at_pole)
        def _():
            copy(pack.at[0], slot.at[0], mirror, q, send_sem.at[2], edge_sem.at[sem]).start()

        @pl.when(not_south)
        def _():
            copy(pack.at[1], slot.at[0], p, q - 1, send_sem.at[1], edge_sem.at[sem]).start()

        @pl.when(not_pole)
        def _():
            copy(pack.at[0], slot.at[1], p, q + 1, send_sem.at[2], edge_sem.at[sem + 1]).start()

    def met(slot, sem):
        drain(slot.at[0], edge_sem.at[sem])

        @pl.when(not_south)
        def _():
            drain(slot.at[1], edge_sem.at[sem + 1])

    meet(edges, slots, 0)

    def sides(first, rows, sem):
        rows = pl.ds(first, rows)
        copy(pack_out.at[1, rows], pack_in.at[0, rows], west_dev, q, send_sem.at[0], chunk_sem.at[sem]).start()
        copy(pack_out.at[0, rows], pack_in.at[1, rows], east_dev, q, send_sem.at[0], chunk_sem.at[sem]).start()

    starts = [0] + [NI + c * SIDE for c in range(1, NC + 1)]
    for c in range(NC):
        sides(starts[c], starts[c + 1] - starts[c], c)

    height = zero
    for k in range(K):
        height = height + jnp.where(depth > k + 0.5, thick_ref[k], 0.0)
    width = NJ // NI
    in_block = lane // width == sub
    parts = ((0, EARLY, EARLY * NI), (EARLY, LATE + 3, LATE * NI + 6))

    def pack_strips(which, sign, arrays, rows=()):
        first, count, _ = parts[which]
        given = len(arrays)
        south = zero
        north = zero
        for i, x in enumerate(arrays):
            for start in (0, width):
                moved = pltpu.roll(x, start, 1, stride=width, stride_axis=0)
                row = jnp.sum(jnp.where(in_block, moved, 0.0), axis=0, keepdims=True)
                row = jnp.broadcast_to(row, (NI, NJ))
                if start:
                    north = jnp.where(sub == i, row, north)
                else:
                    south = jnp.where(sub == i, row, south)
        for i, row in enumerate(rows):
            north = jnp.where(sub == given + i, row, north)
            south = jnp.where(sub == given + i, row, south)
        turned = jnp.where(sub >= given, pltpu.roll(north, width, 1), north) if rows else north
        north = jnp.where(at_pole, sign * flip_lanes(turned), north)
        rows = slice(first, first + count)
        strips[0, rows] = south[:count]
        strips[1, rows] = north[:count]

        @pl.when(at_pole)
        def _():
            rims[0, mirror, rows] = north[:count]

    def each_other(fn):
        def visit(r, carry):
            fn(jnp.where(r <= p, r - 1, r))
            return carry

        if n_lon <= 8:
            for r in range(1, n_lon):
                visit(r, 0)
        else:
            lax.fori_loop(1, n_lon, visit, 0)

    def cast(which):
        first, count, size = parts[which]
        mine = tiles.at[p, pl.ds(first * NI, size)]
        rows = pl.ds(first, count)
        pole = at_pole.astype(jnp.int32)
        side, lat = 1 - pole, q + 1 - pole
        slot = jnp.where(at_pole, mirror, p)

        def send(way, side, slot, lon, lat, out):
            copy(strips.at[way, rows], rims.at[side, slot, rows], lon, lat, cast_send.at[out],
                 cast_recv.at[which, 1 + side]).start()

        @pl.when(not_pole)
        def _():
            send(1, 1, p, p, q + 1, 2)

        @pl.when(not_south)
        def _():
            send(0, 0, p, p, q - 1, 1)

        def to(lon):
            @pl.when(not_south)
            def _():
                send(0, 0, p, lon, q - 1, 1)

            send(1, side, slot, lon, lat, 2)
            copy(mine, mine, lon, q, cast_send.at[0], cast_recv.at[which, 0]).start()

        each_other(to)

    def cast_wait(which):
        first, count, size = parts[which]
        rows = pl.ds(first, count)
        drain(tiles.at[pl.ds(0, n_lon - 1), pl.ds(first * NI, size)], cast_recv.at[which, 0])

        @pl.when(at_pole)
        def _():
            drain(rims.at[0, pl.ds(0, n_lon - 1), rows], cast_recv.at[which, 1])

        @pl.when(not_pole)
        def _():
            drain(rims.at[0, pl.ds(0, n_lon), rows], cast_recv.at[which, 1])

        @pl.when(not_south)
        def _():
            drain(rims.at[1, pl.ds(0, n_lon), rows], cast_recv.at[which, 2])

    first_guess = sea_ref[...].astype(F32) * eta_ref[...]
    for i, x in enumerate((height, first_guess, drive_ref[...])):
        tiles[p, i * NI:(i + 1) * NI] = x
    pack_strips(0, 1.0, (height, first_guess, drive_ref[...]))

    near_e = jnp.where(sub == NI - 1, 0.0, jnp.minimum(depth, pltpu.roll(depth, NI - 1, 0)))
    near_w = jnp.where(sub == 0, 0.0, jnp.minimum(depth, pltpu.roll(depth, 1, 0)))
    near_n = jnp.where(lane == NJ - 1, 0.0, jnp.minimum(depth, pltpu.roll(depth, NJ - 1, 1)))
    near_s = jnp.where(lane == 0, 0.0, jnp.minimum(depth, pltpu.roll(depth, 1, 1)))
    lat_index = (q * NJ + lane).astype(F32)
    coriolis = CORIOLIS * (2.0 * (lat_index + 0.5) / (n_lat * NJ) - 1.0)

    def gate(d, kf, x):
        return jnp.where(d > kf, x, 0.0)

    def inner_lap(x, kf):
        total = gate(near_e, kf, pltpu.roll(x, NI - 1, 0) - x) + gate(near_w, kf, pltpu.roll(x, 1, 0) - x)
        return total + (gate(near_n, kf, pltpu.roll(x, NJ - 1, 1) - x) + gate(near_s, kf, pltpu.roll(x, 1, 1) - x))

    def before_level(k, pc):
        kf = lax.convert_element_type(k, F32) + 0.5
        u, v = u_ref[k], v_ref[k]
        laps[0, k] = inner_lap(u, kf)
        laps[1, k] = inner_lap(v, kf)
        pc = pc + gate(depth, kf, (CONTRACTION * s_ref[k] - EXPANSION * t_ref[k]) * thick_ref[k])
        pressure[k] = pc
        grad_x = gate(near_e, kf, pltpu.roll(pc, NI - 1, 0) - pc) + gate(near_w, kf, pc - pltpu.roll(pc, 1, 0))
        grad_y = gate(near_n, kf, pltpu.roll(pc, NJ - 1, 1) - pc) + gate(near_s, kf, pc - pltpu.roll(pc, 1, 1))
        ou_ref[k] = u + coriolis * v - (0.5 * PRESSURE_SCALE) * grad_x
        ov_ref[k] = v - coriolis * u - (0.5 * PRESSURE_SCALE) * grad_y
        return pc

    def before_chunk(c, pc):
        for i in range(KC):
            pc = before_level(c * KC + i, pc)
        return pc

    lax.fori_loop(0, NC, before_chunk, zero)

    cast(0)
    sides(REST, 2 * K, NC)
    met(slots, 0)

    sign = jnp.where(lane >= 2 * K, -1.0, 1.0).astype(F32)

    def arrived(slot, i, fold):
        north = jnp.where(at_pole, flip_rows(slot[0, i]) * fold, slot[0, i])
        return north, jnp.where(not_south, slot[1, i], 0.0)

    pn0, ps0 = arrived(slots, 0, sign)
    pn1, ps1 = arrived(slots, 1, 1.0)

    def shift_e(x, row):
        return jnp.where(sub == NI - 1, row, pltpu.roll(x, NI - 1, 0))

    def shift_w(x, row):
        return jnp.where(sub == 0, row, pltpu.roll(x, 1, 0))

    rim[0] = pn0
    rim[1] = ps0

    drain(pack_in.at[:, 0:starts[1]], chunk_sem.at[0])
    base_e = pack_in[0, 0:1, :]
    base_w = pack_in[1, 0:1, :]
    is_w = sub == 0
    is_s = lane == 0
    depth_ew = jnp.where(is_w, base_w, base_e)
    depth_ns = jnp.where(is_s, ps1, pltpu.roll(pn1, NJ - 1, 1))
    on_ew = jnp.logical_or(is_w, sub == NI - 1)
    on_ns = jnp.logical_or(is_s, lane == NJ - 1)
    near_ew = jnp.where(on_ew, jnp.minimum(depth, depth_ew), 0.0)
    near_ns = jnp.where(on_ns, jnp.minimum(depth, depth_ns), 0.0)
    scale_ew = jnp.where(is_w, 0.5 * PRESSURE_SCALE, -0.5 * PRESSURE_SCALE)
    scale_ns = jnp.where(is_s, 0.5 * PRESSURE_SCALE, -0.5 * PRESSURE_SCALE)

    def rim_ns(north, south, k):
        x = pltpu.roll(north, (NJ - 1 - k) % NJ, 1)
        return jnp.where(is_s, pltpu.roll(south, (NJ - k) % NJ, 1), x)

    def side_ew(c, row):
        row = NI + c * SIDE + row
        return jnp.where(is_w, pack_in[1, row:row + 1, :], pack_in[0, row:row + 1, :])

    totals = [zero] * 2
    exports = [zero] * 2
    exports_ns = [zero] * 2
    for c in range(NC):
        if c:
            drain(pack_in.at[:, starts[c]:starts[c + 1]], chunk_sem.at[c])
        for i in range(KC):
            k = c * KC + i
            kf = k + 0.5
            h = thick_ref[k]
            pc = pressure[k]
            push_ew = scale_ew * gate(near_ew, kf, pc)
            push_ns = scale_ns * gate(near_ns, kf, pc)
            exports[0] = exports[0] - h * push_ew
            exports_ns[1] = exports_ns[1] - h * push_ns
            u_part = ou_ref[k] - push_ew
            v_part = ov_ref[k] - push_ns
            for m, (x, part, out) in enumerate(((u_ref[k], u_part, ou_ref), (v_ref[k], v_part, ov_ref))):
                at = (2 + m) * K + k
                lap = laps[m, k] + gate(near_ew, kf, side_ew(c, m * KC + i) - x)
                lap = lap + gate(near_ns, kf, rim_ns(rim[0], rim[1], at) - x)
                edge_lap = FRICTION * gate(near_ew, kf, lap)
                laps[m, k] = lap
                edge_ns = FRICTION * gate(near_ns, kf, lap)
                star = gate(depth, kf, part - FRICTION * inner_lap(lap, kf) + (edge_lap + edge_ns))
                out[k] = star
                totals[m] = totals[m] + h * star
                exports[m] = exports[m] - h * edge_lap
                exports_ns[m] = exports_ns[m] - h * edge_ns

    tiles[p, EARLY * NI:(EARLY + 1) * NI] = totals[0]
    tiles[p, (EARLY + 1) * NI:(EARLY + 2) * NI] = totals[1]
    for m in range(2):
        row = (EARLY + LATE) * NI + 2 * m
        tiles[p, row:row + 1] = exports[m][0:1]
        tiles[p, row + 1:row + 2] = exports[m][NI - 1:]
    out_rows = zero
    for row, x in ((0, exports[0][0:1]), (1, exports[1][0:1]), (NI - 2, exports[1][NI - 1:]), (NI - 1, exports[0][NI - 1:])):
        out_rows = jnp.where(sub == row, jnp.broadcast_to(x, (NI, NJ)), out_rows)
    ns_rows = []
    for m, x in enumerate(exports_ns):
        x = jnp.where(lane == 0, pltpu.roll(x, 1, 1), jnp.where(lane == NJ - 1, pltpu.roll(x, NJ - 1, 1), 0.0))
        x = jnp.sum(pltpu.roll(x, 0, 1, stride=width, stride_axis=0), axis=0, keepdims=True)
        row = (EARLY + LATE) * NI + 4 + m
        tiles[p, row:row + 1] = x
        ns_rows.append(jnp.broadcast_to(x, (NI, NJ)))
    pack_strips(1, -1.0, (*totals, out_rows), ns_rows)
    cast(1)

    levels_out = (pressure, laps.at[0], laps.at[1])
    for side, d in enumerate((NI - 1, 0)):
        for m, x in enumerate(levels_out):
            row = REST + (2 + m) * K
            pack_out[side, row:row + K, :] = x[:, d, :]
    n2 = s2 = zero
    for m, x in enumerate(levels_out):
        for k in range(K):
            n2 = put(n2, x[k], NJ - 1, m * K + k)
            s2 = put(s2, x[k], 0, m * K + k)
    lap_edges[0] = n2
    lap_edges[1] = s2
    meet(lap_edges, lap_slots, 2)
    sides(REST + 2 * K, 3 * K, NC + 1)

    cast_wait(0)
    flat = tiles.reshape(n_lon * TILES * NI, NJ)
    flat_rim = rims.reshape(2 * n_lon * NI, NJ)
    lanes = iota((n_lon, NJ), 1)

    def loader(f):
        main = [flat[pl.ds(f * NI + s, n_lon, stride=TILES * NI), :] for s in range(NI)]
        north = flat_rim[pl.ds(f, n_lon, stride=NI), :]
        south = jnp.where(not_south, flat_rim[pl.ds(n_lon * NI + f, n_lon, stride=NI), :], 0.0)
        outer = []
        for s in range(NI):
            x = jnp.where(lanes >= NJ - width, pltpu.roll(south, (NJ - width - width * s) % NJ, 1), 0.0)
            outer.append(jnp.where(lanes < width, pltpu.roll(north, (NJ - width * s) % NJ, 1), x))
        return [main, outer]

    def rim_rows(f):
        north = flat_rim[pl.ds(f, n_lon, stride=NI), :]
        south = jnp.where(not_south, flat_rim[pl.ds(n_lon * NI + f, n_lon, stride=NI), :], 0.0)
        return jnp.where(lanes % width == width - 1, north, south)

    def share(total):
        sums[q] = jnp.broadcast_to(total, (NI, NJ))
        for r in range(1, n_lat):
            lat = lax.rem(q + r, n_lat)
            copy(sums.at[q], sums.at[q], p, lat, cast_send.at[3], cast_recv.at[2, 0]).start()


    def late_wait():
        cast_wait(1)

    x, slope_x, slope_y = surface_solve(loader, rim_rows, late_wait, share, n_lon, K, NI, NJ)
    for i, field in enumerate((x, slope_x, slope_y)):
        for s in range(NI):
            held[i, pl.ds(s, n_lon, stride=NI), :] = field[s]
    block = pl.ds(pl.multiple_of(p * NI, NI), NI)
    ox_ref[0] = held[0, block, :]
    slope_u = GRAVITY * held[1, block, :]
    slope_v = GRAVITY * held[2, block, :]
    drain(pack_in.at[:, REST:REST + 2 * K], chunk_sem.at[NC])
    drain(pack_in.at[:, REST + 2 * K:], chunk_sem.at[NC + 1])
    met(lap_slots, 2)
    fold = jnp.where(lane < K, 1.0, -1.0)
    rim[2] = jnp.where(at_pole, flip_rows(lap_slots[0]) * fold, lap_slots[0])
    rim[3] = jnp.where(not_south, lap_slots[1], 0.0)
    both_e = jnp.minimum(depth, shift_e(depth, base_e))
    both_w = jnp.minimum(depth, shift_w(depth, base_w))
    both_n = jnp.where(lane == NJ - 1, near_ns, near_n)
    both_s = jnp.where(is_s, near_ns, near_s)

    def shift_n(x, packed, source):
        return jnp.where(lane == NJ - 1, pltpu.roll(packed, NJ - 1 - source, 1), pltpu.roll(x, NJ - 1, 1))

    def shift_s(x, packed, source):
        return jnp.where(lane == 0, pltpu.roll(packed, lax.rem(NJ - source, NJ), 1), pltpu.roll(x, 1, 1))

    def around(c, inner, ref, f):
        k = c * KC + inner
        x = ref[k]
        row = pl.ds(NI + c * SIDE + (f - 2) * KC + inner if f >= 2 else REST + f * K + k, 1)
        return (x, shift_e(x, pack_in[0, row, :]), shift_w(x, pack_in[1, row, :]),
                shift_n(x, rim[0], f * K + k), shift_s(x, rim[1], f * K + k))

    def beyond_ew(f, k):
        row = pl.ds(REST + f * K + k, 1)
        return jnp.where(is_w, pack_in[1, row, :], pack_in[0, row, :])

    def beyond_ns(f, k):
        at = f * K + k
        north = pltpu.roll(rim[2], NJ - 1 - at, 1)
        return jnp.where(is_s, pltpu.roll(rim[3], lax.rem(NJ - at, NJ), 1), north)

    def tracers(c, i, carry):
        k = c * KC + i
        flux_t, flux_s = carry
        kf = lax.convert_element_type(k, F32) + 0.5
        h = thick_ref[k]
        nxt = jnp.minimum(k + 1, K - 1)
        h_next = thick_ref[nxt]
        hv = jnp.full((NI, NJ), h, F32)
        inv_space = 1.0 / (0.5 * (hv + h_next))
        inv_h = MIXING / hv

        def wet(d):
            return jnp.where(d > kf, 1.0, 0.0)

        mc = wet(depth)
        me, mw, mn, ms = wet(both_e), wet(both_w), wet(both_n), wet(both_s)
        below = jnp.where(jnp.logical_and(depth > kf + 1.0, k < K - 1), inv_space, 0.0)
        t = around(c, i, t_ref, 0)
        s = around(c, i, s_ref, 1)
        u0, ue, uw = around(c, i, u_ref, 2)[:3]
        v0, _, _, vn, vs = around(c, i, v_ref, 3)
        ae = 0.25 * me * (u0 + ue)
        aw = 0.25 * mw * (u0 + uw)
        an = 0.25 * mn * (v0 + vn)
        as_ = 0.25 * ms * (v0 + vs)
        ge, gw, gn, gs = DIFFUSION * me, DIFFUSION * mw, DIFFUSION * mn, DIFFUSION * ms

        def tracer(x, ref, flux_above):
            c, e, w, n, so = x
            total = aw * (w + c) - gw * (c - w) - ae * (c + e) + ge * (e - c)
            total = total + as_ * (so + c) - gs * (c - so) - an * (c + n) + gn * (n - c)
            flux = below * (ref[nxt] - c)
            return mc * (c + total + inv_h * (flux - flux_above)), flux

        new_t, flux_t = tracer(t, t_ref, flux_t)
        new_s, flux_s = tracer(s, s_ref, flux_s)
        ot_ref[k] = new_t
        os_ref[k] = new_s
        for m, (out, slope) in enumerate(((ou_ref, slope_u), (ov_ref, slope_v))):
            lap_ew, lap_ns = beyond_ew(3 + m, k), beyond_ns(1 + m, k)
            push = -FRICTION * (gate(near_ew, kf, lap_ew) + gate(near_ns, kf, lap_ns))
            if m == 0:
                push = push + scale_ew * gate(near_ew, kf, beyond_ew(2, k))
            else:
                push = push + scale_ns * gate(near_ns, kf, beyond_ns(0, k))
            star = out[k] + push
            out[k] = gate(depth, kf, star - slope)
        return flux_t, flux_s

    def tracer_chunk(c, carry):
        for i in range(KC):
            carry = tracers(c, i, carry)
        return carry

    lax.fori_loop(0, NC, tracer_chunk, (zero,) * 2)

    drain(pack_out, send_sem.at[0])

    sent = pack_in.at[0, 0:3 * NI]

    @pl.when(not_south)
    def _():
        drain(sent, send_sem.at[1])

    drain(sent, send_sem.at[2])

    used = pl.ds(0, NI)
    drain(tiles.at[pl.ds(0, n_lon - 1), pl.ds(0, (EARLY + LATE) * NI + 6)], cast_send.at[0])

    @pl.when(not_south)
    def _():
        drain(rims.at[0, pl.ds(0, n_lon), used], cast_send.at[1])

    @pl.when(not_pole)
    def _():
        drain(rims.at[0, pl.ds(0, n_lon), used], cast_send.at[2])

    @pl.when(at_pole)
    def _():
        drain(rims.at[0, pl.ds(0, n_lon - 1), used], cast_send.at[2])

    drain(sums.at[pl.ds(0, n_lat - 1)], cast_recv.at[2, 0])
    total = functools.reduce(lambda a, b: a + b, [sums[lat] for lat in range(n_lat)])
    ox_ref[1] = jnp.sqrt(total / (n_lon * NI * n_lat * NJ) + EPSILON)
    drain(sums.at[pl.ds(0, n_lat - 1)], cast_send.at[3])


def surface_solve(load, rim_rows, late_wait, share, n_lon, K, NI, NJ):
    width = NJ // NI
    tiles = range(2)
    lines = range(NI)
    lane = iota((n_lon, NJ), 1)
    edge = jnp.logical_or(lane == 0, lane == NJ - 1)

    def every(fn, *arrays):
        return [[fn(*(a[b][s] for a in arrays)) for s in lines] for b in tiles]

    def east(x):
        return [x[b][1:] + [pltpu.roll(x[b][0], n_lon - 1, 0)] for b in tiles]

    def west(x):
        return [[pltpu.roll(x[b][NI - 1], 1, 0)] + x[b][:-1] for b in tiles]

    def joined(x, shift, edge):
        moved = [[pltpu.roll(x[b][s], shift, 1) for s in lines] for b in tiles]
        return [[jnp.where(lane == edge, moved[1 - b][s], moved[b][s]) for s in lines] for b in tiles]

    def north(x):
        return joined(x, NJ - 1, NJ - 1)

    def south(x):
        return joined(x, 1, 0)

    height = load(0)
    scale = lambda a, c: jnp.minimum(a, c) * (1.0 / K)
    w_e = every(scale, height, east(height))
    w_w = every(scale, height, west(height))
    w_n = every(scale, height, north(height))
    w_s = every(scale, height, south(height))
    diag = every(lambda a, b, c, d: STORAGE + a + b + c + d, w_e, w_w, w_n, w_s)

    def apply(x):
        return every(
            lambda dg, c, we, e, ww, w, wn, n, ws, s: dg * c - (we * e + ww * w + wn * n + ws * s),
            diag, x, w_e, east(x), w_w, west(x), w_n, north(x), w_s, south(x))

    middle = NI // 2
    spans = [(s, s - 1, s + 1) for s in range(middle)]
    spans += [(s, s + 1, s - 1) for s in range(NI - 1, middle - 1, -1)]
    pivots, carries, factors = ([[None] * NI for _ in tiles] for _ in range(3))
    joints = []
    for b in tiles:
        for s, before, after in spans:
            back, ahead = (w_w, w_e) if after > s else (w_e, w_w)
            pivot = diag[b][s]
            if s not in (0, NI - 1):
                pivot = pivot + back[b][s] * factors[b][before]
            pivots[b][s] = 1.0 / pivot
            carries[b][s] = back[b][s] * pivots[b][s]
            factors[b][s] = -ahead[b][s] * pivots[b][s]
        joints.append(1.0 / (1.0 - factors[b][middle - 1] * factors[b][middle]))

    def precondition(r):
        out = []
        for b in tiles:
            part = [None] * NI
            for s, before, after in spans:
                part[s] = r[b][s] * pivots[b][s]
                if s not in (0, NI - 1):
                    part[s] = part[s] + carries[b][s] * part[before]
            low, high = part[middle - 1], part[middle]
            part[middle - 1] = (low - factors[b][middle - 1] * high) * joints[b]
            part[middle] = (high - factors[b][middle] * low) * joints[b]
            for s in range(middle - 2, -1, -1):
                part[s] = part[s] - factors[b][s] * part[s + 1]
            for s in range(middle + 1, NI):
                part[s] = part[s] - factors[b][s] * part[s - 1]
            out.append(part)
        return out

    x = load(1)
    drive = load(2)
    start = every(lambda h, d, a: jnp.where(h > 0.0, d, 0.0) - a, height, drive, apply(x))
    late_wait()
    t_u = load(EARLY)
    t_v = load(EARLY + 1)
    inner, outer = load(EARLY + LATE)
    for m, t in enumerate((t_u, t_v)):
        for b, (from_w, from_e) in enumerate(((inner[2 * m], inner[2 * m + 1]), (outer[m], outer[NI - 1 - m]))):
            t[b][NI - 1] = t[b][NI - 1] + pltpu.roll(from_w, n_lon - 1, 0)
            t[b][0] = t[b][0] + pltpu.roll(from_e, 1, 0)
        own, beyond = inner[4 + m], rim_rows(EARLY + LATE + 1 + m)
        for s in lines:
            for b, row in ((0, beyond), (1, own)):
                moved = pltpu.roll(row, (NJ - width * s) % NJ, 1) if s else row
                t[b][s] = t[b][s] + jnp.where(edge, moved, 0.0)
    residual = every(
        lambda h, d, e, w, n, s: d - jnp.where(h > 0.0, 0.5 * DIVERGENCE * ((e - w) + (n - s)), 0.0),
        height, start, east(t_u), west(t_u), north(t_v), south(t_v))
    mid = 0.5 * (SPECTRUM_HIGH + SPECTRUM_LOW)
    half = 0.5 * (SPECTRUM_HIGH - SPECTRUM_LOW)
    ratio = mid / half
    direction = every(lambda a: a / mid, precondition(residual))
    rho = 1.0 / ratio
    for step in range(ITERS):
        x = every(lambda a, b: a + b, x, direction)
        residual = every(lambda a, b: a - b, residual, apply(direction))
        if step + 1 < ITERS:
            rho_next = 1.0 / (2.0 * ratio - rho)
            keep, gain = rho_next * rho, 2.0 * rho_next / half
            direction = every(lambda d, z: keep * d + gain * z, direction, precondition(residual))
            rho = rho_next
    squares = functools.reduce(lambda a, b: a + b, [a * a for a in residual[0]])
    share(jnp.sum(jnp.sum(squares, axis=1, keepdims=True), axis=0, keepdims=True))
    slope_x = every(lambda e, w: 0.5 * (e - w), east(x), west(x))
    slope_y = every(lambda n, s: 0.5 * (n - s), north(x), south(x))
    return x[0], slope_x[0], slope_y[0]


def finish_kernel(kept, x_ref, ot_ref, os_ref, ou_ref, ov_ref, ox_ref, orms_ref, rms, sem):
    for f, target in enumerate((ot_ref, os_ref, ou_ref, ov_ref)):
        pltpu.make_async_copy(kept.at[f], target, sem.at[0]).start()
    surface = pltpu.make_async_copy(x_ref.at[0], ox_ref, sem.at[1])
    surface.start()
    rms[0] = jnp.max(x_ref[1])
    scalar = pltpu.make_async_copy(rms, orms_ref, sem.at[2])
    scalar.start()
    pltpu.make_async_copy(kept, kept, sem.at[0]).wait()
    surface.wait()
    scalar.wait()


def per_device(n_lon, n_lat, *args):
    K, NI, NJ = args[0].shape
    KC = 8 if K % 8 == 0 else K
    NC = K // KC
    vmem = pl.BlockSpec(memory_space=pltpu.VMEM)
    hbm = pl.BlockSpec(memory_space=pltpu.HBM)
    big = jax.ShapeDtypeStruct((K, NI, NJ), F32)
    tile = jax.ShapeDtypeStruct((NI, NJ), F32)
    one = jax.ShapeDtypeStruct((1,), F32)
    pack = pltpu.VMEM((2, NI + NC * 2 * KC + 5 * K, NJ), F32)

    def room(*lead):
        return pltpu.VMEM((*lead, NI, NJ), F32)

    parts = pl.pallas_call(
        functools.partial(step_kernel, n_lon, n_lat, KC),
        out_shape=(room(4, K), room(2)),
        in_specs=[hbm] * 9,
        out_specs=(vmem,) * 2,
        scratch_shapes=[
            room(4, K), pltpu.VMEM((2, NI, NJ), jnp.int32), room(2), pltpu.SMEM((K,), F32),
            pack, pack, room(2, 2), room(2, 2), room(2), room(2), room(4),
            room(2, K), room(K), pltpu.VMEM((n_lon, TILES * NI, NJ), F32), room(2), room(2, n_lon), room(n_lat),
            pltpu.VMEM((3, n_lon * NI, NJ), F32),
            pltpu.SemaphoreType.DMA((3,)), pltpu.SemaphoreType.DMA((3,)), pltpu.SemaphoreType.DMA((NC + 2,)),
            pltpu.SemaphoreType.DMA((4,)), pltpu.SemaphoreType.DMA((4,)), pltpu.SemaphoreType.DMA((3, 3)),
        ],
        compiler_params=pltpu.CompilerParams(
            collective_id=0, has_side_effects=True),
        name="step",
    )(*args)
    outs = pl.pallas_call(
        finish_kernel,
        out_shape=(big, big, big, big, tile, one),
        in_specs=[vmem] * 2,
        out_specs=(hbm,) * 6,
        scratch_shapes=[pltpu.SMEM((1,), F32), pltpu.SemaphoreType.DMA((3,))],
        name="finish",
    )(*[pltpu.with_memory_space_constraint(part, pltpu.VMEM) for part in parts])
    return outs[:5] + (outs[5].reshape(()),)


def solution(mesh):
    n_lon, n_lat = mesh.shape["lon"], mesh.shape["lat"]
    spec3 = P(None, "lon", "lat")
    spec2 = P("lon", "lat")
    return jax.shard_map(
        functools.partial(per_device, n_lon, n_lat),
        mesh=mesh,
        in_specs=(spec3, spec3, spec3, spec3, spec2, spec2, P(), spec2, spec2),
        out_specs=(spec3, spec3, spec3, spec3, spec2, P()),
        check_vma=False,
    )
```

```python
import functools

import jax
import jax.numpy as jnp
from jax import lax
from jax.experimental import pallas as pl
from jax.experimental.pallas import tpu as pltpu
from jax.sharding import PartitionSpec as P

ITERS = 4
DIFFUSION = 0.15
MIXING = 0.1
EXPANSION = 0.2
CONTRACTION = 0.15
PRESSURE_SCALE = 0.02
CORIOLIS = 0.5
FRICTION = 0.01
DIVERGENCE = 0.3
STORAGE = 0.1
SPECTRUM_LOW = 0.1
SPECTRUM_HIGH = 1.9
GRAVITY = 0.3
EPSILON = 1e-06

MESH = pl.DeviceIdType.MESH
F32 = jnp.float32
EARLY = 3
LATE = 2
TILES = EARLY + LATE + 1


def iota(shape, axis):
    return lax.broadcasted_iota(jnp.int32, shape, axis)


def flip(x, axis):
    return jnp.take_along_axis(x, x.shape[axis] - 1 - iota(x.shape, axis), axis=axis)


def flip_rows(x):
    return flip(x, 0)


def flip_lanes(x):
    return flip(x, 1)


def step_kernel(n_lon, n_lat, KC, *refs):
    sources, refs = refs[:9], refs[9:]
    (kept, ox_ref), refs = refs[:2], refs[2:]
    (fields, ints, floats, thick_ref, pack_out, pack_in, edges, slots, lap_edges, lap_slots, rim, laps, pressure, tiles, strips,
     rims, sums, held, load_sem, send_sem, chunk_sem, edge_sem, cast_send, cast_recv) = refs
    _, K, NI, NJ = fields.shape
    NC = K // KC
    SIDE = 2 * KC
    REST = NI + NC * SIDE
    t_ref, s_ref, u_ref, v_ref = (fields.at[f] for f in range(4))
    ot_ref, os_ref, ou_ref, ov_ref = (kept.at[f] for f in range(4))
    num_ref, sea_ref, eta_ref, drive_ref = ints.at[0], ints.at[1], floats.at[0], floats.at[1]
    p = lax.axis_index("lon")
    q = lax.axis_index("lat")
    east_dev = lax.rem(p + 1, n_lon)
    west_dev = lax.rem(p + n_lon - 1, n_lon)
    at_pole = q == n_lat - 1
    not_pole = q < n_lat - 1
    not_south = q > 0
    mirror = n_lon - 1 - p
    lons = [lax.rem(p + r, n_lon) for r in range(min(n_lon, 8))]

    barrier = pltpu.get_barrier_semaphore()

    def greet(lon, lat):
        pl.semaphore_signal(barrier, inc=1, device_id={"lon": lon, "lat": lat}, device_id_type=MESH)

    greet(east_dev, q)
    if n_lon > 2:
        greet(west_dev, q)

    def around_lon(first, last, fn):
        def visit(r, carry):
            fn(lax.rem(p + r, n_lon))
            return carry

        if n_lon <= 8:
            for lon in lons[first:last]:
                fn(lon)
        else:
            lax.fori_loop(first, last, visit, 0)

    @pl.when(at_pole)
    def _():
        around_lon(2, n_lon - 1, lambda lon: greet(lon, q))

    @pl.when(not_south)
    def _():
        around_lon(0, n_lon, lambda lon: greet(lon, q - 1))

    @pl.when(not_pole)
    def _():
        around_lon(0, n_lon, lambda lon: greet(lon, q + 1))

    def load(i, dst, sem):
        pltpu.make_async_copy(sources[i], dst, load_sem.at[sem]).start()

    load(4, num_ref, 1)
    load(5, sea_ref, 1)
    load(7, eta_ref, 1)
    load(8, drive_ref, 1)
    for f in (2, 3, 0, 1):
        load(f, fields.at[f], 0)
    thick_load = pltpu.make_async_copy(sources[6], thick_ref, load_sem.at[2])
    thick_load.start()

    @pl.when(not_pole)
    def _():
        around_lon(2, n_lon - 1, lambda lon: greet(lon, q))

    for lat in range(n_lat):
        @pl.when(jnp.logical_or(q - lat > 1, lat - q > 1))
        def _():
            greet(p, lat)

    def drain(ref, sem):
        pltpu.make_async_copy(ref, ref, sem).wait()

    thick_load.wait()
    drain(fields.at[0, 0:4], load_sem.at[1])
    drain(fields, load_sem.at[0])
    sub = iota((NI, NJ), 0)
    lane = iota((NI, NJ), 1)
    depth = (num_ref[...] * sea_ref[...]).astype(F32)

    for side, d1 in enumerate((NI - 1, 0)):
        for c in range(NC):
            levels = slice(c * KC, (c + 1) * KC)
            for m, ref in enumerate((u_ref, v_ref)):
                row = NI + c * SIDE + m * KC
                pack_out[side, row:row + KC, :] = ref[levels, d1, :]
        for m, ref in enumerate((t_ref, s_ref)):
            row = REST + m * K
            pack_out[side, row:row + K, :] = ref[:, d1, :]
        pack_out[side, 0:NI, :] = jnp.broadcast_to(depth[d1:d1 + 1, :], (NI, NJ))

    zero = jnp.zeros((NI, NJ), F32)

    def put(acc, x, source, target):
        moved = pltpu.roll(x, (target - source) % NJ, 1) if source != target else x
        return jnp.where(lane == target, moved, acc)

    n0 = s0 = zero
    for f, ref in enumerate((t_ref, s_ref, u_ref, v_ref)):
        for k in range(K):
            n0 = put(n0, ref[k], NJ - 1, f * K + k)
            s0 = put(s0, ref[k], 0, f * K + k)
    npk, spk = edges.at[0], edges.at[1]
    npk[0] = n0
    npk[1] = put(zero, depth, NJ - 1, 0)
    spk[0] = s0
    spk[1] = put(zero, depth, 0, 0)

    peers = n_lon + n_lat - 2 + (n_lon - 1) * (not_south.astype(jnp.int32) + not_pole.astype(jnp.int32))
    pl.semaphore_wait(barrier, peers)

    def copy(src, dst, lon, lat, out, into):
        return pltpu.make_async_remote_copy(
            src_ref=src, dst_ref=dst, send_sem=out, recv_sem=into,
            device_id={"lon": lon, "lat": lat}, device_id_type=MESH)

    def meet(pack, slot, sem):
        @pl.when(at_pole)
        def _():
            copy(pack.at[0], slot.at[0], mirror, q, send_sem.at[2], edge_sem.at[sem]).start()

        @pl.when(not_south)
        def _():
            copy(pack.at[1], slot.at[0], p, q - 1, send_sem.at[1], edge_sem.at[sem]).start()

        @pl.when(not_pole)
        def _():
            copy(pack.at[0], slot.at[1], p, q + 1, send_sem.at[2], edge_sem.at[sem + 1]).start()

    def met(slot, sem):
        drain(slot.at[0], edge_sem.at[sem])

        @pl.when(not_south)
        def _():
            drain(slot.at[1], edge_sem.at[sem + 1])

    meet(edges, slots, 0)

    def sides(first, rows, sem):
        rows = pl.ds(first, rows)
        copy(pack_out.at[1, rows], pack_in.at[0, rows], west_dev, q, send_sem.at[0], chunk_sem.at[sem]).start()
        copy(pack_out.at[0, rows], pack_in.at[1, rows], east_dev, q, send_sem.at[0], chunk_sem.at[sem]).start()

    starts = [0] + [NI + c * SIDE for c in range(1, NC + 1)]
    for c in range(NC):
        sides(starts[c], starts[c + 1] - starts[c], c)

    height = zero
    for k in range(K):
        height = height + jnp.where(depth > k + 0.5, thick_ref[k], 0.0)
    width = NJ // NI
    in_block = lane // width == sub
    parts = ((0, EARLY, EARLY * NI), (EARLY, LATE + 3, LATE * NI + 6))

    def pack_strips(which, sign, arrays, rows=()):
        first, count, _ = parts[which]
        given = len(arrays)
        south = zero
        north = zero
        for i, x in enumerate(arrays):
            for start in (0, width):
                moved = pltpu.roll(x, start, 1, stride=width, stride_axis=0)
                row = jnp.sum(jnp.where(in_block, moved, 0.0), axis=0, keepdims=True)
                row = jnp.broadcast_to(row, (NI, NJ))
                if start:
                    north = jnp.where(sub == i, row, north)
                else:
                    south = jnp.where(sub == i, row, south)
        for i, row in enumerate(rows):
            north = jnp.where(sub == given + i, row, north)
            south = jnp.where(sub == given + i, row, south)
        turned = jnp.where(sub >= given, pltpu.roll(north, width, 1), north) if rows else north
        north = jnp.where(at_pole, sign * flip_lanes(turned), north)
        rows = slice(first, first + count)
        strips[0, rows] = south[:count]
        strips[1, rows] = north[:count]

        @pl.when(at_pole)
        def _():
            rims[0, mirror, rows] = north[:count]

    def each_other(fn):
        def visit(r, carry):
            fn(jnp.where(r <= p, r - 1, r))
            return carry

        if n_lon <= 8:
            for r in range(1, n_lon):
                visit(r, 0)
        else:
            lax.fori_loop(1, n_lon, visit, 0)

    def cast(which):
        first, count, size = parts[which]
        mine = tiles.at[p, pl.ds(first * NI, size)]
        rows = pl.ds(first, count)
        pole = at_pole.astype(jnp.int32)
        side, lat = 1 - pole, q + 1 - pole
        slot = jnp.where(at_pole, mirror, p)

        def send(way, side, slot, lon, lat, out):
            copy(strips.at[way, rows], rims.at[side, slot, rows], lon, lat, cast_send.at[out],
                 cast_recv.at[which, 1 + side]).start()

        @pl.when(not_pole)
        def _():
            send(1, 1, p, p, q + 1, 2)

        @pl.when(not_south)
        def _():
            send(0, 0, p, p, q - 1, 1)

        def to(lon):
            @pl.when(not_south)
            def _():
                send(0, 0, p, lon, q - 1, 1)

            send(1, side, slot, lon, lat, 2)
            copy(mine, mine, lon, q, cast_send.at[0], cast_recv.at[which, 0]).start()

        each_other(to)

    def cast_wait(which):
        first, count, size = parts[which]
        rows = pl.ds(first, count)
        drain(tiles.at[pl.ds(0, n_lon - 1), pl.ds(first * NI, size)], cast_recv.at[which, 0])

        @pl.when(at_pole)
        def _():
            drain(rims.at[0, pl.ds(0, n_lon - 1), rows], cast_recv.at[which, 1])

        @pl.when(not_pole)
        def _():
            drain(rims.at[0, pl.ds(0, n_lon), rows], cast_recv.at[which, 1])

        @pl.when(not_south)
        def _():
            drain(rims.at[1, pl.ds(0, n_lon), rows], cast_recv.at[which, 2])

    first_guess = sea_ref[...].astype(F32) * eta_ref[...]
    for i, x in enumerate((height, first_guess, drive_ref[...])):
        tiles[p, i * NI:(i + 1) * NI] = x
    pack_strips(0, 1.0, (height, first_guess, drive_ref[...]))

    near_e = jnp.where(sub == NI - 1, 0.0, jnp.minimum(depth, pltpu.roll(depth, NI - 1, 0)))
    near_w = jnp.where(sub == 0, 0.0, jnp.minimum(depth, pltpu.roll(depth, 1, 0)))
    near_n = jnp.where(lane == NJ - 1, 0.0, jnp.minimum(depth, pltpu.roll(depth, NJ - 1, 1)))
    near_s = jnp.where(lane == 0, 0.0, jnp.minimum(depth, pltpu.roll(depth, 1, 1)))
    lat_index = (q * NJ + lane).astype(F32)
    coriolis = CORIOLIS * (2.0 * (lat_index + 0.5) / (n_lat * NJ) - 1.0)

    def gate(d, kf, x):
        return jnp.where(d > kf, x, 0.0)

    def inner_lap(x, kf):
        total = gate(near_e, kf, pltpu.roll(x, NI - 1, 0) - x) + gate(near_w, kf, pltpu.roll(x, 1, 0) - x)
        return total + (gate(near_n, kf, pltpu.roll(x, NJ - 1, 1) - x) + gate(near_s, kf, pltpu.roll(x, 1, 1) - x))

    def before_level(k, carry):
        pc, tu, tv = carry
        kf = lax.convert_element_type(k, F32) + 0.5
        u, v = u_ref[k], v_ref[k]
        laps[0, k] = inner_lap(u, kf)
        laps[1, k] = inner_lap(v, kf)
        pc = pc + gate(depth, kf, (CONTRACTION * s_ref[k] - EXPANSION * t_ref[k]) * thick_ref[k])
        pressure[k] = pc
        grad_x = gate(near_e, kf, pltpu.roll(pc, NI - 1, 0) - pc) + gate(near_w, kf, pc - pltpu.roll(pc, 1, 0))
        grad_y = gate(near_n, kf, pltpu.roll(pc, NJ - 1, 1) - pc) + gate(near_s, kf, pc - pltpu.roll(pc, 1, 1))
        u_part = u + coriolis * v - (0.5 * PRESSURE_SCALE) * grad_x
        v_part = v - coriolis * u - (0.5 * PRESSURE_SCALE) * grad_y
        ou_ref[k] = u_part
        ov_ref[k] = v_part
        h = thick_ref[k]
        return pc, tu + gate(depth, kf, h * u_part), tv + gate(depth, kf, h * v_part)

    def before_chunk(c, carry):
        for i in range(KC):
            carry = before_level(c * KC + i, carry)
        return carry

    totals = list(lax.fori_loop(0, NC, before_chunk, (zero,) * 3)[1:])

    cast(0)
    met(slots, 0)

    sign = jnp.where(lane >= 2 * K, -1.0, 1.0).astype(F32)

    def arrived(slot, i, fold):
        north = jnp.where(at_pole, flip_rows(slot[0, i]) * fold, slot[0, i])
        return north, jnp.where(not_south, slot[1, i], 0.0)

    pn0, ps0 = arrived(slots, 0, sign)
    pn1, ps1 = arrived(slots, 1, 1.0)

    def shift_e(x, row):
        return jnp.where(sub == NI - 1, row, pltpu.roll(x, NI - 1, 0))

    def shift_w(x, row):
        return jnp.where(sub == 0, row, pltpu.roll(x, 1, 0))

    rim[0] = pn0
    rim[1] = ps0

    drain(pack_in.at[:, 0:starts[1]], chunk_sem.at[0])
    sides(REST, 2 * K, NC)
    base_e = pack_in[0, 0:1, :]
    base_w = pack_in[1, 0:1, :]
    is_w = sub == 0
    is_s = lane == 0
    depth_ew = jnp.where(is_w, base_w, base_e)
    depth_ns = jnp.where(is_s, ps1, pltpu.roll(pn1, NJ - 1, 1))
    on_ew = jnp.logical_or(is_w, sub == NI - 1)
    on_ns = jnp.logical_or(is_s, lane == NJ - 1)
    near_ew = jnp.where(on_ew, jnp.minimum(depth, depth_ew), 0.0)
    near_ns = jnp.where(on_ns, jnp.minimum(depth, depth_ns), 0.0)
    scale_ew = jnp.where(is_w, 0.5 * PRESSURE_SCALE, -0.5 * PRESSURE_SCALE)
    scale_ns = jnp.where(is_s, 0.5 * PRESSURE_SCALE, -0.5 * PRESSURE_SCALE)

    def rim_ns(north, south, k):
        x = pltpu.roll(north, (NJ - 1 - k) % NJ, 1)
        return jnp.where(is_s, pltpu.roll(south, (NJ - k) % NJ, 1), x)

    def side_ew(c, row):
        row = NI + c * SIDE + row
        return jnp.where(is_w, pack_in[1, row:row + 1, :], pack_in[0, row:row + 1, :])

    both_e = jnp.where(sub == NI - 1, near_ew, near_e)
    both_w = jnp.where(is_w, near_ew, near_w)
    both_n = jnp.where(lane == NJ - 1, near_ns, near_n)
    both_s = jnp.where(is_s, near_ns, near_s)
    overlaps = (both_e, both_w, both_n, both_s)
    sums_lap = [[zero] * 4 for _ in range(2)]
    push_ew = push_ns = zero
    for c in range(NC):
        if c:
            drain(pack_in.at[:, starts[c]:starts[c + 1]], chunk_sem.at[c])
        for i in range(KC):
            k = c * KC + i
            kf = k + 0.5
            h = thick_ref[k]
            hp = h * pressure[k]
            push_ew = push_ew + gate(near_ew, kf, hp)
            push_ns = push_ns + gate(near_ns, kf, hp)
            for m, x in enumerate((u_ref[k], v_ref[k])):
                lap = laps[m, k] + gate(near_ew, kf, side_ew(c, m * KC + i) - x)
                lap = lap + gate(near_ns, kf, rim_ns(rim[0], rim[1], (2 + m) * K + k) - x)
                laps[m, k] = lap
                hl = h * lap
                sums_lap[m] = [a + gate(d, kf, hl) for a, d in zip(sums_lap[m], overlaps)]
    push_ew = scale_ew * push_ew
    push_ns = scale_ns * push_ns
    exports, exports_ns = [], []
    for m, (a_e, a_w, a_n, a_s) in enumerate(sums_lap):
        given = jnp.where(sub == NI - 1, 0.0, pltpu.roll(a_w, NI - 1, 0)) + jnp.where(is_w, 0.0, pltpu.roll(a_e, 1, 0))
        given = given + jnp.where(lane == NJ - 1, 0.0, pltpu.roll(a_s, NJ - 1, 1))
        given = given + jnp.where(is_s, 0.0, pltpu.roll(a_n, 1, 1))
        totals[m] = totals[m] + FRICTION * ((a_e + a_w) + (a_n + a_s) - given)
        exports.append(-FRICTION * jnp.where(is_w, a_w, a_e))
        exports_ns.append(-FRICTION * jnp.where(is_s, a_s, a_n))
    totals = [totals[0] - push_ew, totals[1] - push_ns]
    exports[0] = exports[0] - push_ew
    exports_ns[1] = exports_ns[1] - push_ns

    tiles[p, EARLY * NI:(EARLY + 1) * NI] = totals[0]
    tiles[p, (EARLY + 1) * NI:(EARLY + 2) * NI] = totals[1]
    for m in range(2):
        row = (EARLY + LATE) * NI + 2 * m
        tiles[p, row:row + 1] = exports[m][0:1]
        tiles[p, row + 1:row + 2] = exports[m][NI - 1:]
    out_rows = zero
    for row, x in ((0, exports[0][0:1]), (1, exports[1][0:1]), (NI - 2, exports[1][NI - 1:]), (NI - 1, exports[0][NI - 1:])):
        out_rows = jnp.where(sub == row, jnp.broadcast_to(x, (NI, NJ)), out_rows)
    ns_rows = []
    for m, x in enumerate(exports_ns):
        x = jnp.where(lane == 0, pltpu.roll(x, 1, 1), jnp.where(lane == NJ - 1, pltpu.roll(x, NJ - 1, 1), 0.0))
        x = jnp.sum(pltpu.roll(x, 0, 1, stride=width, stride_axis=0), axis=0, keepdims=True)
        row = (EARLY + LATE) * NI + 4 + m
        tiles[p, row:row + 1] = x
        ns_rows.append(jnp.broadcast_to(x, (NI, NJ)))
    pack_strips(1, -1.0, (*totals, out_rows), ns_rows)
    cast(1)

    for side, (d, push) in enumerate(((NI - 1, 0.5 * PRESSURE_SCALE), (0, -0.5 * PRESSURE_SCALE))):
        row = REST + 2 * K
        pack_out[side, row:row + K, :] = push * pressure[:, d, :] - FRICTION * laps[0, :, d, :]
        pack_out[side, row + K:row + 2 * K, :] = -FRICTION * laps[1, :, d, :]
    n2 = s2 = zero
    for k in range(K):
        for m, x in enumerate((-FRICTION * laps[0, k], -FRICTION * laps[1, k] - scale_ns * pressure[k])):
            n2 = put(n2, x, NJ - 1, m * K + k)
            s2 = put(s2, x, 0, m * K + k)
    lap_edges[0] = n2
    lap_edges[1] = s2
    meet(lap_edges, lap_slots, 2)
    sides(REST + 2 * K, 2 * K, NC + 1)

    def level(c, carry):
        for i in range(KC):
            k = c * KC + i
            kf = lax.convert_element_type(k, F32) + 0.5
            pc = pressure[k]
            parts = (ou_ref[k] - scale_ew * gate(near_ew, kf, pc), ov_ref[k] - scale_ns * gate(near_ns, kf, pc))
            for m, (part, out) in enumerate(zip(parts, (ou_ref, ov_ref))):
                lap = laps[m, k]
                inner = inner_lap(lap, kf) - gate(near_ew, kf, lap) - gate(near_ns, kf, lap)
                out[k] = gate(depth, kf, part - FRICTION * inner)
        return carry

    lax.fori_loop(0, NC, level, 0)

    cast_wait(0)
    flat = tiles.reshape(n_lon * TILES * NI, NJ)
    flat_rim = rims.reshape(2 * n_lon * NI, NJ)
    lanes = iota((n_lon, NJ), 1)

    def loader(f):
        main = [flat[pl.ds(f * NI + s, n_lon, stride=TILES * NI), :] for s in range(NI)]
        north = flat_rim[pl.ds(f, n_lon, stride=NI), :]
        south = jnp.where(not_south, flat_rim[pl.ds(n_lon * NI + f, n_lon, stride=NI), :], 0.0)
        outer = []
        for s in range(NI):
            x = jnp.where(lanes >= NJ - width, pltpu.roll(south, (NJ - width - width * s) % NJ, 1), 0.0)
            outer.append(jnp.where(lanes < width, pltpu.roll(north, (NJ - width * s) % NJ, 1), x))
        return [main, outer]

    def rim_rows(f):
        north = flat_rim[pl.ds(f, n_lon, stride=NI), :]
        south = jnp.where(not_south, flat_rim[pl.ds(n_lon * NI + f, n_lon, stride=NI), :], 0.0)
        return jnp.where(lanes % width == width - 1, north, south)

    def share(total):
        sums[q] = jnp.broadcast_to(total, (NI, NJ))
        for r in range(1, n_lat):
            lat = lax.rem(q + r, n_lat)
            copy(sums.at[q], sums.at[q], p, lat, cast_send.at[3], cast_recv.at[2, 0]).start()


    def late_wait():
        cast_wait(1)

    x, slope_x, slope_y = surface_solve(loader, rim_rows, late_wait, share, n_lon, K, NI, NJ)
    for i, field in enumerate((x, slope_x, slope_y)):
        for s in range(NI):
            held[i, pl.ds(s, n_lon, stride=NI), :] = field[s]
    block = pl.ds(pl.multiple_of(p * NI, NI), NI)
    ox_ref[0] = held[0, block, :]
    slope_u = GRAVITY * held[1, block, :]
    slope_v = GRAVITY * held[2, block, :]
    drain(pack_in.at[:, REST:REST + 2 * K], chunk_sem.at[NC])
    drain(pack_in.at[:, REST + 2 * K:], chunk_sem.at[NC + 1])
    met(lap_slots, 2)
    rim[2] = jnp.where(at_pole, -flip_rows(lap_slots[0]), lap_slots[0])
    rim[3] = jnp.where(not_south, lap_slots[1], 0.0)
    def shift_n(x, packed, source):
        return jnp.where(lane == NJ - 1, pltpu.roll(packed, NJ - 1 - source, 1), pltpu.roll(x, NJ - 1, 1))

    def shift_s(x, packed, source):
        return jnp.where(lane == 0, pltpu.roll(packed, lax.rem(NJ - source, NJ), 1), pltpu.roll(x, 1, 1))

    def around(c, inner, ref, f):
        k = c * KC + inner
        x = ref[k]
        row = pl.ds(NI + c * SIDE + (f - 2) * KC + inner if f >= 2 else REST + f * K + k, 1)
        return (x, shift_e(x, pack_in[0, row, :]), shift_w(x, pack_in[1, row, :]),
                shift_n(x, rim[0], f * K + k), shift_s(x, rim[1], f * K + k))

    def beyond_ew(f, k):
        row = pl.ds(REST + f * K + k, 1)
        return jnp.where(is_w, pack_in[1, row, :], pack_in[0, row, :])

    def beyond_ns(f, k):
        at = f * K + k
        north = pltpu.roll(rim[2], NJ - 1 - at, 1)
        return jnp.where(is_s, pltpu.roll(rim[3], lax.rem(NJ - at, NJ), 1), north)

    def tracers(c, i, carry):
        k = c * KC + i
        flux_t, flux_s = carry
        kf = lax.convert_element_type(k, F32) + 0.5
        h = thick_ref[k]
        nxt = jnp.minimum(k + 1, K - 1)
        h_next = thick_ref[nxt]
        hv = jnp.full((NI, NJ), h, F32)
        inv_space = 1.0 / (0.5 * (hv + h_next))
        inv_h = MIXING / hv

        def wet(d):
            return jnp.where(d > kf, 1.0, 0.0)

        mc = wet(depth)
        me, mw, mn, ms = wet(both_e), wet(both_w), wet(both_n), wet(both_s)
        below = jnp.where(jnp.logical_and(depth > kf + 1.0, k < K - 1), inv_space, 0.0)
        t = around(c, i, t_ref, 0)
        s = around(c, i, s_ref, 1)
        u0, ue, uw = around(c, i, u_ref, 2)[:3]
        v0, _, _, vn, vs = around(c, i, v_ref, 3)
        ae = 0.25 * me * (u0 + ue)
        aw = 0.25 * mw * (u0 + uw)
        an = 0.25 * mn * (v0 + vn)
        as_ = 0.25 * ms * (v0 + vs)
        ge, gw, gn, gs = DIFFUSION * me, DIFFUSION * mw, DIFFUSION * mn, DIFFUSION * ms

        def tracer(x, ref, flux_above):
            c, e, w, n, so = x
            total = aw * (w + c) - gw * (c - w) - ae * (c + e) + ge * (e - c)
            total = total + as_ * (so + c) - gs * (c - so) - an * (c + n) + gn * (n - c)
            flux = below * (ref[nxt] - c)
            return mc * (c + total + inv_h * (flux - flux_above)), flux

        new_t, flux_t = tracer(t, t_ref, flux_t)
        new_s, flux_s = tracer(s, s_ref, flux_s)
        ot_ref[k] = new_t
        os_ref[k] = new_s
        for m, (out, slope) in enumerate(((ou_ref, slope_u), (ov_ref, slope_v))):
            star = out[k] + gate(near_ew, kf, beyond_ew(2 + m, k)) + gate(near_ns, kf, beyond_ns(m, k))
            out[k] = gate(depth, kf, star - slope)
        return flux_t, flux_s

    def tracer_chunk(c, carry):
        for i in range(KC):
            carry = tracers(c, i, carry)
        return carry

    lax.fori_loop(0, NC, tracer_chunk, (zero,) * 2)

    drain(pack_out, send_sem.at[0])

    sent = pack_in.at[0, 0:3 * NI]

    @pl.when(not_south)
    def _():
        drain(sent, send_sem.at[1])

    drain(sent, send_sem.at[2])

    used = pl.ds(0, NI)
    drain(tiles.at[pl.ds(0, n_lon - 1), pl.ds(0, (EARLY + LATE) * NI + 6)], cast_send.at[0])

    @pl.when(not_south)
    def _():
        drain(rims.at[0, pl.ds(0, n_lon), used], cast_send.at[1])

    @pl.when(not_pole)
    def _():
        drain(rims.at[0, pl.ds(0, n_lon), used], cast_send.at[2])

    @pl.when(at_pole)
    def _():
        drain(rims.at[0, pl.ds(0, n_lon - 1), used], cast_send.at[2])

    drain(sums.at[pl.ds(0, n_lat - 1)], cast_recv.at[2, 0])
    total = functools.reduce(lambda a, b: a + b, [sums[lat] for lat in range(n_lat)])
    ox_ref[1] = jnp.sqrt(total / (n_lon * NI * n_lat * NJ) + EPSILON)
    drain(sums.at[pl.ds(0, n_lat - 1)], cast_send.at[3])


def surface_solve(load, rim_rows, late_wait, share, n_lon, K, NI, NJ):
    width = NJ // NI
    tiles = range(2)
    lines = range(NI)
    lane = iota((n_lon, NJ), 1)
    edge = jnp.logical_or(lane == 0, lane == NJ - 1)

    def every(fn, *arrays):
        return [[fn(*(a[b][s] for a in arrays)) for s in lines] for b in tiles]

    def east(x):
        return [x[b][1:] + [pltpu.roll(x[b][0], n_lon - 1, 0)] for b in tiles]

    def west(x):
        return [[pltpu.roll(x[b][NI - 1], 1, 0)] + x[b][:-1] for b in tiles]

    def joined(x, shift, edge):
        moved = [[pltpu.roll(x[b][s], shift, 1) for s in lines] for b in tiles]
        return [[jnp.where(lane == edge, moved[1 - b][s], moved[b][s]) for s in lines] for b in tiles]

    def north(x):
        return joined(x, NJ - 1, NJ - 1)

    def south(x):
        return joined(x, 1, 0)

    height = load(0)
    scale = lambda a, c: jnp.minimum(a, c) * (1.0 / K)
    w_e = every(scale, height, east(height))
    w_w = every(scale, height, west(height))
    w_n = every(scale, height, north(height))
    w_s = every(scale, height, south(height))
    diag = every(lambda a, b, c, d: STORAGE + a + b + c + d, w_e, w_w, w_n, w_s)

    def apply(x):
        return every(
            lambda dg, c, we, e, ww, w, wn, n, ws, s: dg * c - (we * e + ww * w + wn * n + ws * s),
            diag, x, w_e, east(x), w_w, west(x), w_n, north(x), w_s, south(x))

    middle = NI // 2
    spans = [(s, s - 1, s + 1) for s in range(middle)]
    spans += [(s, s + 1, s - 1) for s in range(NI - 1, middle - 1, -1)]
    pivots, carries, factors = ([[None] * NI for _ in tiles] for _ in range(3))
    joints = []
    for b in tiles:
        for s, before, after in spans:
            back, ahead = (w_w, w_e) if after > s else (w_e, w_w)
            pivot = diag[b][s]
            if s not in (0, NI - 1):
                pivot = pivot + back[b][s] * factors[b][before]
            pivots[b][s] = 1.0 / pivot
            carries[b][s] = back[b][s] * pivots[b][s]
            factors[b][s] = -ahead[b][s] * pivots[b][s]
        joints.append(1.0 / (1.0 - factors[b][middle - 1] * factors[b][middle]))

    def precondition(r):
        out = []
        for b in tiles:
            part = [None] * NI
            for s, before, after in spans:
                part[s] = r[b][s] * pivots[b][s]
                if s not in (0, NI - 1):
                    part[s] = part[s] + carries[b][s] * part[before]
            low, high = part[middle - 1], part[middle]
            part[middle - 1] = (low - factors[b][middle - 1] * high) * joints[b]
            part[middle] = (high - factors[b][middle] * low) * joints[b]
            for s in range(middle - 2, -1, -1):
                part[s] = part[s] - factors[b][s] * part[s + 1]
            for s in range(middle + 1, NI):
                part[s] = part[s] - factors[b][s] * part[s - 1]
            out.append(part)
        return out

    x = load(1)
    drive = load(2)
    start = every(lambda h, d, a: jnp.where(h > 0.0, d, 0.0) - a, height, drive, apply(x))
    late_wait()
    t_u = load(EARLY)
    t_v = load(EARLY + 1)
    inner, outer = load(EARLY + LATE)
    for m, t in enumerate((t_u, t_v)):
        for b, (from_w, from_e) in enumerate(((inner[2 * m], inner[2 * m + 1]), (outer[m], outer[NI - 1 - m]))):
            t[b][NI - 1] = t[b][NI - 1] + pltpu.roll(from_w, n_lon - 1, 0)
            t[b][0] = t[b][0] + pltpu.roll(from_e, 1, 0)
        own, beyond = inner[4 + m], rim_rows(EARLY + LATE + 1 + m)
        for s in lines:
            for b, row in ((0, beyond), (1, own)):
                moved = pltpu.roll(row, (NJ - width * s) % NJ, 1) if s else row
                t[b][s] = t[b][s] + jnp.where(edge, moved, 0.0)
    residual = every(
        lambda h, d, e, w, n, s: d - jnp.where(h > 0.0, 0.5 * DIVERGENCE * ((e - w) + (n - s)), 0.0),
        height, start, east(t_u), west(t_u), north(t_v), south(t_v))
    mid = 0.5 * (SPECTRUM_HIGH + SPECTRUM_LOW)
    half = 0.5 * (SPECTRUM_HIGH - SPECTRUM_LOW)
    ratio = mid / half
    direction = every(lambda a: a / mid, precondition(residual))
    rho = 1.0 / ratio
    for step in range(ITERS):
        x = every(lambda a, b: a + b, x, direction)
        residual = every(lambda a, b: a - b, residual, apply(direction))
        if step + 1 < ITERS:
            rho_next = 1.0 / (2.0 * ratio - rho)
            keep, gain = rho_next * rho, 2.0 * rho_next / half
            direction = every(lambda d, z: keep * d + gain * z, direction, precondition(residual))
            rho = rho_next
    squares = functools.reduce(lambda a, b: a + b, [a * a for a in residual[0]])
    share(jnp.sum(jnp.sum(squares, axis=1, keepdims=True), axis=0, keepdims=True))
    slope_x = every(lambda e, w: 0.5 * (e - w), east(x), west(x))
    slope_y = every(lambda n, s: 0.5 * (n - s), north(x), south(x))
    return x[0], slope_x[0], slope_y[0]


def finish_kernel(kept, x_ref, ot_ref, os_ref, ou_ref, ov_ref, ox_ref, orms_ref, rms, sem):
    for f, target in enumerate((ot_ref, os_ref, ou_ref, ov_ref)):
        pltpu.make_async_copy(kept.at[f], target, sem.at[0]).start()
    surface = pltpu.make_async_copy(x_ref.at[0], ox_ref, sem.at[1])
    surface.start()
    rms[0] = jnp.max(x_ref[1])
    scalar = pltpu.make_async_copy(rms, orms_ref, sem.at[2])
    scalar.start()
    pltpu.make_async_copy(kept, kept, sem.at[0]).wait()
    surface.wait()
    scalar.wait()


def per_device(n_lon, n_lat, *args):
    K, NI, NJ = args[0].shape
    KC = 8 if K % 8 == 0 else K
    NC = K // KC
    vmem = pl.BlockSpec(memory_space=pltpu.VMEM)
    hbm = pl.BlockSpec(memory_space=pltpu.HBM)
    big = jax.ShapeDtypeStruct((K, NI, NJ), F32)
    tile = jax.ShapeDtypeStruct((NI, NJ), F32)
    one = jax.ShapeDtypeStruct((1,), F32)
    pack = pltpu.VMEM((2, NI + NC * 2 * KC + 4 * K, NJ), F32)

    def room(*lead):
        return pltpu.VMEM((*lead, NI, NJ), F32)

    parts = pl.pallas_call(
        functools.partial(step_kernel, n_lon, n_lat, KC),
        out_shape=(room(4, K), room(2)),
        in_specs=[hbm] * 9,
        out_specs=(vmem,) * 2,
        scratch_shapes=[
            room(4, K), pltpu.VMEM((2, NI, NJ), jnp.int32), room(2), pltpu.SMEM((K,), F32),
            pack, pack, room(2, 2), room(2, 2), room(2), room(2), room(4),
            room(2, K), room(K), pltpu.VMEM((n_lon, TILES * NI, NJ), F32), room(2), room(2, n_lon), room(n_lat),
            pltpu.VMEM((3, n_lon * NI, NJ), F32),
            pltpu.SemaphoreType.DMA((3,)), pltpu.SemaphoreType.DMA((3,)), pltpu.SemaphoreType.DMA((NC + 2,)),
            pltpu.SemaphoreType.DMA((4,)), pltpu.SemaphoreType.DMA((4,)), pltpu.SemaphoreType.DMA((3, 3)),
        ],
        compiler_params=pltpu.CompilerParams(
            collective_id=0, has_side_effects=True),
        name="step",
    )(*args)
    outs = pl.pallas_call(
        finish_kernel,
        out_shape=(big, big, big, big, tile, one),
        in_specs=[vmem] * 2,
        out_specs=(hbm,) * 6,
        scratch_shapes=[pltpu.SMEM((1,), F32), pltpu.SemaphoreType.DMA((3,))],
        name="finish",
    )(*[pltpu.with_memory_space_constraint(part, pltpu.VMEM) for part in parts])
    return outs[:5] + (outs[5].reshape(()),)


def solution(mesh):
    n_lon, n_lat = mesh.shape["lon"], mesh.shape["lat"]
    spec3 = P(None, "lon", "lat")
    spec2 = P("lon", "lat")
    return jax.shard_map(
        functools.partial(per_device, n_lon, n_lat),
        mesh=mesh,
        in_specs=(spec3, spec3, spec3, spec3, spec2, spec2, P(), spec2, spec2),
        out_specs=(spec3, spec3, spec3, spec3, spec2, P()),
        check_vma=False,
    )
```

```python
import functools

import jax
import jax.numpy as jnp
from jax import lax
from jax.experimental import pallas as pl
from jax.experimental.pallas import tpu as pltpu
from jax.sharding import PartitionSpec as P

ITERS = 4
DIFFUSION = 0.15
MIXING = 0.1
EXPANSION = 0.2
CONTRACTION = 0.15
PRESSURE_SCALE = 0.02
CORIOLIS = 0.5
FRICTION = 0.01
DIVERGENCE = 0.3
STORAGE = 0.1
SPECTRUM_LOW = 0.1
SPECTRUM_HIGH = 1.9
GRAVITY = 0.3
EPSILON = 1e-06

MESH = pl.DeviceIdType.MESH
F32 = jnp.float32
EARLY = 3
LATE = 2
TILES = EARLY + LATE + 1


def iota(shape, axis):
    return lax.broadcasted_iota(jnp.int32, shape, axis)


def flip(x, axis):
    return jnp.take_along_axis(x, x.shape[axis] - 1 - iota(x.shape, axis), axis=axis)


def flip_rows(x):
    return flip(x, 0)


def flip_lanes(x):
    return flip(x, 1)


def step_kernel(n_lon, n_lat, KC, *refs):
    sources, refs = refs[:9], refs[9:]
    (kept, ox_ref), refs = refs[:2], refs[2:]
    (fields, ints, floats, thick_ref, pack_out, pack_in, edges, slots, lap_edges, lap_slots, rim, laps, pressure, tiles, strips,
     rims, sums, held, load_sem, send_sem, chunk_sem, edge_sem, cast_send, cast_recv) = refs
    _, K, NI, NJ = fields.shape
    NC = K // KC
    SIDE = 2 * KC
    REST = NI + NC * SIDE
    t_ref, s_ref, u_ref, v_ref = (fields.at[f] for f in range(4))
    ot_ref, os_ref, ou_ref, ov_ref = (kept.at[f] for f in range(4))
    num_ref, sea_ref, eta_ref, drive_ref = ints.at[0], ints.at[1], floats.at[0], floats.at[1]
    p = lax.axis_index("lon")
    q = lax.axis_index("lat")
    east_dev = lax.rem(p + 1, n_lon)
    west_dev = lax.rem(p + n_lon - 1, n_lon)
    at_pole = q == n_lat - 1
    not_pole = q < n_lat - 1
    not_south = q > 0
    mirror = n_lon - 1 - p
    lons = [lax.rem(p + r, n_lon) for r in range(min(n_lon, 8))]

    barrier = pltpu.get_barrier_semaphore()

    def greet(lon, lat):
        pl.semaphore_signal(barrier, inc=1, device_id={"lon": lon, "lat": lat}, device_id_type=MESH)

    greet(east_dev, q)
    if n_lon > 2:
        greet(west_dev, q)

    def around_lon(first, last, fn):
        def visit(r, carry):
            fn(lax.rem(p + r, n_lon))
            return carry

        if n_lon <= 8:
            for lon in lons[first:last]:
                fn(lon)
        else:
            lax.fori_loop(first, last, visit, 0)

    @pl.when(at_pole)
    def _():
        around_lon(2, n_lon - 1, lambda lon: greet(lon, q))

    @pl.when(not_south)
    def _():
        around_lon(0, n_lon, lambda lon: greet(lon, q - 1))

    @pl.when(not_pole)
    def _():
        around_lon(0, n_lon, lambda lon: greet(lon, q + 1))

    def load(i, dst, sem):
        pltpu.make_async_copy(sources[i], dst, load_sem.at[sem]).start()

    load(4, num_ref, 1)
    load(5, sea_ref, 1)
    load(7, eta_ref, 1)
    load(8, drive_ref, 1)
    for f in (2, 3, 0, 1):
        load(f, fields.at[f], 0)
    thick_load = pltpu.make_async_copy(sources[6], thick_ref, load_sem.at[2])
    thick_load.start()

    @pl.when(not_pole)
    def _():
        around_lon(2, n_lon - 1, lambda lon: greet(lon, q))

    for lat in range(n_lat):
        @pl.when(jnp.logical_or(q - lat > 1, lat - q > 1))
        def _():
            greet(p, lat)

    def drain(ref, sem):
        pltpu.make_async_copy(ref, ref, sem).wait()

    thick_load.wait()
    drain(fields.at[0, 0:4], load_sem.at[1])
    drain(fields, load_sem.at[0])
    sub = iota((NI, NJ), 0)
    lane = iota((NI, NJ), 1)
    depth = (num_ref[...] * sea_ref[...]).astype(F32)

    for side, d1 in enumerate((NI - 1, 0)):
        for c in range(NC):
            levels = slice(c * KC, (c + 1) * KC)
            for m, ref in enumerate((u_ref, v_ref)):
                row = NI + c * SIDE + m * KC
                pack_out[side, row:row + KC, :] = ref[levels, d1, :]
        for m, ref in enumerate((t_ref, s_ref)):
            row = REST + m * K
            pack_out[side, row:row + K, :] = ref[:, d1, :]
        pack_out[side, 0:NI, :] = jnp.broadcast_to(depth[d1:d1 + 1, :], (NI, NJ))

    zero = jnp.zeros((NI, NJ), F32)

    def put(acc, x, source, target):
        moved = pltpu.roll(x, (target - source) % NJ, 1) if source != target else x
        return jnp.where(lane == target, moved, acc)

    n0 = s0 = zero
    for f, ref in enumerate((t_ref, s_ref, u_ref, v_ref)):
        for k in range(K):
            n0 = put(n0, ref[k], NJ - 1, f * K + k)
            s0 = put(s0, ref[k], 0, f * K + k)
    npk, spk = edges.at[0], edges.at[1]
    npk[0] = n0
    npk[1] = put(zero, depth, NJ - 1, 0)
    spk[0] = s0
    spk[1] = put(zero, depth, 0, 0)

    peers = n_lon + n_lat - 2 + (n_lon - 1) * (not_south.astype(jnp.int32) + not_pole.astype(jnp.int32))
    pl.semaphore_wait(barrier, peers)

    def copy(src, dst, lon, lat, out, into):
        return pltpu.make_async_remote_copy(
            src_ref=src, dst_ref=dst, send_sem=out, recv_sem=into,
            device_id={"lon": lon, "lat": lat}, device_id_type=MESH)

    def meet_pole(pack, slot, sem):
        @pl.when(at_pole)
        def _():
            copy(pack.at[0], slot.at[0], mirror, q, send_sem.at[2], edge_sem.at[sem]).start()

    def meet_near(pack, slot, sem):
        @pl.when(not_south)
        def _():
            copy(pack.at[1], slot.at[0], p, q - 1, send_sem.at[1], edge_sem.at[sem]).start()

        @pl.when(not_pole)
        def _():
            copy(pack.at[0], slot.at[1], p, q + 1, send_sem.at[2], edge_sem.at[sem + 1]).start()

    def met(slot, sem):
        drain(slot.at[0], edge_sem.at[sem])

        @pl.when(not_south)
        def _():
            drain(slot.at[1], edge_sem.at[sem + 1])

    meet_pole(edges, slots, 0)

    def aside(way, first, rows, sem):
        rows = pl.ds(first, rows)
        lon = west_dev if way else east_dev
        copy(pack_out.at[way, rows], pack_in.at[1 - way, rows], lon, q, send_sem.at[0], chunk_sem.at[sem]).start()

    def sides(first, rows, sem):
        aside(1, first, rows, sem)
        aside(0, first, rows, sem)

    half = (NC + 1) // 2
    bounds = ((0, NI + half * SIDE), (NI + half * SIDE, REST)) if NC > 1 else ((0, REST),)
    for way in (1, 0):
        for i, (first, last) in enumerate(bounds):
            aside(way, first, last - first, i)
    meet_near(edges, slots, 0)

    height = zero
    for k in range(K):
        height = height + jnp.where(depth > k + 0.5, thick_ref[k], 0.0)
    width = NJ // NI
    in_block = lane // width == sub
    parts = ((0, EARLY, EARLY * NI), (EARLY, LATE + 3, LATE * NI + 6))

    def pack_strips(which, sign, arrays, rows=()):
        first, count, _ = parts[which]
        given = len(arrays)
        south = zero
        north = zero
        for i, x in enumerate(arrays):
            for start in (0, width):
                moved = pltpu.roll(x, start, 1, stride=width, stride_axis=0)
                row = jnp.sum(jnp.where(in_block, moved, 0.0), axis=0, keepdims=True)
                row = jnp.broadcast_to(row, (NI, NJ))
                if start:
                    north = jnp.where(sub == i, row, north)
                else:
                    south = jnp.where(sub == i, row, south)
        for i, row in enumerate(rows):
            north = jnp.where(sub == given + i, row, north)
            south = jnp.where(sub == given + i, row, south)
        turned = jnp.where(sub >= given, pltpu.roll(north, width, 1), north) if rows else north
        north = jnp.where(at_pole, sign * flip_lanes(turned), north)
        rows = slice(first, first + count)
        strips[0, rows] = south[:count]
        strips[1, rows] = north[:count]

        @pl.when(at_pole)
        def _():
            rims[0, mirror, rows] = north[:count]

    def each_other(fn):
        def visit(r, carry):
            fn(jnp.where(r <= p, r - 1, r))
            return carry

        if n_lon <= 8:
            for r in range(1, n_lon):
                visit(r, 0)
        else:
            lax.fori_loop(1, n_lon, visit, 0)

    def cast(which):
        first, count, size = parts[which]
        mine = tiles.at[p, pl.ds(first * NI, size)]
        rows = pl.ds(first, count)
        pole = at_pole.astype(jnp.int32)
        side, lat = 1 - pole, q + 1 - pole
        slot = jnp.where(at_pole, mirror, p)

        def send(way, side, slot, lon, lat, out):
            copy(strips.at[way, rows], rims.at[side, slot, rows], lon, lat, cast_send.at[out],
                 cast_recv.at[3 * which + 1 + side]).start()

        @pl.when(not_pole)
        def _():
            send(1, 1, p, p, q + 1, 2)

        @pl.when(not_south)
        def _():
            send(0, 0, p, p, q - 1, 1)

        def to(lon):
            @pl.when(not_south)
            def _():
                send(0, 0, p, lon, q - 1, 1)

            send(1, side, slot, lon, lat, 2)
            copy(mine, mine, lon, q, cast_send.at[0], cast_recv.at[3 * which]).start()

        each_other(to)

    def cast_wait(which):
        first, count, size = parts[which]
        rows = pl.ds(first, count)
        drain(tiles.at[pl.ds(0, n_lon - 1), pl.ds(first * NI, size)], cast_recv.at[3 * which])

        @pl.when(at_pole)
        def _():
            drain(rims.at[0, pl.ds(0, n_lon - 1), rows], cast_recv.at[3 * which + 1])

        @pl.when(not_pole)
        def _():
            drain(rims.at[0, pl.ds(0, n_lon), rows], cast_recv.at[3 * which + 1])

        @pl.when(not_south)
        def _():
            drain(rims.at[1, pl.ds(0, n_lon), rows], cast_recv.at[3 * which + 2])

    first_guess = sea_ref[...].astype(F32) * eta_ref[...]
    for i, x in enumerate((height, first_guess, drive_ref[...])):
        tiles[p, i * NI:(i + 1) * NI] = x
    pack_strips(0, 1.0, (height, first_guess, drive_ref[...]))

    near_e = jnp.where(sub == NI - 1, 0.0, jnp.minimum(depth, pltpu.roll(depth, NI - 1, 0)))
    near_w = jnp.where(sub == 0, 0.0, jnp.minimum(depth, pltpu.roll(depth, 1, 0)))
    near_n = jnp.where(lane == NJ - 1, 0.0, jnp.minimum(depth, pltpu.roll(depth, NJ - 1, 1)))
    near_s = jnp.where(lane == 0, 0.0, jnp.minimum(depth, pltpu.roll(depth, 1, 1)))
    lat_index = (q * NJ + lane).astype(F32)
    coriolis = CORIOLIS * (2.0 * (lat_index + 0.5) / (n_lat * NJ) - 1.0)

    def gate(d, kf, x):
        return jnp.where(d > kf, x, 0.0)

    def inner_lap(x, kf):
        total = gate(near_e, kf, pltpu.roll(x, NI - 1, 0) - x) + gate(near_w, kf, pltpu.roll(x, 1, 0) - x)
        return total + (gate(near_n, kf, pltpu.roll(x, NJ - 1, 1) - x) + gate(near_s, kf, pltpu.roll(x, 1, 1) - x))

    def before_level(k, carry):
        pc, tu, tv = carry
        kf = lax.convert_element_type(k, F32) + 0.5
        u, v = u_ref[k], v_ref[k]
        laps[0, k] = inner_lap(u, kf)
        laps[1, k] = inner_lap(v, kf)
        pc = pc + gate(depth, kf, (CONTRACTION * s_ref[k] - EXPANSION * t_ref[k]) * thick_ref[k])
        pressure[k] = pc
        grad_x = gate(near_e, kf, pltpu.roll(pc, NI - 1, 0) - pc) + gate(near_w, kf, pc - pltpu.roll(pc, 1, 0))
        grad_y = gate(near_n, kf, pltpu.roll(pc, NJ - 1, 1) - pc) + gate(near_s, kf, pc - pltpu.roll(pc, 1, 1))
        u_part = u + coriolis * v - (0.5 * PRESSURE_SCALE) * grad_x
        v_part = v - coriolis * u - (0.5 * PRESSURE_SCALE) * grad_y
        ou_ref[k] = u_part
        ov_ref[k] = v_part
        h = thick_ref[k]
        return pc, tu + gate(depth, kf, h * u_part), tv + gate(depth, kf, h * v_part)

    def before_chunk(c, carry):
        for i in range(KC):
            carry = before_level(c * KC + i, carry)
        return carry

    totals = list(lax.fori_loop(0, NC, before_chunk, (zero,) * 3)[1:])

    cast(0)
    met(slots, 0)

    sign = jnp.where(lane >= 2 * K, -1.0, 1.0).astype(F32)

    def arrived(slot, i, fold):
        north = jnp.where(at_pole, flip_rows(slot[0, i]) * fold, slot[0, i])
        return north, jnp.where(not_south, slot[1, i], 0.0)

    pn0, ps0 = arrived(slots, 0, sign)
    pn1, ps1 = arrived(slots, 1, 1.0)

    def shift_e(x, row):
        return jnp.where(sub == NI - 1, row, pltpu.roll(x, NI - 1, 0))

    def shift_w(x, row):
        return jnp.where(sub == 0, row, pltpu.roll(x, 1, 0))

    rim[0] = pn0
    rim[1] = ps0

    drain(pack_in.at[:, bounds[0][0]:bounds[0][1]], chunk_sem.at[0])
    sides(REST, 2 * K, 2)
    base_e = pack_in[0, 0:1, :]
    base_w = pack_in[1, 0:1, :]
    is_w = sub == 0
    is_s = lane == 0
    depth_ew = jnp.where(is_w, base_w, base_e)
    depth_ns = jnp.where(is_s, ps1, pltpu.roll(pn1, NJ - 1, 1))
    on_ew = jnp.logical_or(is_w, sub == NI - 1)
    on_ns = jnp.logical_or(is_s, lane == NJ - 1)
    near_ew = jnp.where(on_ew, jnp.minimum(depth, depth_ew), 0.0)
    near_ns = jnp.where(on_ns, jnp.minimum(depth, depth_ns), 0.0)
    scale_ew = jnp.where(is_w, 0.5 * PRESSURE_SCALE, -0.5 * PRESSURE_SCALE)
    scale_ns = jnp.where(is_s, 0.5 * PRESSURE_SCALE, -0.5 * PRESSURE_SCALE)

    def rim_ns(north, south, k):
        x = pltpu.roll(north, (NJ - 1 - k) % NJ, 1)
        return jnp.where(is_s, pltpu.roll(south, (NJ - k) % NJ, 1), x)

    def side_ew(c, row):
        row = NI + c * SIDE + row
        return jnp.where(is_w, pack_in[1, row:row + 1, :], pack_in[0, row:row + 1, :])

    both_e = jnp.where(sub == NI - 1, near_ew, near_e)
    both_w = jnp.where(is_w, near_ew, near_w)
    both_n = jnp.where(lane == NJ - 1, near_ns, near_n)
    both_s = jnp.where(is_s, near_ns, near_s)
    overlaps = (both_e, both_w, both_n, both_s)
    sums_lap = [[zero] * 4 for _ in range(2)]
    push_ew = push_ns = zero
    for c in range(NC):
        if c == half and NC > 1:
            drain(pack_in.at[:, bounds[1][0]:bounds[1][1]], chunk_sem.at[1])
        for i in range(KC):
            k = c * KC + i
            kf = k + 0.5
            h = thick_ref[k]
            hp = h * pressure[k]
            push_ew = push_ew + gate(near_ew, kf, hp)
            push_ns = push_ns + gate(near_ns, kf, hp)
            for m, x in enumerate((u_ref[k], v_ref[k])):
                lap = laps[m, k] + gate(near_ew, kf, side_ew(c, m * KC + i) - x)
                lap = lap + gate(near_ns, kf, rim_ns(rim[0], rim[1], (2 + m) * K + k) - x)
                laps[m, k] = lap
                hl = h * lap
                sums_lap[m] = [a + gate(d, kf, hl) for a, d in zip(sums_lap[m], overlaps)]
    push_ew = scale_ew * push_ew
    push_ns = scale_ns * push_ns
    exports, exports_ns = [], []
    for m, (a_e, a_w, a_n, a_s) in enumerate(sums_lap):
        given = jnp.where(sub == NI - 1, 0.0, pltpu.roll(a_w, NI - 1, 0)) + jnp.where(is_w, 0.0, pltpu.roll(a_e, 1, 0))
        given = given + jnp.where(lane == NJ - 1, 0.0, pltpu.roll(a_s, NJ - 1, 1))
        given = given + jnp.where(is_s, 0.0, pltpu.roll(a_n, 1, 1))
        totals[m] = totals[m] + FRICTION * ((a_e + a_w) + (a_n + a_s) - given)
        exports.append(-FRICTION * jnp.where(is_w, a_w, a_e))
        exports_ns.append(-FRICTION * jnp.where(is_s, a_s, a_n))
    totals = [totals[0] - push_ew, totals[1] - push_ns]
    exports[0] = exports[0] - push_ew
    exports_ns[1] = exports_ns[1] - push_ns

    tiles[p, EARLY * NI:(EARLY + 1) * NI] = totals[0]
    tiles[p, (EARLY + 1) * NI:(EARLY + 2) * NI] = totals[1]
    for m in range(2):
        row = (EARLY + LATE) * NI + 2 * m
        tiles[p, row:row + 1] = exports[m][0:1]
        tiles[p, row + 1:row + 2] = exports[m][NI - 1:]
    out_rows = zero
    for row, x in ((0, exports[0][0:1]), (1, exports[1][0:1]), (NI - 2, exports[1][NI - 1:]), (NI - 1, exports[0][NI - 1:])):
        out_rows = jnp.where(sub == row, jnp.broadcast_to(x, (NI, NJ)), out_rows)
    ns_rows = []
    for m, x in enumerate(exports_ns):
        x = jnp.where(lane == 0, pltpu.roll(x, 1, 1), jnp.where(lane == NJ - 1, pltpu.roll(x, NJ - 1, 1), 0.0))
        x = jnp.sum(pltpu.roll(x, 0, 1, stride=width, stride_axis=0), axis=0, keepdims=True)
        row = (EARLY + LATE) * NI + 4 + m
        tiles[p, row:row + 1] = x
        ns_rows.append(jnp.broadcast_to(x, (NI, NJ)))
    pack_strips(1, -1.0, (*totals, out_rows), ns_rows)
    cast(1)

    for side, (d, push) in enumerate(((NI - 1, 0.5 * PRESSURE_SCALE), (0, -0.5 * PRESSURE_SCALE))):
        row = REST + 2 * K
        pack_out[side, row:row + K, :] = push * pressure[:, d, :] - FRICTION * laps[0, :, d, :]
        pack_out[side, row + K:row + 2 * K, :] = -FRICTION * laps[1, :, d, :]
    n2 = s2 = zero
    for k in range(K):
        for m, x in enumerate((-FRICTION * laps[0, k], -FRICTION * laps[1, k] - scale_ns * pressure[k])):
            n2 = put(n2, x, NJ - 1, m * K + k)
            s2 = put(s2, x, 0, m * K + k)
    lap_edges[0] = n2
    lap_edges[1] = s2
    meet_pole(lap_edges, lap_slots, 2)
    meet_near(lap_edges, lap_slots, 2)
    sides(REST + 2 * K, 2 * K, 3)

    def level(c, carry):
        for i in range(KC):
            k = c * KC + i
            kf = lax.convert_element_type(k, F32) + 0.5
            pc = pressure[k]
            parts = (ou_ref[k] - scale_ew * gate(near_ew, kf, pc), ov_ref[k] - scale_ns * gate(near_ns, kf, pc))
            for m, (part, out) in enumerate(zip(parts, (ou_ref, ov_ref))):
                lap = laps[m, k]
                inner = inner_lap(lap, kf) - gate(near_ew, kf, lap) - gate(near_ns, kf, lap)
                out[k] = gate(depth, kf, part - FRICTION * inner)
        return carry

    lax.fori_loop(0, NC, level, 0)

    cast_wait(0)
    flat = tiles.reshape(n_lon * TILES * NI, NJ)
    flat_rim = rims.reshape(2 * n_lon * NI, NJ)
    lanes = iota((n_lon, NJ), 1)

    def loader(f):
        main = [flat[pl.ds(f * NI + s, n_lon, stride=TILES * NI), :] for s in range(NI)]
        north = flat_rim[pl.ds(f, n_lon, stride=NI), :]
        south = jnp.where(not_south, flat_rim[pl.ds(n_lon * NI + f, n_lon, stride=NI), :], 0.0)
        outer = []
        for s in range(NI):
            x = jnp.where(lanes >= NJ - width, pltpu.roll(south, (NJ - width - width * s) % NJ, 1), 0.0)
            outer.append(jnp.where(lanes < width, pltpu.roll(north, (NJ - width * s) % NJ, 1), x))
        return [main, outer]

    def rim_rows(f):
        north = flat_rim[pl.ds(f, n_lon, stride=NI), :]
        south = jnp.where(not_south, flat_rim[pl.ds(n_lon * NI + f, n_lon, stride=NI), :], 0.0)
        return jnp.where(lanes % width == width - 1, north, south)

    def share(total):
        sums[q] = jnp.broadcast_to(total, (NI, NJ))
        for r in range(1, n_lat):
            lat = lax.rem(q + r, n_lat)
            copy(sums.at[q], sums.at[q], p, lat, cast_send.at[3], cast_recv.at[6]).start()


    def late_wait():
        cast_wait(1)

    x, slope_x, slope_y = surface_solve(loader, rim_rows, late_wait, share, n_lon, K, NI, NJ)
    for i, field in enumerate((x, slope_x, slope_y)):
        for s in range(NI):
            held[i, pl.ds(s, n_lon, stride=NI), :] = field[s]
    block = pl.ds(pl.multiple_of(p * NI, NI), NI)
    ox_ref[0] = held[0, block, :]
    slope_u = GRAVITY * held[1, block, :]
    slope_v = GRAVITY * held[2, block, :]
    drain(pack_in.at[:, REST:REST + 2 * K], chunk_sem.at[2])
    drain(pack_in.at[:, REST + 2 * K:], chunk_sem.at[3])
    met(lap_slots, 2)
    rim[2] = jnp.where(at_pole, -flip_rows(lap_slots[0]), lap_slots[0])
    rim[3] = jnp.where(not_south, lap_slots[1], 0.0)
    def shift_n(x, packed, source):
        return jnp.where(lane == NJ - 1, pltpu.roll(packed, NJ - 1 - source, 1), pltpu.roll(x, NJ - 1, 1))

    def shift_s(x, packed, source):
        return jnp.where(lane == 0, pltpu.roll(packed, lax.rem(NJ - source, NJ), 1), pltpu.roll(x, 1, 1))

    def around(c, inner, ref, f):
        k = c * KC + inner
        x = ref[k]
        row = pl.ds(NI + c * SIDE + (f - 2) * KC + inner if f >= 2 else REST + f * K + k, 1)
        return (x, shift_e(x, pack_in[0, row, :]), shift_w(x, pack_in[1, row, :]),
                shift_n(x, rim[0], f * K + k), shift_s(x, rim[1], f * K + k))

    def beyond_ew(f, k):
        row = pl.ds(REST + f * K + k, 1)
        return jnp.where(is_w, pack_in[1, row, :], pack_in[0, row, :])

    def beyond_ns(f, k):
        at = f * K + k
        north = pltpu.roll(rim[2], NJ - 1 - at, 1)
        return jnp.where(is_s, pltpu.roll(rim[3], lax.rem(NJ - at, NJ), 1), north)

    def tracers(c, i, carry):
        k = c * KC + i
        flux_t, flux_s = carry
        kf = lax.convert_element_type(k, F32) + 0.5
        h = thick_ref[k]
        nxt = jnp.minimum(k + 1, K - 1)
        h_next = thick_ref[nxt]
        hv = jnp.full((NI, NJ), h, F32)
        inv_space = 1.0 / (0.5 * (hv + h_next))
        inv_h = MIXING / hv

        def wet(d):
            return jnp.where(d > kf, 1.0, 0.0)

        mc = wet(depth)
        me, mw, mn, ms = wet(both_e), wet(both_w), wet(both_n), wet(both_s)
        below = jnp.where(jnp.logical_and(depth > kf + 1.0, k < K - 1), inv_space, 0.0)
        t = around(c, i, t_ref, 0)
        s = around(c, i, s_ref, 1)
        u0, ue, uw = around(c, i, u_ref, 2)[:3]
        v0, _, _, vn, vs = around(c, i, v_ref, 3)
        ae = 0.25 * me * (u0 + ue)
        aw = 0.25 * mw * (u0 + uw)
        an = 0.25 * mn * (v0 + vn)
        as_ = 0.25 * ms * (v0 + vs)
        ge, gw, gn, gs = DIFFUSION * me, DIFFUSION * mw, DIFFUSION * mn, DIFFUSION * ms

        def tracer(x, ref, flux_above):
            c, e, w, n, so = x
            total = aw * (w + c) - gw * (c - w) - ae * (c + e) + ge * (e - c)
            total = total + as_ * (so + c) - gs * (c - so) - an * (c + n) + gn * (n - c)
            flux = below * (ref[nxt] - c)
            return mc * (c + total + inv_h * (flux - flux_above)), flux

        new_t, flux_t = tracer(t, t_ref, flux_t)
        new_s, flux_s = tracer(s, s_ref, flux_s)
        ot_ref[k] = new_t
        os_ref[k] = new_s
        for m, (out, slope) in enumerate(((ou_ref, slope_u), (ov_ref, slope_v))):
            star = out[k] + gate(near_ew, kf, beyond_ew(2 + m, k)) + gate(near_ns, kf, beyond_ns(m, k))
            out[k] = gate(depth, kf, star - slope)
        return flux_t, flux_s

    def tracer_chunk(c, carry):
        for i in range(KC):
            carry = tracers(c, i, carry)
        return carry

    lax.fori_loop(0, NC, tracer_chunk, (zero,) * 2)

    drain(pack_out, send_sem.at[0])

    sent = pack_in.at[0, 0:3 * NI]

    @pl.when(not_south)
    def _():
        drain(sent, send_sem.at[1])

    drain(sent, send_sem.at[2])

    used = pl.ds(0, NI)
    drain(tiles.at[pl.ds(0, n_lon - 1), pl.ds(0, (EARLY + LATE) * NI + 6)], cast_send.at[0])

    @pl.when(not_south)
    def _():
        drain(rims.at[0, pl.ds(0, n_lon), used], cast_send.at[1])

    @pl.when(not_pole)
    def _():
        drain(rims.at[0, pl.ds(0, n_lon), used], cast_send.at[2])

    @pl.when(at_pole)
    def _():
        drain(rims.at[0, pl.ds(0, n_lon - 1), used], cast_send.at[2])

    drain(sums.at[pl.ds(0, n_lat - 1)], cast_recv.at[6])
    total = functools.reduce(lambda a, b: a + b, [sums[lat] for lat in range(n_lat)])
    ox_ref[1] = jnp.sqrt(total / (n_lon * NI * n_lat * NJ) + EPSILON)
    drain(sums.at[pl.ds(0, n_lat - 1)], cast_send.at[3])


def surface_solve(load, rim_rows, late_wait, share, n_lon, K, NI, NJ):
    width = NJ // NI
    tiles = range(2)
    lines = range(NI)
    lane = iota((n_lon, NJ), 1)
    edge = jnp.logical_or(lane == 0, lane == NJ - 1)

    def every(fn, *arrays):
        return [[fn(*(a[b][s] for a in arrays)) for s in lines] for b in tiles]

    def east(x):
        return [x[b][1:] + [pltpu.roll(x[b][0], n_lon - 1, 0)] for b in tiles]

    def west(x):
        return [[pltpu.roll(x[b][NI - 1], 1, 0)] + x[b][:-1] for b in tiles]

    def joined(x, shift, edge):
        moved = [[pltpu.roll(x[b][s], shift, 1) for s in lines] for b in tiles]
        return [[jnp.where(lane == edge, moved[1 - b][s], moved[b][s]) for s in lines] for b in tiles]

    def north(x):
        return joined(x, NJ - 1, NJ - 1)

    def south(x):
        return joined(x, 1, 0)

    height = load(0)
    scale = lambda a, c: jnp.minimum(a, c) * (1.0 / K)
    w_e = every(scale, height, east(height))
    w_w = every(scale, height, west(height))
    w_n = every(scale, height, north(height))
    w_s = every(scale, height, south(height))
    diag = every(lambda a, b, c, d: STORAGE + a + b + c + d, w_e, w_w, w_n, w_s)

    def apply(x):
        return every(
            lambda dg, c, we, e, ww, w, wn, n, ws, s: dg * c - (we * e + ww * w + wn * n + ws * s),
            diag, x, w_e, east(x), w_w, west(x), w_n, north(x), w_s, south(x))

    middle = NI // 2
    spans = [(s, s - 1, s + 1) for s in range(middle)]
    spans += [(s, s + 1, s - 1) for s in range(NI - 1, middle - 1, -1)]
    pivots, carries, factors = ([[None] * NI for _ in tiles] for _ in range(3))
    joints = []
    for b in tiles:
        for s, before, after in spans:
            back, ahead = (w_w, w_e) if after > s else (w_e, w_w)
            pivot = diag[b][s]
            if s not in (0, NI - 1):
                pivot = pivot + back[b][s] * factors[b][before]
            pivots[b][s] = 1.0 / pivot
            carries[b][s] = back[b][s] * pivots[b][s]
            factors[b][s] = -ahead[b][s] * pivots[b][s]
        joints.append(1.0 / (1.0 - factors[b][middle - 1] * factors[b][middle]))

    def precondition(r):
        out = []
        for b in tiles:
            part = [None] * NI
            for s, before, after in spans:
                part[s] = r[b][s] * pivots[b][s]
                if s not in (0, NI - 1):
                    part[s] = part[s] + carries[b][s] * part[before]
            low, high = part[middle - 1], part[middle]
            part[middle - 1] = (low - factors[b][middle - 1] * high) * joints[b]
            part[middle] = (high - factors[b][middle] * low) * joints[b]
            for s in range(middle - 2, -1, -1):
                part[s] = part[s] - factors[b][s] * part[s + 1]
            for s in range(middle + 1, NI):
                part[s] = part[s] - factors[b][s] * part[s - 1]
            out.append(part)
        return out

    x = load(1)
    drive = load(2)
    start = every(lambda h, d, a: jnp.where(h > 0.0, d, 0.0) - a, height, drive, apply(x))
    late_wait()
    t_u = load(EARLY)
    t_v = load(EARLY + 1)
    inner, outer = load(EARLY + LATE)
    for m, t in enumerate((t_u, t_v)):
        for b, (from_w, from_e) in enumerate(((inner[2 * m], inner[2 * m + 1]), (outer[m], outer[NI - 1 - m]))):
            t[b][NI - 1] = t[b][NI - 1] + pltpu.roll(from_w, n_lon - 1, 0)
            t[b][0] = t[b][0] + pltpu.roll(from_e, 1, 0)
        own, beyond = inner[4 + m], rim_rows(EARLY + LATE + 1 + m)
        for s in lines:
            for b, row in ((0, beyond), (1, own)):
                moved = pltpu.roll(row, (NJ - width * s) % NJ, 1) if s else row
                t[b][s] = t[b][s] + jnp.where(edge, moved, 0.0)
    residual = every(
        lambda h, d, e, w, n, s: d - jnp.where(h > 0.0, 0.5 * DIVERGENCE * ((e - w) + (n - s)), 0.0),
        height, start, east(t_u), west(t_u), north(t_v), south(t_v))
    mid = 0.5 * (SPECTRUM_HIGH + SPECTRUM_LOW)
    half = 0.5 * (SPECTRUM_HIGH - SPECTRUM_LOW)
    ratio = mid / half

    def across(d):
        out = every(lambda wn, n, ws, s: wn * n + ws * s, w_n, north(d), w_s, south(d))
        for b in tiles:
            out[b][NI - 1] = out[b][NI - 1] + w_e[b][NI - 1] * pltpu.roll(d[b][0], n_lon - 1, 0)
            out[b][0] = out[b][0] + w_w[b][0] * pltpu.roll(d[b][NI - 1], 1, 0)
        return out

    direction = precondition(residual)
    image = residual
    if mid != 1.0:
        direction, image = (every(lambda a: a / mid, f) for f in (direction, image))
    rho = 1.0 / ratio
    for step in range(ITERS):
        x = every(lambda a, b: a + b, x, direction)
        if step == 0 and mid == 1.0:
            residual = across(direction)
        else:
            residual = every(lambda r, m, c: (r - m) + c, residual, image, across(direction))
        if step + 1 < ITERS:
            rho_next = 1.0 / (2.0 * ratio - rho)
            keep, gain = rho_next * rho, 2.0 * rho_next / half
            direction = every(lambda d, z: keep * d + gain * z, direction, precondition(residual))
            image = every(lambda m, r: keep * m + gain * r, image, residual)
            rho = rho_next
    squares = functools.reduce(lambda a, b: a + b, [a * a for a in residual[0]])
    share(jnp.sum(jnp.sum(squares, axis=1, keepdims=True), axis=0, keepdims=True))
    slope_x = every(lambda e, w: 0.5 * (e - w), east(x), west(x))
    slope_y = every(lambda n, s: 0.5 * (n - s), north(x), south(x))
    return x[0], slope_x[0], slope_y[0]


def finish_kernel(kept, x_ref, ot_ref, os_ref, ou_ref, ov_ref, ox_ref, orms_ref, rms, sem):
    K = kept.shape[1]
    piece = K // 4 if K % 4 == 0 else K
    for f, target in enumerate((ot_ref, os_ref, ou_ref, ov_ref)):
        for first in range(0, K, piece):
            levels = pl.ds(first, piece)
            pltpu.make_async_copy(kept.at[f, levels], target.at[levels], sem.at[0]).start()
    surface = pltpu.make_async_copy(x_ref.at[0], ox_ref, sem.at[1])
    surface.start()
    rms[0] = jnp.max(x_ref[1])
    scalar = pltpu.make_async_copy(rms, orms_ref, sem.at[2])
    scalar.start()
    pltpu.make_async_copy(kept, kept, sem.at[0]).wait()
    surface.wait()
    scalar.wait()


def per_device(n_lon, n_lat, *args):
    K, NI, NJ = args[0].shape
    KC = 8 if K % 8 == 0 else K
    NC = K // KC
    vmem = pl.BlockSpec(memory_space=pltpu.VMEM)
    hbm = pl.BlockSpec(memory_space=pltpu.HBM)
    big = jax.ShapeDtypeStruct((K, NI, NJ), F32)
    tile = jax.ShapeDtypeStruct((NI, NJ), F32)
    one = jax.ShapeDtypeStruct((1,), F32)
    pack = pltpu.VMEM((2, NI + NC * 2 * KC + 4 * K, NJ), F32)

    def room(*lead):
        return pltpu.VMEM((*lead, NI, NJ), F32)

    parts = pl.pallas_call(
        functools.partial(step_kernel, n_lon, n_lat, KC),
        out_shape=(room(4, K), room(2)),
        in_specs=[hbm] * 9,
        out_specs=(vmem,) * 2,
        scratch_shapes=[
            room(4, K), pltpu.VMEM((2, NI, NJ), jnp.int32), room(2), pltpu.SMEM((K,), F32),
            pack, pack, room(2, 2), room(2, 2), room(2), room(2), room(4),
            room(2, K), room(K), pltpu.VMEM((n_lon, TILES * NI, NJ), F32), room(2), room(2, n_lon), room(n_lat),
            pltpu.VMEM((3, n_lon * NI, NJ), F32),
            pltpu.SemaphoreType.DMA((3,)), pltpu.SemaphoreType.DMA((3,)), pltpu.SemaphoreType.DMA((4,)),
            pltpu.SemaphoreType.DMA((4,)), pltpu.SemaphoreType.DMA((4,)), pltpu.SemaphoreType.DMA((7,)),
        ],
        compiler_params=pltpu.CompilerParams(
            collective_id=0, has_side_effects=True),
        name="step",
    )(*args)
    outs = pl.pallas_call(
        finish_kernel,
        out_shape=(big, big, big, big, tile, one),
        in_specs=[vmem] * 2,
        out_specs=(hbm,) * 6,
        scratch_shapes=[pltpu.SMEM((1,), F32), pltpu.SemaphoreType.DMA((3,))],
        name="finish",
    )(*[pltpu.with_memory_space_constraint(part, pltpu.VMEM) for part in parts])
    return outs[:5] + (outs[5].reshape(()),)


def solution(mesh):
    n_lon, n_lat = mesh.shape["lon"], mesh.shape["lat"]
    spec3 = P(None, "lon", "lat")
    spec2 = P("lon", "lat")
    return jax.shard_map(
        functools.partial(per_device, n_lon, n_lat),
        mesh=mesh,
        in_specs=(spec3, spec3, spec3, spec3, spec2, spec2, P(), spec2, spec2),
        out_specs=(spec3, spec3, spec3, spec3, spec2, P()),
        check_vma=False,
    )
```

```python
import functools

import jax
import jax.numpy as jnp
from jax import lax
from jax.experimental import pallas as pl
from jax.experimental.pallas import tpu as pltpu
from jax.sharding import PartitionSpec as P

ITERS = 4
DIFFUSION = 0.15
MIXING = 0.1
EXPANSION = 0.2
CONTRACTION = 0.15
PRESSURE_SCALE = 0.02
CORIOLIS = 0.5
FRICTION = 0.01
DIVERGENCE = 0.3
STORAGE = 0.1
SPECTRUM_LOW = 0.1
SPECTRUM_HIGH = 1.9
GRAVITY = 0.3
EPSILON = 1e-06

MESH = pl.DeviceIdType.MESH
F32 = jnp.float32
EARLY = 3
LATE = 2
TILES = EARLY + LATE + 1


def iota(shape, axis):
    return lax.broadcasted_iota(jnp.int32, shape, axis)


def flip(x, axis):
    return jnp.take_along_axis(x, x.shape[axis] - 1 - iota(x.shape, axis), axis=axis)


def flip_rows(x):
    return flip(x, 0)


def flip_lanes(x):
    return flip(x, 1)


def step_kernel(n_lon, n_lat, KC, *refs):
    sources, refs = refs[:9], refs[9:]
    (kept, ox_ref), refs = refs[:2], refs[2:]
    (fields, ints, floats, thick_ref, pack_out, pack_in, edges, slots, lap_edges, lap_slots, rim, laps, pressure, tiles, strips,
     rims, sums, held, load_sem, send_sem, chunk_sem, edge_sem, cast_send, cast_recv) = refs
    _, K, NI, NJ = fields.shape
    NC = K // KC
    SIDE = 2 * KC
    REST = NI + NC * SIDE
    t_ref, s_ref, u_ref, v_ref = (fields.at[f] for f in range(4))
    ot_ref, os_ref, ou_ref, ov_ref = (kept.at[f] for f in range(4))
    num_ref, sea_ref, eta_ref, drive_ref = ints.at[0], ints.at[1], floats.at[0], floats.at[1]
    p = lax.axis_index("lon")
    q = lax.axis_index("lat")
    east_dev = lax.rem(p + 1, n_lon)
    west_dev = lax.rem(p + n_lon - 1, n_lon)
    at_pole = q == n_lat - 1
    not_pole = q < n_lat - 1
    not_south = q > 0
    mirror = n_lon - 1 - p
    lons = [lax.rem(p + r, n_lon) for r in range(min(n_lon, 8))]

    barrier = pltpu.get_barrier_semaphore()

    def greet(lon, lat):
        pl.semaphore_signal(barrier, inc=1, device_id={"lon": lon, "lat": lat}, device_id_type=MESH)

    greet(east_dev, q)
    if n_lon > 2:
        greet(west_dev, q)

    def around_lon(first, last, fn):
        def visit(r, carry):
            fn(lax.rem(p + r, n_lon))
            return carry

        if n_lon <= 8:
            for lon in lons[first:last]:
                fn(lon)
        else:
            lax.fori_loop(first, last, visit, 0)

    @pl.when(at_pole)
    def _():
        around_lon(2, n_lon - 1, lambda lon: greet(lon, q))

    @pl.when(not_south)
    def _():
        around_lon(0, n_lon, lambda lon: greet(lon, q - 1))

    @pl.when(not_pole)
    def _():
        around_lon(0, n_lon, lambda lon: greet(lon, q + 1))

    def load(i, dst, sem):
        pltpu.make_async_copy(sources[i], dst, load_sem.at[sem]).start()

    load(4, num_ref, 1)
    load(5, sea_ref, 1)
    load(7, eta_ref, 1)
    load(8, drive_ref, 1)
    for f in (2, 3, 0, 1):
        load(f, fields.at[f], 0)
    thick_load = pltpu.make_async_copy(sources[6], thick_ref, load_sem.at[2])
    thick_load.start()

    @pl.when(not_pole)
    def _():
        around_lon(2, n_lon - 1, lambda lon: greet(lon, q))

    for lat in range(n_lat):
        @pl.when(jnp.logical_or(q - lat > 1, lat - q > 1))
        def _():
            greet(p, lat)

    def drain(ref, sem):
        pltpu.make_async_copy(ref, ref, sem).wait()

    thick_load.wait()
    drain(fields.at[0, 0:4], load_sem.at[1])
    drain(fields, load_sem.at[0])
    sub = iota((NI, NJ), 0)
    lane = iota((NI, NJ), 1)
    depth = (num_ref[...] * sea_ref[...]).astype(F32)

    for side, d1 in enumerate((NI - 1, 0)):
        for c in range(NC):
            levels = slice(c * KC, (c + 1) * KC)
            for m, ref in enumerate((u_ref, v_ref)):
                row = NI + c * SIDE + m * KC
                pack_out[side, row:row + KC, :] = ref[levels, d1, :]
        for m, ref in enumerate((t_ref, s_ref)):
            row = REST + m * K
            pack_out[side, row:row + K, :] = ref[:, d1, :]
        pack_out[side, 0:NI, :] = jnp.broadcast_to(depth[d1:d1 + 1, :], (NI, NJ))

    zero = jnp.zeros((NI, NJ), F32)

    def put(acc, x, source, target):
        moved = pltpu.roll(x, (target - source) % NJ, 1) if source != target else x
        return jnp.where(lane == target, moved, acc)

    n0 = s0 = zero
    for f, ref in enumerate((t_ref, s_ref, u_ref, v_ref)):
        for k in range(K):
            n0 = put(n0, ref[k], NJ - 1, f * K + k)
            s0 = put(s0, ref[k], 0, f * K + k)
    npk, spk = edges.at[0], edges.at[1]
    npk[0] = n0
    npk[1] = put(zero, depth, NJ - 1, 0)
    spk[0] = s0
    spk[1] = put(zero, depth, 0, 0)

    peers = n_lon + n_lat - 2 + (n_lon - 1) * (not_south.astype(jnp.int32) + not_pole.astype(jnp.int32))
    pl.semaphore_wait(barrier, peers)

    def copy(src, dst, lon, lat, out, into):
        return pltpu.make_async_remote_copy(
            src_ref=src, dst_ref=dst, send_sem=out, recv_sem=into,
            device_id={"lon": lon, "lat": lat}, device_id_type=MESH)

    def meet_pole(pack, slot, sem):
        @pl.when(at_pole)
        def _():
            copy(pack.at[0], slot.at[0], mirror, q, send_sem.at[2], edge_sem.at[sem]).start()

    def meet_near(pack, slot, sem):
        @pl.when(not_south)
        def _():
            copy(pack.at[1], slot.at[0], p, q - 1, send_sem.at[1], edge_sem.at[sem]).start()

        @pl.when(not_pole)
        def _():
            copy(pack.at[0], slot.at[1], p, q + 1, send_sem.at[2], edge_sem.at[sem + 1]).start()

    def met(slot, sem):
        drain(slot.at[0], edge_sem.at[sem])

        @pl.when(not_south)
        def _():
            drain(slot.at[1], edge_sem.at[sem + 1])

    meet_pole(edges, slots, 0)

    def aside(way, first, rows, sem):
        rows = pl.ds(first, rows)
        lon = west_dev if way else east_dev
        copy(pack_out.at[way, rows], pack_in.at[1 - way, rows], lon, q, send_sem.at[0], chunk_sem.at[sem]).start()

    def sides(first, rows, sem):
        aside(1, first, rows, sem)
        aside(0, first, rows, sem)

    half = (NC + 1) // 2
    bounds = ((0, NI + half * SIDE), (NI + half * SIDE, REST)) if NC > 1 else ((0, REST),)
    for way in (1, 0):
        for i, (first, last) in enumerate(bounds):
            aside(way, first, last - first, i)
    meet_near(edges, slots, 0)

    height = zero
    for k in range(K):
        height = height + jnp.where(depth > k + 0.5, thick_ref[k], 0.0)
    width = NJ // NI
    in_block = lane // width == sub
    parts = ((0, EARLY, EARLY * NI), (EARLY, LATE + 3, LATE * NI + 6))

    def pack_strips(which, sign, arrays, rows=()):
        first, count, _ = parts[which]
        given = len(arrays)
        south = zero
        north = zero
        for i, x in enumerate(arrays):
            for start in (0, width):
                moved = pltpu.roll(x, start, 1, stride=width, stride_axis=0)
                row = jnp.sum(jnp.where(in_block, moved, 0.0), axis=0, keepdims=True)
                row = jnp.broadcast_to(row, (NI, NJ))
                if start:
                    north = jnp.where(sub == i, row, north)
                else:
                    south = jnp.where(sub == i, row, south)
        for i, row in enumerate(rows):
            north = jnp.where(sub == given + i, row, north)
            south = jnp.where(sub == given + i, row, south)
        turned = jnp.where(sub >= given, pltpu.roll(north, width, 1), north) if rows else north
        north = jnp.where(at_pole, sign * flip_lanes(turned), north)
        rows = slice(first, first + count)
        strips[0, rows] = south[:count]
        strips[1, rows] = north[:count]

        @pl.when(at_pole)
        def _():
            rims[0, mirror, rows] = north[:count]

    def each_other(fn):
        def visit(r, carry):
            fn(jnp.where(r <= p, r - 1, r))
            return carry

        if n_lon <= 8:
            for r in range(1, n_lon):
                visit(r, 0)
        else:
            lax.fori_loop(1, n_lon, visit, 0)

    def cast(which):
        first, count, size = parts[which]
        mine = tiles.at[p, pl.ds(first * NI, size)]
        rows = pl.ds(first, count)
        pole = at_pole.astype(jnp.int32)
        side, lat = 1 - pole, q + 1 - pole
        slot = jnp.where(at_pole, mirror, p)

        def send(way, side, slot, lon, lat, out):
            copy(strips.at[way, rows], rims.at[side, slot, rows], lon, lat, cast_send.at[out],
                 cast_recv.at[3 * which + 1 + side]).start()

        @pl.when(not_pole)
        def _():
            send(1, 1, p, p, q + 1, 2)

        @pl.when(not_south)
        def _():
            send(0, 0, p, p, q - 1, 1)

        def to(lon):
            copy(mine, mine, lon, q, cast_send.at[0], cast_recv.at[3 * which]).start()

            @pl.when(not_south)
            def _():
                send(0, 0, p, lon, q - 1, 1)

            send(1, side, slot, lon, lat, 2)
        each_other(to)

    def cast_wait(which):
        first, count, size = parts[which]
        rows = pl.ds(first, count)
        drain(tiles.at[pl.ds(0, n_lon - 1), pl.ds(first * NI, size)], cast_recv.at[3 * which])

        @pl.when(at_pole)
        def _():
            drain(rims.at[0, pl.ds(0, n_lon - 1), rows], cast_recv.at[3 * which + 1])

        @pl.when(not_pole)
        def _():
            drain(rims.at[0, pl.ds(0, n_lon), rows], cast_recv.at[3 * which + 1])

        @pl.when(not_south)
        def _():
            drain(rims.at[1, pl.ds(0, n_lon), rows], cast_recv.at[3 * which + 2])

    first_guess = sea_ref[...].astype(F32) * eta_ref[...]
    for i, x in enumerate((height, first_guess, drive_ref[...])):
        tiles[p, i * NI:(i + 1) * NI] = x
    pack_strips(0, 1.0, (height, first_guess, drive_ref[...]))

    near_e = jnp.where(sub == NI - 1, 0.0, jnp.minimum(depth, pltpu.roll(depth, NI - 1, 0)))
    near_w = jnp.where(sub == 0, 0.0, jnp.minimum(depth, pltpu.roll(depth, 1, 0)))
    near_n = jnp.where(lane == NJ - 1, 0.0, jnp.minimum(depth, pltpu.roll(depth, NJ - 1, 1)))
    near_s = jnp.where(lane == 0, 0.0, jnp.minimum(depth, pltpu.roll(depth, 1, 1)))
    lat_index = (q * NJ + lane).astype(F32)
    coriolis = CORIOLIS * (2.0 * (lat_index + 0.5) / (n_lat * NJ) - 1.0)

    def gate(d, kf, x):
        return jnp.where(d > kf, x, 0.0)

    def inner_lap(x, kf):
        total = gate(near_e, kf, pltpu.roll(x, NI - 1, 0) - x) + gate(near_w, kf, pltpu.roll(x, 1, 0) - x)
        return total + (gate(near_n, kf, pltpu.roll(x, NJ - 1, 1) - x) + gate(near_s, kf, pltpu.roll(x, 1, 1) - x))

    def before_level(k, carry):
        pc, tu, tv = carry
        kf = lax.convert_element_type(k, F32) + 0.5
        u, v = u_ref[k], v_ref[k]
        laps[0, k] = inner_lap(u, kf)
        laps[1, k] = inner_lap(v, kf)
        pc = pc + gate(depth, kf, (CONTRACTION * s_ref[k] - EXPANSION * t_ref[k]) * thick_ref[k])
        pressure[k] = pc
        grad_x = gate(near_e, kf, pltpu.roll(pc, NI - 1, 0) - pc) + gate(near_w, kf, pc - pltpu.roll(pc, 1, 0))
        grad_y = gate(near_n, kf, pltpu.roll(pc, NJ - 1, 1) - pc) + gate(near_s, kf, pc - pltpu.roll(pc, 1, 1))
        u_part = u + coriolis * v - (0.5 * PRESSURE_SCALE) * grad_x
        v_part = v - coriolis * u - (0.5 * PRESSURE_SCALE) * grad_y
        ou_ref[k] = u_part
        ov_ref[k] = v_part
        h = thick_ref[k]
        return pc, tu + gate(depth, kf, h * u_part), tv + gate(depth, kf, h * v_part)

    def before_chunk(c, carry):
        for i in range(KC):
            carry = before_level(c * KC + i, carry)
        return carry

    totals = list(lax.fori_loop(0, NC, before_chunk, (zero,) * 3)[1:])

    cast(0)
    met(slots, 0)

    sign = jnp.where(lane >= 2 * K, -1.0, 1.0).astype(F32)

    def arrived(slot, i, fold):
        north = jnp.where(at_pole, flip_rows(slot[0, i]) * fold, slot[0, i])
        return north, jnp.where(not_south, slot[1, i], 0.0)

    pn0, ps0 = arrived(slots, 0, sign)
    pn1, ps1 = arrived(slots, 1, 1.0)

    def shift_e(x, row):
        return jnp.where(sub == NI - 1, row, pltpu.roll(x, NI - 1, 0))

    def shift_w(x, row):
        return jnp.where(sub == 0, row, pltpu.roll(x, 1, 0))

    rim[0] = pn0
    rim[1] = ps0

    drain(pack_in.at[:, bounds[0][0]:bounds[0][1]], chunk_sem.at[0])
    sides(REST, 2 * K, 2)
    base_e = pack_in[0, 0:1, :]
    base_w = pack_in[1, 0:1, :]
    is_w = sub == 0
    is_s = lane == 0
    depth_ew = jnp.where(is_w, base_w, base_e)
    depth_ns = jnp.where(is_s, ps1, pltpu.roll(pn1, NJ - 1, 1))
    on_ew = jnp.logical_or(is_w, sub == NI - 1)
    on_ns = jnp.logical_or(is_s, lane == NJ - 1)
    near_ew = jnp.where(on_ew, jnp.minimum(depth, depth_ew), 0.0)
    near_ns = jnp.where(on_ns, jnp.minimum(depth, depth_ns), 0.0)
    scale_ew = jnp.where(is_w, 0.5 * PRESSURE_SCALE, -0.5 * PRESSURE_SCALE)
    scale_ns = jnp.where(is_s, 0.5 * PRESSURE_SCALE, -0.5 * PRESSURE_SCALE)

    def rim_ns(north, south, k):
        x = pltpu.roll(north, (NJ - 1 - k) % NJ, 1)
        return jnp.where(is_s, pltpu.roll(south, (NJ - k) % NJ, 1), x)

    def side_ew(c, row):
        row = NI + c * SIDE + row
        return jnp.where(is_w, pack_in[1, row:row + 1, :], pack_in[0, row:row + 1, :])

    both_e = jnp.where(sub == NI - 1, near_ew, near_e)
    both_w = jnp.where(is_w, near_ew, near_w)
    both_n = jnp.where(lane == NJ - 1, near_ns, near_n)
    both_s = jnp.where(is_s, near_ns, near_s)
    overlaps = (both_e, both_w, both_n, both_s)
    sums_lap = [[zero] * 4 for _ in range(2)]
    push_ew = push_ns = zero
    for c in range(NC):
        if c == half and NC > 1:
            drain(pack_in.at[:, bounds[1][0]:bounds[1][1]], chunk_sem.at[1])
        for i in range(KC):
            k = c * KC + i
            kf = k + 0.5
            h = thick_ref[k]
            hp = h * pressure[k]
            push_ew = push_ew + gate(near_ew, kf, hp)
            push_ns = push_ns + gate(near_ns, kf, hp)
            for m, x in enumerate((u_ref[k], v_ref[k])):
                lap = laps[m, k] + gate(near_ew, kf, side_ew(c, m * KC + i) - x)
                lap = lap + gate(near_ns, kf, rim_ns(rim[0], rim[1], (2 + m) * K + k) - x)
                laps[m, k] = lap
                hl = h * lap
                sums_lap[m] = [a + gate(d, kf, hl) for a, d in zip(sums_lap[m], overlaps)]
    push_ew = scale_ew * push_ew
    push_ns = scale_ns * push_ns
    exports, exports_ns = [], []
    for m, (a_e, a_w, a_n, a_s) in enumerate(sums_lap):
        given = jnp.where(sub == NI - 1, 0.0, pltpu.roll(a_w, NI - 1, 0)) + jnp.where(is_w, 0.0, pltpu.roll(a_e, 1, 0))
        given = given + jnp.where(lane == NJ - 1, 0.0, pltpu.roll(a_s, NJ - 1, 1))
        given = given + jnp.where(is_s, 0.0, pltpu.roll(a_n, 1, 1))
        totals[m] = totals[m] + FRICTION * ((a_e + a_w) + (a_n + a_s) - given)
        exports.append(-FRICTION * jnp.where(is_w, a_w, a_e))
        exports_ns.append(-FRICTION * jnp.where(is_s, a_s, a_n))
    totals = [totals[0] - push_ew, totals[1] - push_ns]
    exports[0] = exports[0] - push_ew
    exports_ns[1] = exports_ns[1] - push_ns

    tiles[p, EARLY * NI:(EARLY + 1) * NI] = totals[0]
    tiles[p, (EARLY + 1) * NI:(EARLY + 2) * NI] = totals[1]
    for m in range(2):
        row = (EARLY + LATE) * NI + 2 * m
        tiles[p, row:row + 1] = exports[m][0:1]
        tiles[p, row + 1:row + 2] = exports[m][NI - 1:]
    out_rows = zero
    for row, x in ((0, exports[0][0:1]), (1, exports[1][0:1]), (NI - 2, exports[1][NI - 1:]), (NI - 1, exports[0][NI - 1:])):
        out_rows = jnp.where(sub == row, jnp.broadcast_to(x, (NI, NJ)), out_rows)
    ns_rows = []
    for m, x in enumerate(exports_ns):
        x = jnp.where(lane == 0, pltpu.roll(x, 1, 1), jnp.where(lane == NJ - 1, pltpu.roll(x, NJ - 1, 1), 0.0))
        x = jnp.sum(pltpu.roll(x, 0, 1, stride=width, stride_axis=0), axis=0, keepdims=True)
        row = (EARLY + LATE) * NI + 4 + m
        tiles[p, row:row + 1] = x
        ns_rows.append(jnp.broadcast_to(x, (NI, NJ)))
    pack_strips(1, -1.0, (*totals, out_rows), ns_rows)
    cast(1)

    for side, (d, push) in enumerate(((NI - 1, 0.5 * PRESSURE_SCALE), (0, -0.5 * PRESSURE_SCALE))):
        row = REST + 2 * K
        pack_out[side, row:row + K, :] = push * pressure[:, d, :] - FRICTION * laps[0, :, d, :]
        pack_out[side, row + K:row + 2 * K, :] = -FRICTION * laps[1, :, d, :]
    n2 = s2 = zero
    for k in range(K):
        for m, x in enumerate((-FRICTION * laps[0, k], -FRICTION * laps[1, k] - scale_ns * pressure[k])):
            n2 = put(n2, x, NJ - 1, m * K + k)
            s2 = put(s2, x, 0, m * K + k)
    lap_edges[0] = n2
    lap_edges[1] = s2
    meet_pole(lap_edges, lap_slots, 2)
    meet_near(lap_edges, lap_slots, 2)
    sides(REST + 2 * K, 2 * K, 3)

    def level(c, carry):
        for i in range(KC):
            k = c * KC + i
            kf = lax.convert_element_type(k, F32) + 0.5
            pc = pressure[k]
            parts = (ou_ref[k] - scale_ew * gate(near_ew, kf, pc), ov_ref[k] - scale_ns * gate(near_ns, kf, pc))
            for m, (part, out) in enumerate(zip(parts, (ou_ref, ov_ref))):
                lap = laps[m, k]
                inner = inner_lap(lap, kf) - gate(near_ew, kf, lap) - gate(near_ns, kf, lap)
                out[k] = gate(depth, kf, part - FRICTION * inner)
        return carry

    lax.fori_loop(0, NC, level, 0)

    cast_wait(0)
    flat = tiles.reshape(n_lon * TILES * NI, NJ)
    flat_rim = rims.reshape(2 * n_lon * NI, NJ)
    lanes = iota((n_lon, NJ), 1)

    def loader(f):
        main = [flat[pl.ds(f * NI + s, n_lon, stride=TILES * NI), :] for s in range(NI)]
        north = flat_rim[pl.ds(f, n_lon, stride=NI), :]
        south = jnp.where(not_south, flat_rim[pl.ds(n_lon * NI + f, n_lon, stride=NI), :], 0.0)
        outer = []
        for s in range(NI):
            x = jnp.where(lanes >= NJ - width, pltpu.roll(south, (NJ - width - width * s) % NJ, 1), 0.0)
            outer.append(jnp.where(lanes < width, pltpu.roll(north, (NJ - width * s) % NJ, 1), x))
        return [main, outer]

    def rim_rows(f):
        north = flat_rim[pl.ds(f, n_lon, stride=NI), :]
        south = jnp.where(not_south, flat_rim[pl.ds(n_lon * NI + f, n_lon, stride=NI), :], 0.0)
        return jnp.where(lanes % width == width - 1, north, south)

    def share(total):
        sums[q] = jnp.broadcast_to(total, (NI, NJ))
        mine = sums.at[q, pl.ds(0, 1)]
        for r in range(1, n_lat):
            lat = jnp.where(r <= q, r - 1, r)
            copy(mine, mine, p, lat, cast_send.at[3], cast_recv.at[6]).start()


    def late_wait():
        cast_wait(1)

    x, slope_x, slope_y = surface_solve(loader, rim_rows, late_wait, share, n_lon, K, NI, NJ)
    for i, field in enumerate((x, slope_x, slope_y)):
        for s in range(NI):
            held[i, pl.ds(s, n_lon, stride=NI), :] = field[s]
    block = pl.ds(pl.multiple_of(p * NI, NI), NI)
    ox_ref[0] = held[0, block, :]
    slope_u = GRAVITY * held[1, block, :]
    slope_v = GRAVITY * held[2, block, :]
    drain(pack_in.at[:, REST:REST + 2 * K], chunk_sem.at[2])
    drain(pack_in.at[:, REST + 2 * K:], chunk_sem.at[3])
    met(lap_slots, 2)
    rim[2] = jnp.where(at_pole, -flip_rows(lap_slots[0]), lap_slots[0])
    rim[3] = jnp.where(not_south, lap_slots[1], 0.0)
    def shift_n(x, packed, source):
        return jnp.where(lane == NJ - 1, pltpu.roll(packed, NJ - 1 - source, 1), pltpu.roll(x, NJ - 1, 1))

    def shift_s(x, packed, source):
        return jnp.where(lane == 0, pltpu.roll(packed, lax.rem(NJ - source, NJ), 1), pltpu.roll(x, 1, 1))

    def around(c, inner, ref, f):
        k = c * KC + inner
        x = ref[k]
        row = pl.ds(NI + c * SIDE + (f - 2) * KC + inner if f >= 2 else REST + f * K + k, 1)
        return (x, shift_e(x, pack_in[0, row, :]), shift_w(x, pack_in[1, row, :]),
                shift_n(x, rim[0], f * K + k), shift_s(x, rim[1], f * K + k))

    def beyond_ew(f, k):
        row = pl.ds(REST + f * K + k, 1)
        return jnp.where(is_w, pack_in[1, row, :], pack_in[0, row, :])

    def beyond_ns(f, k):
        at = f * K + k
        north = pltpu.roll(rim[2], NJ - 1 - at, 1)
        return jnp.where(is_s, pltpu.roll(rim[3], lax.rem(NJ - at, NJ), 1), north)

    def tracers(c, i, carry):
        k = c * KC + i
        flux_t, flux_s = carry
        kf = lax.convert_element_type(k, F32) + 0.5
        h = thick_ref[k]
        nxt = jnp.minimum(k + 1, K - 1)
        h_next = thick_ref[nxt]
        hv = jnp.full((NI, NJ), h, F32)
        inv_space = 1.0 / (0.5 * (hv + h_next))
        inv_h = MIXING / hv

        def wet(d):
            return jnp.where(d > kf, 1.0, 0.0)

        mc = wet(depth)
        me, mw, mn, ms = wet(both_e), wet(both_w), wet(both_n), wet(both_s)
        below = jnp.where(jnp.logical_and(depth > kf + 1.0, k < K - 1), inv_space, 0.0)
        t = around(c, i, t_ref, 0)
        s = around(c, i, s_ref, 1)
        u0, ue, uw = around(c, i, u_ref, 2)[:3]
        v0, _, _, vn, vs = around(c, i, v_ref, 3)
        ae = 0.25 * me * (u0 + ue)
        aw = 0.25 * mw * (u0 + uw)
        an = 0.25 * mn * (v0 + vn)
        as_ = 0.25 * ms * (v0 + vs)
        ge, gw, gn, gs = DIFFUSION * me, DIFFUSION * mw, DIFFUSION * mn, DIFFUSION * ms

        def tracer(x, ref, flux_above):
            c, e, w, n, so = x
            total = aw * (w + c) - gw * (c - w) - ae * (c + e) + ge * (e - c)
            total = total + as_ * (so + c) - gs * (c - so) - an * (c + n) + gn * (n - c)
            flux = below * (ref[nxt] - c)
            return mc * (c + total + inv_h * (flux - flux_above)), flux

        new_t, flux_t = tracer(t, t_ref, flux_t)
        new_s, flux_s = tracer(s, s_ref, flux_s)
        ot_ref[k] = new_t
        os_ref[k] = new_s
        for m, (out, slope) in enumerate(((ou_ref, slope_u), (ov_ref, slope_v))):
            star = out[k] + gate(near_ew, kf, beyond_ew(2 + m, k)) + gate(near_ns, kf, beyond_ns(m, k))
            out[k] = gate(depth, kf, star - slope)
        return flux_t, flux_s

    def tracer_chunk(c, carry):
        for i in range(KC):
            carry = tracers(c, i, carry)
        return carry

    lax.fori_loop(0, NC, tracer_chunk, (zero,) * 2)

    drain(pack_out, send_sem.at[0])

    sent = pack_in.at[0, 0:3 * NI]

    @pl.when(not_south)
    def _():
        drain(sent, send_sem.at[1])

    drain(sent, send_sem.at[2])

    used = pl.ds(0, NI)
    drain(tiles.at[pl.ds(0, n_lon - 1), pl.ds(0, (EARLY + LATE) * NI + 6)], cast_send.at[0])

    @pl.when(not_south)
    def _():
        drain(rims.at[0, pl.ds(0, n_lon), used], cast_send.at[1])

    @pl.when(not_pole)
    def _():
        drain(rims.at[0, pl.ds(0, n_lon), used], cast_send.at[2])

    @pl.when(at_pole)
    def _():
        drain(rims.at[0, pl.ds(0, n_lon - 1), used], cast_send.at[2])

    drain(sums.at[pl.ds(0, n_lat - 1), pl.ds(0, 1)], cast_recv.at[6])
    total = functools.reduce(lambda a, b: a + b, [sums[lat, 0:1] for lat in range(n_lat)])
    rms = jnp.sqrt(total / (n_lon * NI * n_lat * NJ) + EPSILON)
    ox_ref[1] = jnp.broadcast_to(rms, (NI, NJ))
    drain(sums.at[pl.ds(0, n_lat - 1), pl.ds(0, 1)], cast_send.at[3])


def surface_solve(load, rim_rows, late_wait, share, n_lon, K, NI, NJ):
    width = NJ // NI
    tiles = range(2)
    lines = range(NI)
    lane = iota((n_lon, NJ), 1)
    edge = jnp.logical_or(lane == 0, lane == NJ - 1)

    def every(fn, *arrays):
        return [[fn(*(a[b][s] for a in arrays)) for s in lines] for b in tiles]

    def east(x):
        return [x[b][1:] + [pltpu.roll(x[b][0], n_lon - 1, 0)] for b in tiles]

    def west(x):
        return [[pltpu.roll(x[b][NI - 1], 1, 0)] + x[b][:-1] for b in tiles]

    def joined(x, shift, edge):
        moved = [[pltpu.roll(x[b][s], shift, 1) for s in lines] for b in tiles]
        return [[jnp.where(lane == edge, moved[1 - b][s], moved[b][s]) for s in lines] for b in tiles]

    def north(x):
        return joined(x, NJ - 1, NJ - 1)

    def south(x):
        return joined(x, 1, 0)

    height = load(0)
    scale = lambda a, c: jnp.minimum(a, c) * (1.0 / K)
    w_e = every(scale, height, east(height))
    w_w = every(scale, height, west(height))
    w_n = every(scale, height, north(height))
    w_s = every(scale, height, south(height))
    diag = every(lambda a, b, c, d: STORAGE + a + b + c + d, w_e, w_w, w_n, w_s)

    def apply(x):
        return every(
            lambda dg, c, we, e, ww, w, wn, n, ws, s: dg * c - (we * e + ww * w + wn * n + ws * s),
            diag, x, w_e, east(x), w_w, west(x), w_n, north(x), w_s, south(x))

    middle = NI // 2
    spans = [(s, s - 1, s + 1) for s in range(middle)]
    spans += [(s, s + 1, s - 1) for s in range(NI - 1, middle - 1, -1)]
    pivots, carries, factors = ([[None] * NI for _ in tiles] for _ in range(3))
    joints = []
    for b in tiles:
        for s, before, after in spans:
            back, ahead = (w_w, w_e) if after > s else (w_e, w_w)
            pivot = diag[b][s]
            if s not in (0, NI - 1):
                pivot = pivot + back[b][s] * factors[b][before]
            pivots[b][s] = 1.0 / pivot
            carries[b][s] = back[b][s] * pivots[b][s]
            factors[b][s] = -ahead[b][s] * pivots[b][s]
        joints.append(1.0 / (1.0 - factors[b][middle - 1] * factors[b][middle]))

    def precondition(r):
        out = []
        for b in tiles:
            part = [None] * NI
            for s, before, after in spans:
                part[s] = r[b][s] * pivots[b][s]
                if s not in (0, NI - 1):
                    part[s] = part[s] + carries[b][s] * part[before]
            low, high = part[middle - 1], part[middle]
            part[middle - 1] = (low - factors[b][middle - 1] * high) * joints[b]
            part[middle] = (high - factors[b][middle] * low) * joints[b]
            for s in range(middle - 2, -1, -1):
                part[s] = part[s] - factors[b][s] * part[s + 1]
            for s in range(middle + 1, NI):
                part[s] = part[s] - factors[b][s] * part[s - 1]
            out.append(part)
        return out

    x = load(1)
    drive = load(2)
    start = every(lambda h, d, a: jnp.where(h > 0.0, d, 0.0) - a, height, drive, apply(x))
    late_wait()
    t_u = load(EARLY)
    t_v = load(EARLY + 1)
    inner, outer = load(EARLY + LATE)
    for m, t in enumerate((t_u, t_v)):
        for b, (from_w, from_e) in enumerate(((inner[2 * m], inner[2 * m + 1]), (outer[m], outer[NI - 1 - m]))):
            t[b][NI - 1] = t[b][NI - 1] + pltpu.roll(from_w, n_lon - 1, 0)
            t[b][0] = t[b][0] + pltpu.roll(from_e, 1, 0)
        own, beyond = inner[4 + m], rim_rows(EARLY + LATE + 1 + m)
        for s in lines:
            for b, row in ((0, beyond), (1, own)):
                moved = pltpu.roll(row, (NJ - width * s) % NJ, 1) if s else row
                t[b][s] = t[b][s] + jnp.where(edge, moved, 0.0)
    residual = every(
        lambda h, d, e, w, n, s: d - jnp.where(h > 0.0, 0.5 * DIVERGENCE * ((e - w) + (n - s)), 0.0),
        height, start, east(t_u), west(t_u), north(t_v), south(t_v))
    mid = 0.5 * (SPECTRUM_HIGH + SPECTRUM_LOW)
    half = 0.5 * (SPECTRUM_HIGH - SPECTRUM_LOW)
    ratio = mid / half

    def across(d):
        out = every(lambda wn, n, ws, s: wn * n + ws * s, w_n, north(d), w_s, south(d))
        for b in tiles:
            out[b][NI - 1] = out[b][NI - 1] + w_e[b][NI - 1] * pltpu.roll(d[b][0], n_lon - 1, 0)
            out[b][0] = out[b][0] + w_w[b][0] * pltpu.roll(d[b][NI - 1], 1, 0)
        return out

    direction = precondition(residual)
    image = residual
    if mid != 1.0:
        direction, image = (every(lambda a: a / mid, f) for f in (direction, image))
    rho = 1.0 / ratio
    for step in range(ITERS):
        x = every(lambda a, b: a + b, x, direction)
        if step == 0 and mid == 1.0:
            residual = across(direction)
        else:
            residual = every(lambda r, m, c: (r - m) + c, residual, image, across(direction))
        if step + 1 < ITERS:
            rho_next = 1.0 / (2.0 * ratio - rho)
            keep, gain = rho_next * rho, 2.0 * rho_next / half
            direction = every(lambda d, z: keep * d + gain * z, direction, precondition(residual))
            image = every(lambda m, r: keep * m + gain * r, image, residual)
            rho = rho_next
    squares = functools.reduce(lambda a, b: a + b, [a * a for a in residual[0]])
    share(jnp.sum(jnp.sum(squares, axis=1, keepdims=True), axis=0, keepdims=True))
    slope_x = every(lambda e, w: 0.5 * (e - w), east(x), west(x))
    slope_y = every(lambda n, s: 0.5 * (n - s), north(x), south(x))
    return x[0], slope_x[0], slope_y[0]


def finish_kernel(kept, x_ref, ot_ref, os_ref, ou_ref, ov_ref, ox_ref, orms_ref, rms, sem):
    K = kept.shape[1]
    piece = K // 4 if K % 4 == 0 else K
    for f, target in enumerate((ot_ref, os_ref, ou_ref, ov_ref)):
        for first in range(0, K, piece):
            levels = pl.ds(first, piece)
            pltpu.make_async_copy(kept.at[f, levels], target.at[levels], sem.at[0]).start()
    surface = pltpu.make_async_copy(x_ref.at[0], ox_ref, sem.at[1])
    surface.start()
    rms[0] = jnp.max(x_ref[1])
    scalar = pltpu.make_async_copy(rms, orms_ref, sem.at[2])
    scalar.start()
    pltpu.make_async_copy(kept, kept, sem.at[0]).wait()
    surface.wait()
    scalar.wait()


def per_device(n_lon, n_lat, *args):
    K, NI, NJ = args[0].shape
    KC = 8 if K % 8 == 0 else K
    NC = K // KC
    vmem = pl.BlockSpec(memory_space=pltpu.VMEM)
    hbm = pl.BlockSpec(memory_space=pltpu.HBM)
    big = jax.ShapeDtypeStruct((K, NI, NJ), F32)
    tile = jax.ShapeDtypeStruct((NI, NJ), F32)
    one = jax.ShapeDtypeStruct((1,), F32)
    pack = pltpu.VMEM((2, NI + NC * 2 * KC + 4 * K, NJ), F32)

    def room(*lead):
        return pltpu.VMEM((*lead, NI, NJ), F32)

    parts = pl.pallas_call(
        functools.partial(step_kernel, n_lon, n_lat, KC),
        out_shape=(room(4, K), room(2)),
        in_specs=[hbm] * 9,
        out_specs=(vmem,) * 2,
        scratch_shapes=[
            room(4, K), pltpu.VMEM((2, NI, NJ), jnp.int32), room(2), pltpu.SMEM((K,), F32),
            pack, pack, room(2, 2), room(2, 2), room(2), room(2), room(4),
            room(2, K), room(K), pltpu.VMEM((n_lon, TILES * NI, NJ), F32), room(2), room(2, n_lon), room(n_lat),
            pltpu.VMEM((3, n_lon * NI, NJ), F32),
            pltpu.SemaphoreType.DMA((3,)), pltpu.SemaphoreType.DMA((3,)), pltpu.SemaphoreType.DMA((4,)),
            pltpu.SemaphoreType.DMA((4,)), pltpu.SemaphoreType.DMA((4,)), pltpu.SemaphoreType.DMA((7,)),
        ],
        compiler_params=pltpu.CompilerParams(
            collective_id=0, has_side_effects=True),
        name="step",
    )(*args)
    outs = pl.pallas_call(
        finish_kernel,
        out_shape=(big, big, big, big, tile, one),
        in_specs=[vmem] * 2,
        out_specs=(hbm,) * 6,
        scratch_shapes=[pltpu.SMEM((1,), F32), pltpu.SemaphoreType.DMA((3,))],
        name="finish",
    )(*[pltpu.with_memory_space_constraint(part, pltpu.VMEM) for part in parts])
    return outs[:5] + (outs[5].reshape(()),)


def solution(mesh):
    n_lon, n_lat = mesh.shape["lon"], mesh.shape["lat"]
    spec3 = P(None, "lon", "lat")
    spec2 = P("lon", "lat")
    return jax.shard_map(
        functools.partial(per_device, n_lon, n_lat),
        mesh=mesh,
        in_specs=(spec3, spec3, spec3, spec3, spec2, spec2, P(), spec2, spec2),
        out_specs=(spec3, spec3, spec3, spec3, spec2, P()),
        check_vma=False,
    )
```

```python
import functools

import jax
import jax.numpy as jnp
from jax import lax
from jax.experimental import pallas as pl
from jax.experimental.pallas import tpu as pltpu
from jax.sharding import PartitionSpec as P

ITERS = 4
DIFFUSION = 0.15
MIXING = 0.1
EXPANSION = 0.2
CONTRACTION = 0.15
PRESSURE_SCALE = 0.02
CORIOLIS = 0.5
FRICTION = 0.01
DIVERGENCE = 0.3
STORAGE = 0.1
SPECTRUM_LOW = 0.1
SPECTRUM_HIGH = 1.9
GRAVITY = 0.3
EPSILON = 1e-06

MESH = pl.DeviceIdType.MESH
F32 = jnp.float32
EARLY = 3
LATE = 2
TILES = EARLY + LATE + 1


def iota(shape, axis):
    return lax.broadcasted_iota(jnp.int32, shape, axis)


def flip(x, axis):
    return jnp.take_along_axis(x, x.shape[axis] - 1 - iota(x.shape, axis), axis=axis)


def flip_rows(x):
    return flip(x, 0)


def flip_lanes(x):
    return flip(x, 1)


def step_kernel(n_lon, n_lat, KC, *refs):
    sources, refs = refs[:9], refs[9:]
    (kept, ox_ref), refs = refs[:2], refs[2:]
    (fields, ints, floats, thick_ref, pack_out, pack_in, edges, slots, lap_edges, lap_slots, rim, laps, pressure, tiles, strips,
     rims, sums, held, load_sem, send_sem, chunk_sem, edge_sem, cast_send, cast_recv) = refs
    _, K, NI, NJ = fields.shape
    NC = K // KC
    SIDE = 2 * KC
    REST = NI + NC * SIDE
    t_ref, s_ref, u_ref, v_ref = (fields.at[f] for f in range(4))
    ot_ref, os_ref, ou_ref, ov_ref = (kept.at[f] for f in range(4))
    num_ref, sea_ref, eta_ref, drive_ref = ints.at[0], ints.at[1], floats.at[0], floats.at[1]
    p = lax.axis_index("lon")
    q = lax.axis_index("lat")
    east_dev = lax.rem(p + 1, n_lon)
    west_dev = lax.rem(p + n_lon - 1, n_lon)
    at_pole = q == n_lat - 1
    not_pole = q < n_lat - 1
    not_south = q > 0
    mirror = n_lon - 1 - p
    lons = [lax.rem(p + r, n_lon) for r in range(min(n_lon, 8))]

    barrier = pltpu.get_barrier_semaphore()

    def greet(lon, lat):
        pl.semaphore_signal(barrier, inc=1, device_id={"lon": lon, "lat": lat}, device_id_type=MESH)

    greet(east_dev, q)
    if n_lon > 2:
        greet(west_dev, q)

    def around_lon(first, last, fn):
        def visit(r, carry):
            fn(lax.rem(p + r, n_lon))
            return carry

        if n_lon <= 8:
            for lon in lons[first:last]:
                fn(lon)
        else:
            lax.fori_loop(first, last, visit, 0)

    @pl.when(at_pole)
    def _():
        around_lon(2, n_lon - 1, lambda lon: greet(lon, q))

    @pl.when(not_south)
    def _():
        around_lon(0, n_lon, lambda lon: greet(lon, q - 1))

    @pl.when(not_pole)
    def _():
        around_lon(0, n_lon, lambda lon: greet(lon, q + 1))

    def load(i, dst, sem):
        pltpu.make_async_copy(sources[i], dst, load_sem.at[sem]).start()

    load(4, num_ref, 1)
    load(5, sea_ref, 1)
    load(7, eta_ref, 1)
    load(8, drive_ref, 1)
    for f in (2, 3, 0, 1):
        load(f, fields.at[f], 0)
    thick_load = pltpu.make_async_copy(sources[6], thick_ref, load_sem.at[2])
    thick_load.start()

    @pl.when(not_pole)
    def _():
        around_lon(2, n_lon - 1, lambda lon: greet(lon, q))

    for lat in range(n_lat):
        @pl.when(jnp.logical_or(q - lat > 1, lat - q > 1))
        def _():
            greet(p, lat)

    def drain(ref, sem):
        pltpu.make_async_copy(ref, ref, sem).wait()

    thick_load.wait()
    drain(fields.at[0, 0:4], load_sem.at[1])
    drain(fields, load_sem.at[0])
    sub = iota((NI, NJ), 0)
    lane = iota((NI, NJ), 1)
    depth = (num_ref[...] * sea_ref[...]).astype(F32)

    for side, d1 in enumerate((NI - 1, 0)):
        for c in range(NC):
            levels = slice(c * KC, (c + 1) * KC)
            for m, ref in enumerate((u_ref, v_ref)):
                row = NI + c * SIDE + m * KC
                pack_out[side, row:row + KC, :] = ref[levels, d1, :]
        for m, ref in enumerate((t_ref, s_ref)):
            row = REST + m * K
            pack_out[side, row:row + K, :] = ref[:, d1, :]
        pack_out[side, 0:NI, :] = jnp.broadcast_to(depth[d1:d1 + 1, :], (NI, NJ))

    zero = jnp.zeros((NI, NJ), F32)

    def put(acc, x, source, target):
        moved = pltpu.roll(x, (target - source) % NJ, 1) if source != target else x
        return jnp.where(lane == target, moved, acc)

    n0 = s0 = zero
    for f, ref in enumerate((t_ref, s_ref, u_ref, v_ref)):
        for k in range(K):
            n0 = put(n0, ref[k], NJ - 1, f * K + k)
            s0 = put(s0, ref[k], 0, f * K + k)
    npk, spk = edges.at[0], edges.at[1]
    npk[0] = n0
    npk[1] = put(zero, depth, NJ - 1, 0)
    spk[0] = s0
    spk[1] = put(zero, depth, 0, 0)

    peers = n_lon + n_lat - 2 + (n_lon - 1) * (not_south.astype(jnp.int32) + not_pole.astype(jnp.int32))
    pl.semaphore_wait(barrier, peers)

    def copy(src, dst, lon, lat, out, into):
        return pltpu.make_async_remote_copy(
            src_ref=src, dst_ref=dst, send_sem=out, recv_sem=into,
            device_id={"lon": lon, "lat": lat}, device_id_type=MESH)

    def meet_pole(pack, slot, sem):
        @pl.when(at_pole)
        def _():
            copy(pack.at[0], slot.at[0], mirror, q, send_sem.at[2], edge_sem.at[sem]).start()

    def meet_near(pack, slot, sem):
        @pl.when(not_south)
        def _():
            copy(pack.at[1], slot.at[0], p, q - 1, send_sem.at[1], edge_sem.at[sem]).start()

        @pl.when(not_pole)
        def _():
            copy(pack.at[0], slot.at[1], p, q + 1, send_sem.at[2], edge_sem.at[sem + 1]).start()

    def met(slot, sem):
        drain(slot.at[0], edge_sem.at[sem])

        @pl.when(not_south)
        def _():
            drain(slot.at[1], edge_sem.at[sem + 1])

    meet_pole(edges, slots, 0)

    def aside(way, first, rows, sem):
        rows = pl.ds(first, rows)
        lon = west_dev if way else east_dev
        copy(pack_out.at[way, rows], pack_in.at[1 - way, rows], lon, q, send_sem.at[0], chunk_sem.at[sem]).start()

    def sides(first, rows, sem):
        aside(1, first, rows, sem)
        aside(0, first, rows, sem)

    half = (NC + 1) // 2
    bounds = ((0, NI + half * SIDE), (NI + half * SIDE, REST)) if NC > 1 else ((0, REST),)
    for way in (1, 0):
        for i, (first, last) in enumerate(bounds):
            aside(way, first, last - first, i)
    meet_near(edges, slots, 0)

    height = zero
    for k in range(K):
        height = height + jnp.where(depth > k + 0.5, thick_ref[k], 0.0)
    width = NJ // NI
    in_block = lane // width == sub
    parts = ((0, EARLY, EARLY * NI), (EARLY, LATE + 3, LATE * NI + 6))

    def pack_strips(which, sign, arrays, rows=()):
        first, count, _ = parts[which]
        given = len(arrays)
        south = zero
        north = zero
        for i, x in enumerate(arrays):
            for start in (0, width):
                moved = pltpu.roll(x, start, 1, stride=width, stride_axis=0)
                row = jnp.sum(jnp.where(in_block, moved, 0.0), axis=0, keepdims=True)
                row = jnp.broadcast_to(row, (NI, NJ))
                if start:
                    north = jnp.where(sub == i, row, north)
                else:
                    south = jnp.where(sub == i, row, south)
        for i, row in enumerate(rows):
            north = jnp.where(sub == given + i, row, north)
            south = jnp.where(sub == given + i, row, south)
        turned = jnp.where(sub >= given, pltpu.roll(north, width, 1), north) if rows else north
        north = jnp.where(at_pole, sign * flip_lanes(turned), north)
        rows = slice(first, first + count)
        strips[0, rows] = south[:count]
        strips[1, rows] = north[:count]

        @pl.when(at_pole)
        def _():
            rims[0, mirror, rows] = north[:count]

    def each_other(fn):
        def visit(r, carry):
            fn(jnp.where(r <= p, r - 1, r))
            return carry

        if n_lon <= 8:
            for r in range(1, n_lon):
                visit(r, 0)
        else:
            lax.fori_loop(1, n_lon, visit, 0)

    def cast(which):
        first, count, size = parts[which]
        mine = tiles.at[p, pl.ds(first * NI, size)]
        rows = pl.ds(first, count)
        pole = at_pole.astype(jnp.int32)
        side, lat = 1 - pole, q + 1 - pole
        slot = jnp.where(at_pole, mirror, p)

        def send(way, side, slot, lon, lat, out):
            copy(strips.at[way, rows], rims.at[side, slot, rows], lon, lat, cast_send.at[out],
                 cast_recv.at[3 * which + 1 + side]).start()

        @pl.when(not_pole)
        def _():
            send(1, 1, p, p, q + 1, 2)

        @pl.when(not_south)
        def _():
            send(0, 0, p, p, q - 1, 1)

        def to(lon):
            copy(mine, mine, lon, q, cast_send.at[0], cast_recv.at[3 * which]).start()

            @pl.when(not_south)
            def _():
                send(0, 0, p, lon, q - 1, 1)

            send(1, side, slot, lon, lat, 2)
        each_other(to)

    def cast_wait(which):
        first, count, size = parts[which]
        rows = pl.ds(first, count)
        drain(tiles.at[pl.ds(0, n_lon - 1), pl.ds(first * NI, size)], cast_recv.at[3 * which])

        @pl.when(at_pole)
        def _():
            drain(rims.at[0, pl.ds(0, n_lon - 1), rows], cast_recv.at[3 * which + 1])

        @pl.when(not_pole)
        def _():
            drain(rims.at[0, pl.ds(0, n_lon), rows], cast_recv.at[3 * which + 1])

        @pl.when(not_south)
        def _():
            drain(rims.at[1, pl.ds(0, n_lon), rows], cast_recv.at[3 * which + 2])

    first_guess = sea_ref[...].astype(F32) * eta_ref[...]
    for i, x in enumerate((height, first_guess, drive_ref[...])):
        tiles[p, i * NI:(i + 1) * NI] = x
    pack_strips(0, 1.0, (height, first_guess, drive_ref[...]))

    near_e = jnp.where(sub == NI - 1, 0.0, jnp.minimum(depth, pltpu.roll(depth, NI - 1, 0)))
    near_w = jnp.where(sub == 0, 0.0, jnp.minimum(depth, pltpu.roll(depth, 1, 0)))
    near_n = jnp.where(lane == NJ - 1, 0.0, jnp.minimum(depth, pltpu.roll(depth, NJ - 1, 1)))
    near_s = jnp.where(lane == 0, 0.0, jnp.minimum(depth, pltpu.roll(depth, 1, 1)))
    lat_index = (q * NJ + lane).astype(F32)
    coriolis = CORIOLIS * (2.0 * (lat_index + 0.5) / (n_lat * NJ) - 1.0)

    def gate(d, kf, x):
        return jnp.where(d > kf, x, 0.0)

    def inner_lap(x, kf):
        total = gate(near_e, kf, pltpu.roll(x, NI - 1, 0) - x) + gate(near_w, kf, pltpu.roll(x, 1, 0) - x)
        return total + (gate(near_n, kf, pltpu.roll(x, NJ - 1, 1) - x) + gate(near_s, kf, pltpu.roll(x, 1, 1) - x))

    def before_level(k, carry):
        pc, tu, tv = carry
        kf = lax.convert_element_type(k, F32) + 0.5
        u, v = u_ref[k], v_ref[k]
        laps[0, k] = inner_lap(u, kf)
        laps[1, k] = inner_lap(v, kf)
        pc = pc + gate(depth, kf, (CONTRACTION * s_ref[k] - EXPANSION * t_ref[k]) * thick_ref[k])
        pressure[k] = pc
        grad_x = gate(near_e, kf, pltpu.roll(pc, NI - 1, 0) - pc) + gate(near_w, kf, pc - pltpu.roll(pc, 1, 0))
        grad_y = gate(near_n, kf, pltpu.roll(pc, NJ - 1, 1) - pc) + gate(near_s, kf, pc - pltpu.roll(pc, 1, 1))
        u_part = u + coriolis * v - (0.5 * PRESSURE_SCALE) * grad_x
        v_part = v - coriolis * u - (0.5 * PRESSURE_SCALE) * grad_y
        ou_ref[k] = u_part
        ov_ref[k] = v_part
        h = thick_ref[k]
        return pc, tu + gate(depth, kf, h * u_part), tv + gate(depth, kf, h * v_part)

    def before_chunk(c, carry):
        for i in range(KC):
            carry = before_level(c * KC + i, carry)
        return carry

    totals = list(lax.fori_loop(0, NC, before_chunk, (zero,) * 3)[1:])

    cast(0)
    met(slots, 0)

    sign = jnp.where(lane >= 2 * K, -1.0, 1.0).astype(F32)

    def arrived(slot, i, fold):
        north = jnp.where(at_pole, flip_rows(slot[0, i]) * fold, slot[0, i])
        return north, jnp.where(not_south, slot[1, i], 0.0)

    pn0, ps0 = arrived(slots, 0, sign)
    pn1, ps1 = arrived(slots, 1, 1.0)

    def shift_e(x, row):
        return jnp.where(sub == NI - 1, row, pltpu.roll(x, NI - 1, 0))

    def shift_w(x, row):
        return jnp.where(sub == 0, row, pltpu.roll(x, 1, 0))

    rim[0] = pn0
    rim[1] = ps0

    drain(pack_in.at[:, bounds[0][0]:bounds[0][1]], chunk_sem.at[0])
    sides(REST, 2 * K, 2)
    base_e = pack_in[0, 0:1, :]
    base_w = pack_in[1, 0:1, :]
    is_w = sub == 0
    is_s = lane == 0
    depth_ew = jnp.where(is_w, base_w, base_e)
    depth_ns = jnp.where(is_s, ps1, pltpu.roll(pn1, NJ - 1, 1))
    on_ew = jnp.logical_or(is_w, sub == NI - 1)
    on_ns = jnp.logical_or(is_s, lane == NJ - 1)
    near_ew = jnp.where(on_ew, jnp.minimum(depth, depth_ew), 0.0)
    near_ns = jnp.where(on_ns, jnp.minimum(depth, depth_ns), 0.0)
    scale_ew = jnp.where(is_w, 0.5 * PRESSURE_SCALE, -0.5 * PRESSURE_SCALE)
    scale_ns = jnp.where(is_s, 0.5 * PRESSURE_SCALE, -0.5 * PRESSURE_SCALE)

    def rim_ns(north, south, k):
        x = pltpu.roll(north, (NJ - 1 - k) % NJ, 1)
        return jnp.where(is_s, pltpu.roll(south, (NJ - k) % NJ, 1), x)

    def side_ew(c, row):
        row = NI + c * SIDE + row
        return jnp.where(is_w, pack_in[1, row:row + 1, :], pack_in[0, row:row + 1, :])

    both_e = jnp.where(sub == NI - 1, near_ew, near_e)
    both_w = jnp.where(is_w, near_ew, near_w)
    both_n = jnp.where(lane == NJ - 1, near_ns, near_n)
    both_s = jnp.where(is_s, near_ns, near_s)
    overlaps = (both_e, both_w, both_n, both_s)
    sums_lap = [[zero] * 4 for _ in range(2)]
    push_ew = push_ns = zero
    for c in range(NC):
        if c == half and NC > 1:
            drain(pack_in.at[:, bounds[1][0]:bounds[1][1]], chunk_sem.at[1])
        for i in range(KC):
            k = c * KC + i
            kf = k + 0.5
            h = thick_ref[k]
            hp = h * pressure[k]
            push_ew = push_ew + gate(near_ew, kf, hp)
            push_ns = push_ns + gate(near_ns, kf, hp)
            for m, x in enumerate((u_ref[k], v_ref[k])):
                lap = laps[m, k] + gate(near_ew, kf, side_ew(c, m * KC + i) - x)
                lap = lap + gate(near_ns, kf, rim_ns(rim[0], rim[1], (2 + m) * K + k) - x)
                laps[m, k] = lap
                hl = h * lap
                sums_lap[m] = [a + gate(d, kf, hl) for a, d in zip(sums_lap[m], overlaps)]
    push_ew = scale_ew * push_ew
    push_ns = scale_ns * push_ns
    exports, exports_ns = [], []
    for m, (a_e, a_w, a_n, a_s) in enumerate(sums_lap):
        given = jnp.where(sub == NI - 1, 0.0, pltpu.roll(a_w, NI - 1, 0)) + jnp.where(is_w, 0.0, pltpu.roll(a_e, 1, 0))
        given = given + jnp.where(lane == NJ - 1, 0.0, pltpu.roll(a_s, NJ - 1, 1))
        given = given + jnp.where(is_s, 0.0, pltpu.roll(a_n, 1, 1))
        totals[m] = totals[m] + FRICTION * ((a_e + a_w) + (a_n + a_s) - given)
        exports.append(-FRICTION * jnp.where(is_w, a_w, a_e))
        exports_ns.append(-FRICTION * jnp.where(is_s, a_s, a_n))
    totals = [totals[0] - push_ew, totals[1] - push_ns]
    exports[0] = exports[0] - push_ew
    exports_ns[1] = exports_ns[1] - push_ns

    tiles[p, EARLY * NI:(EARLY + 1) * NI] = totals[0]
    tiles[p, (EARLY + 1) * NI:(EARLY + 2) * NI] = totals[1]
    for m in range(2):
        row = (EARLY + LATE) * NI + 2 * m
        tiles[p, row:row + 1] = exports[m][0:1]
        tiles[p, row + 1:row + 2] = exports[m][NI - 1:]
    out_rows = zero
    for row, x in ((0, exports[0][0:1]), (1, exports[1][0:1]), (NI - 2, exports[1][NI - 1:]), (NI - 1, exports[0][NI - 1:])):
        out_rows = jnp.where(sub == row, jnp.broadcast_to(x, (NI, NJ)), out_rows)
    ns_rows = []
    for m, x in enumerate(exports_ns):
        x = jnp.where(lane == 0, pltpu.roll(x, 1, 1), jnp.where(lane == NJ - 1, pltpu.roll(x, NJ - 1, 1), 0.0))
        x = jnp.sum(pltpu.roll(x, 0, 1, stride=width, stride_axis=0), axis=0, keepdims=True)
        row = (EARLY + LATE) * NI + 4 + m
        tiles[p, row:row + 1] = x
        ns_rows.append(jnp.broadcast_to(x, (NI, NJ)))
    pack_strips(1, -1.0, (*totals, out_rows), ns_rows)
    cast(1)

    for side, (d, push) in enumerate(((NI - 1, 0.5 * PRESSURE_SCALE), (0, -0.5 * PRESSURE_SCALE))):
        row = REST + 2 * K
        pack_out[side, row:row + K, :] = push * pressure[:, d, :] - FRICTION * laps[0, :, d, :]
        pack_out[side, row + K:row + 2 * K, :] = -FRICTION * laps[1, :, d, :]
    n2 = s2 = zero
    for k in range(K):
        for m, x in enumerate((-FRICTION * laps[0, k], -FRICTION * laps[1, k] - scale_ns * pressure[k])):
            n2 = put(n2, x, NJ - 1, m * K + k)
            s2 = put(s2, x, 0, m * K + k)
    lap_edges[0] = n2
    lap_edges[1] = s2
    meet_pole(lap_edges, lap_slots, 2)
    meet_near(lap_edges, lap_slots, 2)
    sides(REST + 2 * K, 2 * K, 3)

    def level(c, carry):
        for i in range(KC):
            k = c * KC + i
            kf = lax.convert_element_type(k, F32) + 0.5
            pc = pressure[k]
            parts = (ou_ref[k] - scale_ew * gate(near_ew, kf, pc), ov_ref[k] - scale_ns * gate(near_ns, kf, pc))
            for m, (part, out) in enumerate(zip(parts, (ou_ref, ov_ref))):
                lap = laps[m, k]
                inner = inner_lap(lap, kf) - gate(near_ew, kf, lap) - gate(near_ns, kf, lap)
                out[k] = gate(depth, kf, part - FRICTION * inner)
        return carry

    lax.fori_loop(0, NC, level, 0)

    cast_wait(0)
    flat = tiles.reshape(n_lon * TILES * NI, NJ)
    flat_rim = rims.reshape(2 * n_lon * NI, NJ)
    lanes = iota((n_lon, NJ), 1)

    def loader(f):
        main = [flat[pl.ds(f * NI + s, n_lon, stride=TILES * NI), :] for s in range(NI)]
        north = flat_rim[pl.ds(f, n_lon, stride=NI), :]
        south = jnp.where(not_south, flat_rim[pl.ds(n_lon * NI + f, n_lon, stride=NI), :], 0.0)
        outer = []
        for s in range(NI):
            x = jnp.where(lanes >= NJ - width, pltpu.roll(south, (NJ - width - width * s) % NJ, 1), 0.0)
            outer.append(jnp.where(lanes < width, pltpu.roll(north, (NJ - width * s) % NJ, 1), x))
        return [main, outer]

    def rim_rows(f):
        north = flat_rim[pl.ds(f, n_lon, stride=NI), :]
        south = jnp.where(not_south, flat_rim[pl.ds(n_lon * NI + f, n_lon, stride=NI), :], 0.0)
        return jnp.where(lanes % width == width - 1, north, south)

    def share(total):
        sums[q] = jnp.broadcast_to(total, (NI, NJ))
        mine = sums.at[q, pl.ds(0, 1)]
        for r in range(1, n_lat):
            lat = jnp.where(r <= q, r - 1, r)
            copy(mine, mine, p, lat, cast_send.at[3], cast_recv.at[6]).start()


    def late_wait():
        cast_wait(1)

    x, slope_x, slope_y = surface_solve(loader, rim_rows, late_wait, share, n_lon, K, NI, NJ)
    for i, field in enumerate((x, slope_x, slope_y)):
        for s in range(NI):
            held[i, pl.ds(s, n_lon, stride=NI), :] = field[s]
    block = pl.ds(pl.multiple_of(p * NI, NI), NI)
    ox_ref[0] = held[0, block, :]
    slope_u = GRAVITY * held[1, block, :]
    slope_v = GRAVITY * held[2, block, :]
    drain(pack_in.at[:, REST:REST + 2 * K], chunk_sem.at[2])
    drain(pack_in.at[:, REST + 2 * K:], chunk_sem.at[3])
    met(lap_slots, 2)
    rim[2] = jnp.where(at_pole, -flip_rows(lap_slots[0]), lap_slots[0])
    rim[3] = jnp.where(not_south, lap_slots[1], 0.0)
    def shift_n(x, packed, source):
        return jnp.where(lane == NJ - 1, pltpu.roll(packed, NJ - 1 - source, 1), pltpu.roll(x, NJ - 1, 1))

    def shift_s(x, packed, source):
        return jnp.where(lane == 0, pltpu.roll(packed, lax.rem(NJ - source, NJ), 1), pltpu.roll(x, 1, 1))

    def around(c, inner, ref, f):
        k = c * KC + inner
        x = ref[k]
        row = pl.ds(NI + c * SIDE + (f - 2) * KC + inner if f >= 2 else REST + f * K + k, 1)
        return (x, shift_e(x, pack_in[0, row, :]), shift_w(x, pack_in[1, row, :]),
                shift_n(x, rim[0], f * K + k), shift_s(x, rim[1], f * K + k))

    def beyond_ew(f, k):
        row = pl.ds(REST + f * K + k, 1)
        return jnp.where(is_w, pack_in[1, row, :], pack_in[0, row, :])

    def beyond_ns(f, k):
        at = f * K + k
        north = pltpu.roll(rim[2], NJ - 1 - at, 1)
        return jnp.where(is_s, pltpu.roll(rim[3], lax.rem(NJ - at, NJ), 1), north)

    def tracers(c, i, carry):
        k = c * KC + i
        flux_t, flux_s = carry
        kf = lax.convert_element_type(k, F32) + 0.5
        h = thick_ref[k]
        nxt = jnp.minimum(k + 1, K - 1)
        h_next = thick_ref[nxt]
        hv = jnp.full((NI, NJ), h, F32)
        inv_space = 1.0 / (0.5 * (hv + h_next))
        inv_h = MIXING / hv

        def wet(d):
            return jnp.where(d > kf, 1.0, 0.0)

        mc = wet(depth)
        me, mw, mn, ms = wet(both_e), wet(both_w), wet(both_n), wet(both_s)
        below = jnp.where(jnp.logical_and(depth > kf + 1.0, k < K - 1), inv_space, 0.0)
        t = around(c, i, t_ref, 0)
        s = around(c, i, s_ref, 1)
        u0, ue, uw = around(c, i, u_ref, 2)[:3]
        v0, _, _, vn, vs = around(c, i, v_ref, 3)
        ae = 0.25 * me * (u0 + ue)
        aw = 0.25 * mw * (u0 + uw)
        an = 0.25 * mn * (v0 + vn)
        as_ = 0.25 * ms * (v0 + vs)
        ge, gw, gn, gs = DIFFUSION * me, DIFFUSION * mw, DIFFUSION * mn, DIFFUSION * ms

        def tracer(x, ref, flux_above):
            c, e, w, n, so = x
            total = aw * (w + c) - gw * (c - w) - ae * (c + e) + ge * (e - c)
            total = total + as_ * (so + c) - gs * (c - so) - an * (c + n) + gn * (n - c)
            flux = below * (ref[nxt] - c)
            return mc * (c + total + inv_h * (flux - flux_above)), flux

        new_t, flux_t = tracer(t, t_ref, flux_t)
        new_s, flux_s = tracer(s, s_ref, flux_s)
        ot_ref[k] = new_t
        os_ref[k] = new_s
        for m, (out, slope) in enumerate(((ou_ref, slope_u), (ov_ref, slope_v))):
            star = out[k] + gate(near_ew, kf, beyond_ew(2 + m, k)) + gate(near_ns, kf, beyond_ns(m, k))
            out[k] = gate(depth, kf, star - slope)
        return flux_t, flux_s

    def tracer_chunk(c, carry):
        for i in range(KC):
            carry = tracers(c, i, carry)
        return carry

    lax.fori_loop(0, NC, tracer_chunk, (zero,) * 2)

    drain(pack_out, send_sem.at[0])

    sent = pack_in.at[0, 0:3 * NI]

    @pl.when(not_south)
    def _():
        drain(sent, send_sem.at[1])

    drain(sent, send_sem.at[2])

    used = pl.ds(0, NI)
    drain(tiles.at[pl.ds(0, n_lon - 1), pl.ds(0, (EARLY + LATE) * NI + 6)], cast_send.at[0])

    @pl.when(not_south)
    def _():
        drain(rims.at[0, pl.ds(0, n_lon), used], cast_send.at[1])

    @pl.when(not_pole)
    def _():
        drain(rims.at[0, pl.ds(0, n_lon), used], cast_send.at[2])

    @pl.when(at_pole)
    def _():
        drain(rims.at[0, pl.ds(0, n_lon - 1), used], cast_send.at[2])

    drain(sums.at[pl.ds(0, n_lat - 1), pl.ds(0, 1)], cast_recv.at[6])
    total = functools.reduce(lambda a, b: a + b, [sums[lat, 0:1] for lat in range(n_lat)])
    rms = jnp.sqrt(total / (n_lon * NI * n_lat * NJ) + EPSILON)
    ox_ref[1] = jnp.broadcast_to(rms, (NI, NJ))
    drain(sums.at[pl.ds(0, n_lat - 1), pl.ds(0, 1)], cast_send.at[3])


def surface_solve(load, rim_rows, late_wait, share, n_lon, K, NI, NJ):
    width = NJ // NI
    tiles = range(2)
    lines = range(NI)
    lane = iota((n_lon, NJ), 1)
    edge = jnp.logical_or(lane == 0, lane == NJ - 1)

    def every(fn, *arrays):
        return [[fn(*(a[b][s] for a in arrays)) for s in lines] for b in tiles]

    def east(x):
        return [x[b][1:] + [pltpu.roll(x[b][0], n_lon - 1, 0)] for b in tiles]

    def west(x):
        return [[pltpu.roll(x[b][NI - 1], 1, 0)] + x[b][:-1] for b in tiles]

    def joined(x, shift, edge):
        moved = [[pltpu.roll(x[b][s], shift, 1) for s in lines] for b in tiles]
        return [[jnp.where(lane == edge, moved[1 - b][s], moved[b][s]) for s in lines] for b in tiles]

    def north(x):
        return joined(x, NJ - 1, NJ - 1)

    def south(x):
        return joined(x, 1, 0)

    height = load(0)
    scale = lambda a, c: jnp.minimum(a, c) * (1.0 / K)
    w_e = every(scale, height, east(height))
    w_w = every(scale, height, west(height))
    w_n = every(scale, height, north(height))
    w_s = every(scale, height, south(height))
    diag = every(lambda a, b, c, d: STORAGE + a + b + c + d, w_e, w_w, w_n, w_s)

    def apply(x):
        return every(
            lambda dg, c, we, e, ww, w, wn, n, ws, s: dg * c - (we * e + ww * w + wn * n + ws * s),
            diag, x, w_e, east(x), w_w, west(x), w_n, north(x), w_s, south(x))

    middle = NI // 2
    spans = [(s, s - 1, s + 1) for s in range(middle)]
    spans += [(s, s + 1, s - 1) for s in range(NI - 1, middle - 1, -1)]
    pivots, carries, factors = ([[None] * NI for _ in tiles] for _ in range(3))
    joints = []
    for b in tiles:
        for s, before, after in spans:
            back, ahead = (w_w, w_e) if after > s else (w_e, w_w)
            pivot = diag[b][s]
            if s not in (0, NI - 1):
                pivot = pivot + back[b][s] * factors[b][before]
            pivots[b][s] = 1.0 / pivot
            carries[b][s] = back[b][s] * pivots[b][s]
            factors[b][s] = -ahead[b][s] * pivots[b][s]
        joints.append(1.0 / (1.0 - factors[b][middle - 1] * factors[b][middle]))

    def precondition(r):
        out = []
        for b in tiles:
            part = [None] * NI
            for s, before, after in spans:
                part[s] = r[b][s] * pivots[b][s]
                if s not in (0, NI - 1):
                    part[s] = part[s] + carries[b][s] * part[before]
            low, high = part[middle - 1], part[middle]
            part[middle - 1] = (low - factors[b][middle - 1] * high) * joints[b]
            part[middle] = (high - factors[b][middle] * low) * joints[b]
            for s in range(middle - 2, -1, -1):
                part[s] = part[s] - factors[b][s] * part[s + 1]
            for s in range(middle + 1, NI):
                part[s] = part[s] - factors[b][s] * part[s - 1]
            out.append(part)
        return out

    x = load(1)
    drive = load(2)
    start = every(lambda h, d, a: jnp.where(h > 0.0, d, 0.0) - a, height, drive, apply(x))
    late_wait()
    t_u = load(EARLY)
    t_v = load(EARLY + 1)
    inner, outer = load(EARLY + LATE)
    for m, t in enumerate((t_u, t_v)):
        for b, (from_w, from_e) in enumerate(((inner[2 * m], inner[2 * m + 1]), (outer[m], outer[NI - 1 - m]))):
            t[b][NI - 1] = t[b][NI - 1] + pltpu.roll(from_w, n_lon - 1, 0)
            t[b][0] = t[b][0] + pltpu.roll(from_e, 1, 0)
        own, beyond = inner[4 + m], rim_rows(EARLY + LATE + 1 + m)
        for s in lines:
            for b, row in ((0, beyond), (1, own)):
                moved = pltpu.roll(row, (NJ - width * s) % NJ, 1) if s else row
                t[b][s] = t[b][s] + jnp.where(edge, moved, 0.0)
    residual = every(
        lambda h, d, e, w, n, s: d - jnp.where(h > 0.0, 0.5 * DIVERGENCE * ((e - w) + (n - s)), 0.0),
        height, start, east(t_u), west(t_u), north(t_v), south(t_v))
    mid = 0.5 * (SPECTRUM_HIGH + SPECTRUM_LOW)
    half = 0.5 * (SPECTRUM_HIGH - SPECTRUM_LOW)
    ratio = mid / half

    def across(d):
        out = every(lambda wn, n, ws, s: wn * n + ws * s, w_n, north(d), w_s, south(d))
        for b in tiles:
            out[b][NI - 1] = out[b][NI - 1] + w_e[b][NI - 1] * pltpu.roll(d[b][0], n_lon - 1, 0)
            out[b][0] = out[b][0] + w_w[b][0] * pltpu.roll(d[b][NI - 1], 1, 0)
        return out

    direction = precondition(residual)
    image = residual
    if mid != 1.0:
        direction, image = (every(lambda a: a / mid, f) for f in (direction, image))
    rho = 1.0 / ratio
    for step in range(ITERS):
        x = every(lambda a, b: a + b, x, direction)
        if step == 0 and mid == 1.0:
            residual = across(direction)
        else:
            residual = every(lambda r, m, c: (r - m) + c, residual, image, across(direction))
        if step + 1 < ITERS:
            rho_next = 1.0 / (2.0 * ratio - rho)
            keep, gain = rho_next * rho, 2.0 * rho_next / half
            direction = every(lambda d, z: keep * d + gain * z, direction, precondition(residual))
            image = every(lambda m, r: keep * m + gain * r, image, residual)
            rho = rho_next
    squares = [a * a for a in residual[0]]
    while len(squares) > 1:
        squares = [a + b for a, b in zip(squares[::2], squares[1::2])] + squares[len(squares) & ~1:]
    squares = squares[0]
    share(jnp.sum(jnp.sum(squares, axis=1, keepdims=True), axis=0, keepdims=True))
    slope_x = every(lambda e, w: 0.5 * (e - w), east(x), west(x))
    slope_y = every(lambda n, s: 0.5 * (n - s), north(x), south(x))
    return x[0], slope_x[0], slope_y[0]


def finish_kernel(kept, x_ref, ot_ref, os_ref, ou_ref, ov_ref, ox_ref, orms_ref, rms, sem):
    K = kept.shape[1]
    piece = K // 4 if K % 4 == 0 else K
    for f, target in enumerate((ot_ref, os_ref, ou_ref, ov_ref)):
        for first in range(0, K, piece):
            levels = pl.ds(first, piece)
            pltpu.make_async_copy(kept.at[f, levels], target.at[levels], sem.at[0]).start()
    surface = pltpu.make_async_copy(x_ref.at[0], ox_ref, sem.at[1])
    surface.start()
    rms[0] = jnp.max(x_ref[1])
    scalar = pltpu.make_async_copy(rms, orms_ref, sem.at[2])
    scalar.start()
    pltpu.make_async_copy(kept, kept, sem.at[0]).wait()
    surface.wait()
    scalar.wait()


def per_device(n_lon, n_lat, *args):
    K, NI, NJ = args[0].shape
    KC = 8 if K % 8 == 0 else K
    NC = K // KC
    vmem = pl.BlockSpec(memory_space=pltpu.VMEM)
    hbm = pl.BlockSpec(memory_space=pltpu.HBM)
    big = jax.ShapeDtypeStruct((K, NI, NJ), F32)
    tile = jax.ShapeDtypeStruct((NI, NJ), F32)
    one = jax.ShapeDtypeStruct((1,), F32)
    pack = pltpu.VMEM((2, NI + NC * 2 * KC + 4 * K, NJ), F32)

    def room(*lead):
        return pltpu.VMEM((*lead, NI, NJ), F32)

    parts = pl.pallas_call(
        functools.partial(step_kernel, n_lon, n_lat, KC),
        out_shape=(room(4, K), room(2)),
        in_specs=[hbm] * 9,
        out_specs=(vmem,) * 2,
        scratch_shapes=[
            room(4, K), pltpu.VMEM((2, NI, NJ), jnp.int32), room(2), pltpu.SMEM((K,), F32),
            pack, pack, room(2, 2), room(2, 2), room(2), room(2), room(4),
            room(2, K), room(K), pltpu.VMEM((n_lon, TILES * NI, NJ), F32), room(2), room(2, n_lon), room(n_lat),
            pltpu.VMEM((3, n_lon * NI, NJ), F32),
            pltpu.SemaphoreType.DMA((3,)), pltpu.SemaphoreType.DMA((3,)), pltpu.SemaphoreType.DMA((4,)),
            pltpu.SemaphoreType.DMA((4,)), pltpu.SemaphoreType.DMA((4,)), pltpu.SemaphoreType.DMA((7,)),
        ],
        compiler_params=pltpu.CompilerParams(
            collective_id=0, has_side_effects=True),
        name="step",
    )(*args)
    outs = pl.pallas_call(
        finish_kernel,
        out_shape=(big, big, big, big, tile, one),
        in_specs=[vmem] * 2,
        out_specs=(hbm,) * 6,
        scratch_shapes=[pltpu.SMEM((1,), F32), pltpu.SemaphoreType.DMA((3,))],
        name="finish",
    )(*[pltpu.with_memory_space_constraint(part, pltpu.VMEM) for part in parts])
    return outs[:5] + (outs[5].reshape(()),)


def solution(mesh):
    n_lon, n_lat = mesh.shape["lon"], mesh.shape["lat"]
    spec3 = P(None, "lon", "lat")
    spec2 = P("lon", "lat")
    return jax.shard_map(
        functools.partial(per_device, n_lon, n_lat),
        mesh=mesh,
        in_specs=(spec3, spec3, spec3, spec3, spec2, spec2, P(), spec2, spec2),
        out_specs=(spec3, spec3, spec3, spec3, spec2, P()),
        check_vma=False,
    )
```

```python
import functools

import jax
import jax.numpy as jnp
from jax import lax
from jax.experimental import pallas as pl
from jax.experimental.pallas import tpu as pltpu
from jax.sharding import PartitionSpec as P

ITERS = 4
DIFFUSION = 0.15
MIXING = 0.1
EXPANSION = 0.2
CONTRACTION = 0.15
PRESSURE_SCALE = 0.02
CORIOLIS = 0.5
FRICTION = 0.01
DIVERGENCE = 0.3
STORAGE = 0.1
SPECTRUM_LOW = 0.1
SPECTRUM_HIGH = 1.9
GRAVITY = 0.3
EPSILON = 1e-06

MESH = pl.DeviceIdType.MESH
F32 = jnp.float32
EARLY = 3
LATE = 2
TILES = EARLY + LATE + 1


def iota(shape, axis):
    return lax.broadcasted_iota(jnp.int32, shape, axis)


def flip(x, axis):
    return jnp.take_along_axis(x, x.shape[axis] - 1 - iota(x.shape, axis), axis=axis)


def flip_rows(x):
    return flip(x, 0)


def flip_lanes(x):
    return flip(x, 1)


def step_kernel(n_lon, n_lat, KC, *refs):
    sources, refs = refs[:9], refs[9:]
    (kept, ox_ref), refs = refs[:2], refs[2:]
    (fields, ints, floats, thick_ref, pack_out, pack_in, edges, slots, lap_edges, lap_slots, rim, laps, pressure, tiles, strips,
     rims, sums, held, load_sem, send_sem, chunk_sem, edge_sem, cast_send, cast_recv) = refs
    _, K, NI, NJ = fields.shape
    NC = K // KC
    SIDE = 2 * KC
    REST = NI + NC * SIDE
    t_ref, s_ref, u_ref, v_ref = (fields.at[f] for f in range(4))
    ot_ref, os_ref, ou_ref, ov_ref = (kept.at[f] for f in range(4))
    num_ref, sea_ref, eta_ref, drive_ref = ints.at[0], ints.at[1], floats.at[0], floats.at[1]
    p = lax.axis_index("lon")
    q = lax.axis_index("lat")
    east_dev = lax.rem(p + 1, n_lon)
    west_dev = lax.rem(p + n_lon - 1, n_lon)
    at_pole = q == n_lat - 1
    not_pole = q < n_lat - 1
    not_south = q > 0
    mirror = n_lon - 1 - p
    lons = [lax.rem(p + r, n_lon) for r in range(min(n_lon, 8))]

    barrier = pltpu.get_barrier_semaphore()

    def greet(lon, lat):
        pl.semaphore_signal(barrier, inc=1, device_id={"lon": lon, "lat": lat}, device_id_type=MESH)

    greet(east_dev, q)
    if n_lon > 2:
        greet(west_dev, q)

    def around_lon(first, last, fn):
        def visit(r, carry):
            fn(lax.rem(p + r, n_lon))
            return carry

        if n_lon <= 8:
            for lon in lons[first:last]:
                fn(lon)
        else:
            lax.fori_loop(first, last, visit, 0)

    @pl.when(at_pole)
    def _():
        around_lon(2, n_lon - 1, lambda lon: greet(lon, q))

    @pl.when(not_south)
    def _():
        around_lon(0, n_lon, lambda lon: greet(lon, q - 1))

    @pl.when(not_pole)
    def _():
        around_lon(0, n_lon, lambda lon: greet(lon, q + 1))

    def load(i, dst, sem):
        pltpu.make_async_copy(sources[i], dst, load_sem.at[sem]).start()

    load(4, num_ref, 1)
    load(5, sea_ref, 1)
    load(7, eta_ref, 1)
    load(8, drive_ref, 1)
    for f in (2, 3, 0, 1):
        load(f, fields.at[f], 0)
    thick_load = pltpu.make_async_copy(sources[6], thick_ref, load_sem.at[2])
    thick_load.start()

    @pl.when(not_pole)
    def _():
        around_lon(2, n_lon - 1, lambda lon: greet(lon, q))

    for lat in range(n_lat):
        @pl.when(jnp.logical_or(q - lat > 1, lat - q > 1))
        def _():
            greet(p, lat)

    def drain(ref, sem):
        pltpu.make_async_copy(ref, ref, sem).wait()

    thick_load.wait()
    drain(fields.at[0, 0:4], load_sem.at[1])
    drain(fields, load_sem.at[0])
    sub = iota((NI, NJ), 0)
    lane = iota((NI, NJ), 1)
    depth = (num_ref[...] * sea_ref[...]).astype(F32)

    for side, d1 in enumerate((NI - 1, 0)):
        for c in range(NC):
            levels = slice(c * KC, (c + 1) * KC)
            for m, ref in enumerate((u_ref, v_ref)):
                row = NI + c * SIDE + m * KC
                pack_out[side, row:row + KC, :] = ref[levels, d1, :]
        for m, ref in enumerate((t_ref, s_ref)):
            row = REST + m * K
            pack_out[side, row:row + K, :] = ref[:, d1, :]
        pack_out[side, 0:NI, :] = jnp.broadcast_to(depth[d1:d1 + 1, :], (NI, NJ))

    zero = jnp.zeros((NI, NJ), F32)

    def put(acc, x, source, target):
        moved = pltpu.roll(x, (target - source) % NJ, 1) if source != target else x
        return jnp.where(lane == target, moved, acc)

    n0 = s0 = zero
    for f, ref in enumerate((t_ref, s_ref, u_ref, v_ref)):
        for k in range(K):
            n0 = put(n0, ref[k], NJ - 1, f * K + k)
            s0 = put(s0, ref[k], 0, f * K + k)
    npk, spk = edges.at[0], edges.at[1]
    npk[0] = n0
    npk[1] = put(zero, depth, NJ - 1, 0)
    spk[0] = s0
    spk[1] = put(zero, depth, 0, 0)

    peers = n_lon + n_lat - 2 + (n_lon - 1) * (not_south.astype(jnp.int32) + not_pole.astype(jnp.int32))
    pl.semaphore_wait(barrier, peers)

    def copy(src, dst, lon, lat, out, into):
        return pltpu.make_async_remote_copy(
            src_ref=src, dst_ref=dst, send_sem=out, recv_sem=into,
            device_id={"lon": lon, "lat": lat}, device_id_type=MESH)

    def meet_pole(pack, slot, sem):
        @pl.when(at_pole)
        def _():
            copy(pack.at[0], slot.at[0], mirror, q, send_sem.at[2], edge_sem.at[sem]).start()

    def meet_near(pack, slot, sem):
        @pl.when(not_south)
        def _():
            copy(pack.at[1], slot.at[0], p, q - 1, send_sem.at[1], edge_sem.at[sem]).start()

        @pl.when(not_pole)
        def _():
            copy(pack.at[0], slot.at[1], p, q + 1, send_sem.at[2], edge_sem.at[sem + 1]).start()

    def met(slot, sem):
        drain(slot.at[0], edge_sem.at[sem])

        @pl.when(not_south)
        def _():
            drain(slot.at[1], edge_sem.at[sem + 1])

    meet_pole(edges, slots, 0)

    def aside(way, first, rows, sem):
        rows = pl.ds(first, rows)
        lon = west_dev if way else east_dev
        copy(pack_out.at[way, rows], pack_in.at[1 - way, rows], lon, q, send_sem.at[0], chunk_sem.at[sem]).start()

    def sides(first, rows, sem):
        aside(1, first, rows, sem)
        aside(0, first, rows, sem)

    half = (NC + 1) // 2
    bounds = ((0, NI + half * SIDE), (NI + half * SIDE, REST)) if NC > 1 else ((0, REST),)
    for way in (1, 0):
        for i, (first, last) in enumerate(bounds):
            aside(way, first, last - first, i)
    meet_near(edges, slots, 0)

    height = zero
    for k in range(K):
        height = height + jnp.where(depth > k + 0.5, thick_ref[k], 0.0)
    width = NJ // NI
    in_block = lane // width == sub
    parts = ((0, EARLY, EARLY * NI), (EARLY, LATE + 3, LATE * NI + 6))

    def pack_strips(which, sign, arrays, rows=()):
        first, count, _ = parts[which]
        given = len(arrays)
        south = zero
        north = zero
        for i, x in enumerate(arrays):
            for start in (0, width):
                moved = pltpu.roll(x, start, 1, stride=width, stride_axis=0)
                row = jnp.sum(jnp.where(in_block, moved, 0.0), axis=0, keepdims=True)
                row = jnp.broadcast_to(row, (NI, NJ))
                if start:
                    north = jnp.where(sub == i, row, north)
                else:
                    south = jnp.where(sub == i, row, south)
        for i, row in enumerate(rows):
            north = jnp.where(sub == given + i, row, north)
            south = jnp.where(sub == given + i, row, south)
        turned = jnp.where(sub >= given, pltpu.roll(north, width, 1), north) if rows else north
        north = jnp.where(at_pole, sign * flip_lanes(turned), north)
        rows = slice(first, first + count)
        strips[0, rows] = south[:count]
        strips[1, rows] = north[:count]

        @pl.when(at_pole)
        def _():
            rims[0, mirror, rows] = north[:count]

    def each_other(fn):
        def visit(r, carry):
            fn(jnp.where(r <= p, r - 1, r))
            return carry

        if n_lon <= 8:
            for r in range(1, n_lon):
                visit(r, 0)
        else:
            lax.fori_loop(1, n_lon, visit, 0)

    def cast(which):
        first, count, size = parts[which]
        mine = tiles.at[p, pl.ds(first * NI, size)]
        rows = pl.ds(first, count)
        pole = at_pole.astype(jnp.int32)
        side, lat = 1 - pole, q + 1 - pole
        slot = jnp.where(at_pole, mirror, p)

        def send(way, side, slot, lon, lat, out):
            copy(strips.at[way, rows], rims.at[side, slot, rows], lon, lat, cast_send.at[out],
                 cast_recv.at[3 * which + 1 + side]).start()

        @pl.when(not_pole)
        def _():
            send(1, 1, p, p, q + 1, 2)

        @pl.when(not_south)
        def _():
            send(0, 0, p, p, q - 1, 1)

        def to(lon):
            copy(mine, mine, lon, q, cast_send.at[0], cast_recv.at[3 * which]).start()

            @pl.when(not_south)
            def _():
                send(0, 0, p, lon, q - 1, 1)

            send(1, side, slot, lon, lat, 2)
        each_other(to)

    def cast_wait(which):
        first, count, size = parts[which]
        rows = pl.ds(first, count)
        drain(tiles.at[pl.ds(0, n_lon - 1), pl.ds(first * NI, size)], cast_recv.at[3 * which])

        @pl.when(at_pole)
        def _():
            drain(rims.at[0, pl.ds(0, n_lon - 1), rows], cast_recv.at[3 * which + 1])

        @pl.when(not_pole)
        def _():
            drain(rims.at[0, pl.ds(0, n_lon), rows], cast_recv.at[3 * which + 1])

        @pl.when(not_south)
        def _():
            drain(rims.at[1, pl.ds(0, n_lon), rows], cast_recv.at[3 * which + 2])

    first_guess = sea_ref[...].astype(F32) * eta_ref[...]
    for i, x in enumerate((height, first_guess, drive_ref[...])):
        tiles[p, i * NI:(i + 1) * NI] = x
    pack_strips(0, 1.0, (height, first_guess, drive_ref[...]))

    near_e = jnp.where(sub == NI - 1, 0.0, jnp.minimum(depth, pltpu.roll(depth, NI - 1, 0)))
    near_w = jnp.where(sub == 0, 0.0, jnp.minimum(depth, pltpu.roll(depth, 1, 0)))
    near_n = jnp.where(lane == NJ - 1, 0.0, jnp.minimum(depth, pltpu.roll(depth, NJ - 1, 1)))
    near_s = jnp.where(lane == 0, 0.0, jnp.minimum(depth, pltpu.roll(depth, 1, 1)))
    lat_index = (q * NJ + lane).astype(F32)
    coriolis = CORIOLIS * (2.0 * (lat_index + 0.5) / (n_lat * NJ) - 1.0)

    def gate(d, kf, x):
        return jnp.where(d > kf, x, 0.0)

    def inner_lap(x, kf):
        total = gate(near_e, kf, pltpu.roll(x, NI - 1, 0) - x) + gate(near_w, kf, pltpu.roll(x, 1, 0) - x)
        return total + (gate(near_n, kf, pltpu.roll(x, NJ - 1, 1) - x) + gate(near_s, kf, pltpu.roll(x, 1, 1) - x))

    def before_level(k, carry):
        pc, tu, tv = carry
        kf = lax.convert_element_type(k, F32) + 0.5
        u, v = u_ref[k], v_ref[k]
        laps[0, k] = inner_lap(u, kf)
        laps[1, k] = inner_lap(v, kf)
        pc = pc + gate(depth, kf, (CONTRACTION * s_ref[k] - EXPANSION * t_ref[k]) * thick_ref[k])
        pressure[k] = pc
        grad_x = gate(near_e, kf, pltpu.roll(pc, NI - 1, 0) - pc) + gate(near_w, kf, pc - pltpu.roll(pc, 1, 0))
        grad_y = gate(near_n, kf, pltpu.roll(pc, NJ - 1, 1) - pc) + gate(near_s, kf, pc - pltpu.roll(pc, 1, 1))
        u_part = u + coriolis * v - (0.5 * PRESSURE_SCALE) * grad_x
        v_part = v - coriolis * u - (0.5 * PRESSURE_SCALE) * grad_y
        ou_ref[k] = u_part
        ov_ref[k] = v_part
        h = thick_ref[k]
        return pc, tu + gate(depth, kf, h * u_part), tv + gate(depth, kf, h * v_part)

    def before_chunk(c, carry):
        for i in range(KC):
            carry = before_level(c * KC + i, carry)
        return carry

    totals = list(lax.fori_loop(0, NC, before_chunk, (zero,) * 3)[1:])

    cast(0)
    met(slots, 0)

    sign = jnp.where(lane >= 2 * K, -1.0, 1.0).astype(F32)

    def arrived(slot, i, fold):
        north = jnp.where(at_pole, flip_rows(slot[0, i]) * fold, slot[0, i])
        return north, jnp.where(not_south, slot[1, i], 0.0)

    pn0, ps0 = arrived(slots, 0, sign)
    pn1, ps1 = arrived(slots, 1, 1.0)

    def shift_e(x, row):
        return jnp.where(sub == NI - 1, row, pltpu.roll(x, NI - 1, 0))

    def shift_w(x, row):
        return jnp.where(sub == 0, row, pltpu.roll(x, 1, 0))

    rim[0] = pn0
    rim[1] = ps0

    drain(pack_in.at[:, bounds[0][0]:bounds[0][1]], chunk_sem.at[0])
    base_e = pack_in[0, 0:1, :]
    base_w = pack_in[1, 0:1, :]
    is_w = sub == 0
    is_s = lane == 0
    depth_ew = jnp.where(is_w, base_w, base_e)
    depth_ns = jnp.where(is_s, ps1, pltpu.roll(pn1, NJ - 1, 1))
    on_ew = jnp.logical_or(is_w, sub == NI - 1)
    on_ns = jnp.logical_or(is_s, lane == NJ - 1)
    near_ew = jnp.where(on_ew, jnp.minimum(depth, depth_ew), 0.0)
    near_ns = jnp.where(on_ns, jnp.minimum(depth, depth_ns), 0.0)
    scale_ew = jnp.where(is_w, 0.5 * PRESSURE_SCALE, -0.5 * PRESSURE_SCALE)
    scale_ns = jnp.where(is_s, 0.5 * PRESSURE_SCALE, -0.5 * PRESSURE_SCALE)

    def rim_ns(north, south, k):
        x = pltpu.roll(north, (NJ - 1 - k) % NJ, 1)
        return jnp.where(is_s, pltpu.roll(south, (NJ - k) % NJ, 1), x)

    def side_ew(c, row):
        row = NI + c * SIDE + row
        return jnp.where(is_w, pack_in[1, row:row + 1, :], pack_in[0, row:row + 1, :])

    both_e = jnp.where(sub == NI - 1, near_ew, near_e)
    both_w = jnp.where(is_w, near_ew, near_w)
    both_n = jnp.where(lane == NJ - 1, near_ns, near_n)
    both_s = jnp.where(is_s, near_ns, near_s)
    overlaps = (both_e, both_w, both_n, both_s)
    sums_lap = [[zero] * 4 for _ in range(2)]
    push_ew = push_ns = zero
    for c in range(NC):
        if c == half and NC > 1:
            drain(pack_in.at[:, bounds[1][0]:bounds[1][1]], chunk_sem.at[1])
        for i in range(KC):
            k = c * KC + i
            kf = k + 0.5
            h = thick_ref[k]
            hp = h * pressure[k]
            push_ew = push_ew + gate(near_ew, kf, hp)
            push_ns = push_ns + gate(near_ns, kf, hp)
            for m, x in enumerate((u_ref[k], v_ref[k])):
                lap = laps[m, k] + gate(near_ew, kf, side_ew(c, m * KC + i) - x)
                lap = lap + gate(near_ns, kf, rim_ns(rim[0], rim[1], (2 + m) * K + k) - x)
                laps[m, k] = lap
                hl = h * lap
                sums_lap[m] = [a + gate(d, kf, hl) for a, d in zip(sums_lap[m], overlaps)]
    push_ew = scale_ew * push_ew
    push_ns = scale_ns * push_ns
    exports, exports_ns = [], []
    for m, (a_e, a_w, a_n, a_s) in enumerate(sums_lap):
        given = jnp.where(sub == NI - 1, 0.0, pltpu.roll(a_w, NI - 1, 0)) + jnp.where(is_w, 0.0, pltpu.roll(a_e, 1, 0))
        given = given + jnp.where(lane == NJ - 1, 0.0, pltpu.roll(a_s, NJ - 1, 1))
        given = given + jnp.where(is_s, 0.0, pltpu.roll(a_n, 1, 1))
        totals[m] = totals[m] + FRICTION * ((a_e + a_w) + (a_n + a_s) - given)
        exports.append(-FRICTION * jnp.where(is_w, a_w, a_e))
        exports_ns.append(-FRICTION * jnp.where(is_s, a_s, a_n))
    totals = [totals[0] - push_ew, totals[1] - push_ns]
    exports[0] = exports[0] - push_ew
    exports_ns[1] = exports_ns[1] - push_ns

    tiles[p, EARLY * NI:(EARLY + 1) * NI] = totals[0]
    tiles[p, (EARLY + 1) * NI:(EARLY + 2) * NI] = totals[1]
    for m in range(2):
        row = (EARLY + LATE) * NI + 2 * m
        tiles[p, row:row + 1] = exports[m][0:1]
        tiles[p, row + 1:row + 2] = exports[m][NI - 1:]
    out_rows = zero
    for row, x in ((0, exports[0][0:1]), (1, exports[1][0:1]), (NI - 2, exports[1][NI - 1:]), (NI - 1, exports[0][NI - 1:])):
        out_rows = jnp.where(sub == row, jnp.broadcast_to(x, (NI, NJ)), out_rows)
    ns_rows = []
    for m, x in enumerate(exports_ns):
        x = jnp.where(lane == 0, pltpu.roll(x, 1, 1), jnp.where(lane == NJ - 1, pltpu.roll(x, NJ - 1, 1), 0.0))
        x = jnp.sum(pltpu.roll(x, 0, 1, stride=width, stride_axis=0), axis=0, keepdims=True)
        row = (EARLY + LATE) * NI + 4 + m
        tiles[p, row:row + 1] = x
        ns_rows.append(jnp.broadcast_to(x, (NI, NJ)))
    pack_strips(1, -1.0, (*totals, out_rows), ns_rows)
    cast(1)

    sides(REST, 2 * K, 2)
    for side, (d, push) in enumerate(((NI - 1, 0.5 * PRESSURE_SCALE), (0, -0.5 * PRESSURE_SCALE))):
        row = REST + 2 * K
        pack_out[side, row:row + K, :] = push * pressure[:, d, :] - FRICTION * laps[0, :, d, :]
        pack_out[side, row + K:row + 2 * K, :] = -FRICTION * laps[1, :, d, :]
    n2 = s2 = zero
    for k in range(K):
        for m, x in enumerate((-FRICTION * laps[0, k], -FRICTION * laps[1, k] - scale_ns * pressure[k])):
            n2 = put(n2, x, NJ - 1, m * K + k)
            s2 = put(s2, x, 0, m * K + k)
    lap_edges[0] = n2
    lap_edges[1] = s2
    meet_pole(lap_edges, lap_slots, 2)
    meet_near(lap_edges, lap_slots, 2)
    sides(REST + 2 * K, 2 * K, 3)

    def level(c, carry):
        for i in range(KC):
            k = c * KC + i
            kf = lax.convert_element_type(k, F32) + 0.5
            pc = pressure[k]
            parts = (ou_ref[k] - scale_ew * gate(near_ew, kf, pc), ov_ref[k] - scale_ns * gate(near_ns, kf, pc))
            for m, (part, out) in enumerate(zip(parts, (ou_ref, ov_ref))):
                lap = laps[m, k]
                inner = inner_lap(lap, kf) - gate(near_ew, kf, lap) - gate(near_ns, kf, lap)
                out[k] = gate(depth, kf, part - FRICTION * inner)
        return carry

    lax.fori_loop(0, NC, level, 0)

    cast_wait(0)
    flat = tiles.reshape(n_lon * TILES * NI, NJ)
    flat_rim = rims.reshape(2 * n_lon * NI, NJ)
    lanes = iota((n_lon, NJ), 1)

    def loader(f):
        main = [flat[pl.ds(f * NI + s, n_lon, stride=TILES * NI), :] for s in range(NI)]
        north = flat_rim[pl.ds(f, n_lon, stride=NI), :]
        south = jnp.where(not_south, flat_rim[pl.ds(n_lon * NI + f, n_lon, stride=NI), :], 0.0)
        outer = []
        for s in range(NI):
            x = jnp.where(lanes >= NJ - width, pltpu.roll(south, (NJ - width - width * s) % NJ, 1), 0.0)
            outer.append(jnp.where(lanes < width, pltpu.roll(north, (NJ - width * s) % NJ, 1), x))
        return [main, outer]

    def rim_rows(f):
        north = flat_rim[pl.ds(f, n_lon, stride=NI), :]
        south = jnp.where(not_south, flat_rim[pl.ds(n_lon * NI + f, n_lon, stride=NI), :], 0.0)
        return jnp.where(lanes % width == width - 1, north, south)

    def share(total):
        sums[q] = jnp.broadcast_to(total, (NI, NJ))
        mine = sums.at[q, pl.ds(0, 1)]
        for r in range(1, n_lat):
            lat = jnp.where(r <= q, r - 1, r)
            copy(mine, mine, p, lat, cast_send.at[3], cast_recv.at[6]).start()


    def late_wait():
        cast_wait(1)

    x, slope_x, slope_y = surface_solve(loader, rim_rows, late_wait, share, n_lon, K, NI, NJ)
    for i, field in enumerate((x, slope_x, slope_y)):
        for s in range(NI):
            held[i, pl.ds(s, n_lon, stride=NI), :] = field[s]
    block = pl.ds(pl.multiple_of(p * NI, NI), NI)
    ox_ref[0] = held[0, block, :]
    slope_u = GRAVITY * held[1, block, :]
    slope_v = GRAVITY * held[2, block, :]
    drain(pack_in.at[:, REST:REST + 2 * K], chunk_sem.at[2])
    drain(pack_in.at[:, REST + 2 * K:], chunk_sem.at[3])
    met(lap_slots, 2)
    rim[2] = jnp.where(at_pole, -flip_rows(lap_slots[0]), lap_slots[0])
    rim[3] = jnp.where(not_south, lap_slots[1], 0.0)
    def shift_n(x, packed, source):
        return jnp.where(lane == NJ - 1, pltpu.roll(packed, NJ - 1 - source, 1), pltpu.roll(x, NJ - 1, 1))

    def shift_s(x, packed, source):
        return jnp.where(lane == 0, pltpu.roll(packed, lax.rem(NJ - source, NJ), 1), pltpu.roll(x, 1, 1))

    def around(c, inner, ref, f):
        k = c * KC + inner
        x = ref[k]
        row = pl.ds(NI + c * SIDE + (f - 2) * KC + inner if f >= 2 else REST + f * K + k, 1)
        return (x, shift_e(x, pack_in[0, row, :]), shift_w(x, pack_in[1, row, :]),
                shift_n(x, rim[0], f * K + k), shift_s(x, rim[1], f * K + k))

    def beyond_ew(f, k):
        row = pl.ds(REST + f * K + k, 1)
        return jnp.where(is_w, pack_in[1, row, :], pack_in[0, row, :])

    def beyond_ns(f, k):
        at = f * K + k
        north = pltpu.roll(rim[2], NJ - 1 - at, 1)
        return jnp.where(is_s, pltpu.roll(rim[3], lax.rem(NJ - at, NJ), 1), north)

    def tracers(c, i, carry):
        k = c * KC + i
        flux_t, flux_s = carry
        kf = lax.convert_element_type(k, F32) + 0.5
        h = thick_ref[k]
        nxt = jnp.minimum(k + 1, K - 1)
        h_next = thick_ref[nxt]
        hv = jnp.full((NI, NJ), h, F32)
        inv_space = 1.0 / (0.5 * (hv + h_next))
        inv_h = MIXING / hv

        def wet(d):
            return jnp.where(d > kf, 1.0, 0.0)

        mc = wet(depth)
        me, mw, mn, ms = wet(both_e), wet(both_w), wet(both_n), wet(both_s)
        below = jnp.where(jnp.logical_and(depth > kf + 1.0, k < K - 1), inv_space, 0.0)
        t = around(c, i, t_ref, 0)
        s = around(c, i, s_ref, 1)
        u0, ue, uw = around(c, i, u_ref, 2)[:3]
        v0, _, _, vn, vs = around(c, i, v_ref, 3)
        ae = 0.25 * me * (u0 + ue)
        aw = 0.25 * mw * (u0 + uw)
        an = 0.25 * mn * (v0 + vn)
        as_ = 0.25 * ms * (v0 + vs)
        ge, gw, gn, gs = DIFFUSION * me, DIFFUSION * mw, DIFFUSION * mn, DIFFUSION * ms

        def tracer(x, ref, flux_above):
            c, e, w, n, so = x
            total = aw * (w + c) - gw * (c - w) - ae * (c + e) + ge * (e - c)
            total = total + as_ * (so + c) - gs * (c - so) - an * (c + n) + gn * (n - c)
            flux = below * (ref[nxt] - c)
            return mc * (c + total + inv_h * (flux - flux_above)), flux

        new_t, flux_t = tracer(t, t_ref, flux_t)
        new_s, flux_s = tracer(s, s_ref, flux_s)
        ot_ref[k] = new_t
        os_ref[k] = new_s
        for m, (out, slope) in enumerate(((ou_ref, slope_u), (ov_ref, slope_v))):
            star = out[k] + gate(near_ew, kf, beyond_ew(2 + m, k)) + gate(near_ns, kf, beyond_ns(m, k))
            out[k] = gate(depth, kf, star - slope)
        return flux_t, flux_s

    def tracer_chunk(c, carry):
        for i in range(KC):
            carry = tracers(c, i, carry)
        return carry

    lax.fori_loop(0, NC, tracer_chunk, (zero,) * 2)

    drain(pack_out, send_sem.at[0])

    sent = pack_in.at[0, 0:3 * NI]

    @pl.when(not_south)
    def _():
        drain(sent, send_sem.at[1])

    drain(sent, send_sem.at[2])

    used = pl.ds(0, NI)
    drain(tiles.at[pl.ds(0, n_lon - 1), pl.ds(0, (EARLY + LATE) * NI + 6)], cast_send.at[0])

    @pl.when(not_south)
    def _():
        drain(rims.at[0, pl.ds(0, n_lon), used], cast_send.at[1])

    @pl.when(not_pole)
    def _():
        drain(rims.at[0, pl.ds(0, n_lon), used], cast_send.at[2])

    @pl.when(at_pole)
    def _():
        drain(rims.at[0, pl.ds(0, n_lon - 1), used], cast_send.at[2])

    drain(sums.at[pl.ds(0, n_lat - 1), pl.ds(0, 1)], cast_recv.at[6])
    total = functools.reduce(lambda a, b: a + b, [sums[lat, 0:1] for lat in range(n_lat)])
    rms = jnp.sqrt(total / (n_lon * NI * n_lat * NJ) + EPSILON)
    ox_ref[1] = jnp.broadcast_to(rms, (NI, NJ))
    drain(sums.at[pl.ds(0, n_lat - 1), pl.ds(0, 1)], cast_send.at[3])


def surface_solve(load, rim_rows, late_wait, share, n_lon, K, NI, NJ):
    width = NJ // NI
    tiles = range(2)
    lines = range(NI)
    lane = iota((n_lon, NJ), 1)
    edge = jnp.logical_or(lane == 0, lane == NJ - 1)

    def every(fn, *arrays):
        return [[fn(*(a[b][s] for a in arrays)) for s in lines] for b in tiles]

    def east(x):
        return [x[b][1:] + [pltpu.roll(x[b][0], n_lon - 1, 0)] for b in tiles]

    def west(x):
        return [[pltpu.roll(x[b][NI - 1], 1, 0)] + x[b][:-1] for b in tiles]

    def joined(x, shift, edge):
        moved = [[pltpu.roll(x[b][s], shift, 1) for s in lines] for b in tiles]
        return [[jnp.where(lane == edge, moved[1 - b][s], moved[b][s]) for s in lines] for b in tiles]

    def north(x):
        return joined(x, NJ - 1, NJ - 1)

    def south(x):
        return joined(x, 1, 0)

    height = load(0)
    scale = lambda a, c: jnp.minimum(a, c) * (1.0 / K)
    w_e = every(scale, height, east(height))
    w_w = every(scale, height, west(height))
    w_n = every(scale, height, north(height))
    w_s = every(scale, height, south(height))
    diag = every(lambda a, b, c, d: STORAGE + a + b + c + d, w_e, w_w, w_n, w_s)

    def apply(x):
        return every(
            lambda dg, c, we, e, ww, w, wn, n, ws, s: dg * c - (we * e + ww * w + wn * n + ws * s),
            diag, x, w_e, east(x), w_w, west(x), w_n, north(x), w_s, south(x))

    middle = NI // 2
    spans = [(s, s - 1, s + 1) for s in range(middle)]
    spans += [(s, s + 1, s - 1) for s in range(NI - 1, middle - 1, -1)]
    pivots, carries, factors = ([[None] * NI for _ in tiles] for _ in range(3))
    joints = []
    for b in tiles:
        for s, before, after in spans:
            back, ahead = (w_w, w_e) if after > s else (w_e, w_w)
            pivot = diag[b][s]
            if s not in (0, NI - 1):
                pivot = pivot + back[b][s] * factors[b][before]
            pivots[b][s] = 1.0 / pivot
            carries[b][s] = back[b][s] * pivots[b][s]
            factors[b][s] = -ahead[b][s] * pivots[b][s]
        joints.append(1.0 / (1.0 - factors[b][middle - 1] * factors[b][middle]))

    def precondition(r):
        out = []
        for b in tiles:
            part = [None] * NI
            for s, before, after in spans:
                part[s] = r[b][s] * pivots[b][s]
                if s not in (0, NI - 1):
                    part[s] = part[s] + carries[b][s] * part[before]
            low, high = part[middle - 1], part[middle]
            part[middle - 1] = (low - factors[b][middle - 1] * high) * joints[b]
            part[middle] = (high - factors[b][middle] * low) * joints[b]
            for s in range(middle - 2, -1, -1):
                part[s] = part[s] - factors[b][s] * part[s + 1]
            for s in range(middle + 1, NI):
                part[s] = part[s] - factors[b][s] * part[s - 1]
            out.append(part)
        return out

    x = load(1)
    drive = load(2)
    start = every(lambda h, d, a: jnp.where(h > 0.0, d, 0.0) - a, height, drive, apply(x))
    late_wait()
    t_u = load(EARLY)
    t_v = load(EARLY + 1)
    inner, outer = load(EARLY + LATE)
    for m, t in enumerate((t_u, t_v)):
        for b, (from_w, from_e) in enumerate(((inner[2 * m], inner[2 * m + 1]), (outer[m], outer[NI - 1 - m]))):
            t[b][NI - 1] = t[b][NI - 1] + pltpu.roll(from_w, n_lon - 1, 0)
            t[b][0] = t[b][0] + pltpu.roll(from_e, 1, 0)
        own, beyond = inner[4 + m], rim_rows(EARLY + LATE + 1 + m)
        for s in lines:
            for b, row in ((0, beyond), (1, own)):
                moved = pltpu.roll(row, (NJ - width * s) % NJ, 1) if s else row
                t[b][s] = t[b][s] + jnp.where(edge, moved, 0.0)
    residual = every(
        lambda h, d, e, w, n, s: d - jnp.where(h > 0.0, 0.5 * DIVERGENCE * ((e - w) + (n - s)), 0.0),
        height, start, east(t_u), west(t_u), north(t_v), south(t_v))
    mid = 0.5 * (SPECTRUM_HIGH + SPECTRUM_LOW)
    half = 0.5 * (SPECTRUM_HIGH - SPECTRUM_LOW)
    ratio = mid / half

    def across(d):
        out = every(lambda wn, n, ws, s: wn * n + ws * s, w_n, north(d), w_s, south(d))
        for b in tiles:
            out[b][NI - 1] = out[b][NI - 1] + w_e[b][NI - 1] * pltpu.roll(d[b][0], n_lon - 1, 0)
            out[b][0] = out[b][0] + w_w[b][0] * pltpu.roll(d[b][NI - 1], 1, 0)
        return out

    direction = precondition(residual)
    image = residual
    if mid != 1.0:
        direction, image = (every(lambda a: a / mid, f) for f in (direction, image))
    rho = 1.0 / ratio
    for step in range(ITERS):
        x = every(lambda a, b: a + b, x, direction)
        if step == 0 and mid == 1.0:
            residual = across(direction)
        else:
            residual = every(lambda r, m, c: (r - m) + c, residual, image, across(direction))
        if step + 1 < ITERS:
            rho_next = 1.0 / (2.0 * ratio - rho)
            keep, gain = rho_next * rho, 2.0 * rho_next / half
            direction = every(lambda d, z: keep * d + gain * z, direction, precondition(residual))
            image = every(lambda m, r: keep * m + gain * r, image, residual)
            rho = rho_next
    squares = [a * a for a in residual[0]]
    while len(squares) > 1:
        squares = [a + b for a, b in zip(squares[::2], squares[1::2])] + squares[len(squares) & ~1:]
    squares = squares[0]
    share(jnp.sum(jnp.sum(squares, axis=1, keepdims=True), axis=0, keepdims=True))
    slope_x = every(lambda e, w: 0.5 * (e - w), east(x), west(x))
    slope_y = every(lambda n, s: 0.5 * (n - s), north(x), south(x))
    return x[0], slope_x[0], slope_y[0]


def finish_kernel(kept, x_ref, ot_ref, os_ref, ou_ref, ov_ref, ox_ref, orms_ref, rms, sem):
    K = kept.shape[1]
    piece = K // 4 if K % 4 == 0 else K
    for f, target in enumerate((ot_ref, os_ref, ou_ref, ov_ref)):
        for first in range(0, K, piece):
            levels = pl.ds(first, piece)
            pltpu.make_async_copy(kept.at[f, levels], target.at[levels], sem.at[0]).start()
    surface = pltpu.make_async_copy(x_ref.at[0], ox_ref, sem.at[1])
    surface.start()
    rms[0] = jnp.max(x_ref[1])
    scalar = pltpu.make_async_copy(rms, orms_ref, sem.at[2])
    scalar.start()
    pltpu.make_async_copy(kept, kept, sem.at[0]).wait()
    surface.wait()
    scalar.wait()


def per_device(n_lon, n_lat, *args):
    K, NI, NJ = args[0].shape
    KC = 8 if K % 8 == 0 else K
    NC = K // KC
    vmem = pl.BlockSpec(memory_space=pltpu.VMEM)
    hbm = pl.BlockSpec(memory_space=pltpu.HBM)
    big = jax.ShapeDtypeStruct((K, NI, NJ), F32)
    tile = jax.ShapeDtypeStruct((NI, NJ), F32)
    one = jax.ShapeDtypeStruct((1,), F32)
    pack = pltpu.VMEM((2, NI + NC * 2 * KC + 4 * K, NJ), F32)

    def room(*lead):
        return pltpu.VMEM((*lead, NI, NJ), F32)

    parts = pl.pallas_call(
        functools.partial(step_kernel, n_lon, n_lat, KC),
        out_shape=(room(4, K), room(2)),
        in_specs=[hbm] * 9,
        out_specs=(vmem,) * 2,
        scratch_shapes=[
            room(4, K), pltpu.VMEM((2, NI, NJ), jnp.int32), room(2), pltpu.SMEM((K,), F32),
            pack, pack, room(2, 2), room(2, 2), room(2), room(2), room(4),
            room(2, K), room(K), pltpu.VMEM((n_lon, TILES * NI, NJ), F32), room(2), room(2, n_lon), room(n_lat),
            pltpu.VMEM((3, n_lon * NI, NJ), F32),
            pltpu.SemaphoreType.DMA((3,)), pltpu.SemaphoreType.DMA((3,)), pltpu.SemaphoreType.DMA((4,)),
            pltpu.SemaphoreType.DMA((4,)), pltpu.SemaphoreType.DMA((4,)), pltpu.SemaphoreType.DMA((7,)),
        ],
        compiler_params=pltpu.CompilerParams(
            collective_id=0, has_side_effects=True),
        name="step",
    )(*args)
    outs = pl.pallas_call(
        finish_kernel,
        out_shape=(big, big, big, big, tile, one),
        in_specs=[vmem] * 2,
        out_specs=(hbm,) * 6,
        scratch_shapes=[pltpu.SMEM((1,), F32), pltpu.SemaphoreType.DMA((3,))],
        name="finish",
    )(*[pltpu.with_memory_space_constraint(part, pltpu.VMEM) for part in parts])
    return outs[:5] + (outs[5].reshape(()),)


def solution(mesh):
    n_lon, n_lat = mesh.shape["lon"], mesh.shape["lat"]
    spec3 = P(None, "lon", "lat")
    spec2 = P("lon", "lat")
    return jax.shard_map(
        functools.partial(per_device, n_lon, n_lat),
        mesh=mesh,
        in_specs=(spec3, spec3, spec3, spec3, spec2, spec2, P(), spec2, spec2),
        out_specs=(spec3, spec3, spec3, spec3, spec2, P()),
        check_vma=False,
    )
```
